64 devices in a mesh: dp: 4 (over x, y), tp: 16 (over z, core).
Axes of the slice: x: 2, y: 2, z: 8, core: 2. Of those that a mesh axis runs over, the one named last changes fastest.
The devices are a block of a 4x4x8 slice.
Arguments:
- y_one: float32 [192, 64, 1024], P('dp'), parts along dimension 0
- y_two: float32 [192, 64, 1024], P('dp'), parts along dimension 0
- dy_one: float32 [192, 64, 1024], P('dp'), parts along dimension 0
- dy_two: float32 [192, 64, 1024], P('dp'), parts along dimension 0
- seq_lens: int32 [192], P('dp'), parts along dimension 0
- w_query: bfloat16 [1, 1024, 16, 128], P(None, None, 'tp')
- w_key: bfloat16 [1, 1024, 16, 128], P(None, None, 'tp')
- w_value: bfloat16 [1, 1024, 16, 128], P(None, None, 'tp')
- w_out: bfloat16 [1, 16, 128, 1024], P(None, 'tp')
- w_up: bfloat16 [1, 1024, 3072], P(None, None, 'tp')
- w_down: bfloat16 [1, 3072, 1024], P(None, 'tp')
Outputs:
- output 1: float32 [192, 64, 1024], P('dp'), parts along dimension 0
- output 2: float32 [192, 64, 1024], P('dp'), parts along dimension 0
- output 3: float32 [192, 64, 1024], P('dp'), parts along dimension 0
- output 4: float32 [192, 64, 1024], P('dp'), parts along dimension 0
- output 5: float32 [4, 1024, 16, 128], P('dp', None, 'tp'), parts along dimension 0
- output 6: float32 [4, 1024, 16, 128], P('dp', None, 'tp'), parts along dimension 0
- output 7: float32 [4, 1024, 16, 128], P('dp', None, 'tp'), parts along dimension 0
- output 8: float32 [4, 16, 128, 1024], P('dp', 'tp'), parts along dimension 0
- output 9: float32 [4, 1024, 3072], P('dp', None, 'tp'), parts along dimension 0
- output 10: float32 [4, 3072, 1024], P('dp', 'tp'), parts along dimension 0
There are 4 independent parts. The reference program is written for one: setup_inputs(seed, part) draws one part's arguments, and reference() takes and returns one part's arrays. A program takes and returns all parts, laid end to end along the dimension named above; an argument that names none is the same for every part.
All inputs are finite; a program needn't handle non-finite values.
Results may differ from the reference program's by a relative error of at most 0.0067854.
Values are sent between devices in bfloat16 or wider.
A program may use at most 768 MiB of HBM per device.

```python
import functools
import jax
import jax.numpy as jnp
from jax import lax

D = 1024
HEADS = 16
KV_HEADS = 8
HEAD = 128
FF = 3072
LAYERS = 1
SEQS = 3
SEQ = 64
TP = 16
KV_SLOTS = max(KV_HEADS, TP)
REPEAT = KV_SLOTS // KV_HEADS
GROUP = HEADS // KV_SLOTS
BATCH = SEQS * TP
TOKENS = BATCH * SEQ
EPS = 1e-5
SCORE_SCALE = HEAD ** -0.5
OUT_GAIN = 0.5 * (SEQ / 64) ** 0.25


def normal_weights(rng_key, arr_shape, scale_std):
    return (jax.random.normal(rng_key, arr_shape, jnp.float32) * scale_std).astype(jnp.bfloat16)


def draw_lengths(rng_key):
    len_key, top_key, low_key = jax.random.split(rng_key, 3)
    seq_lens = jax.random.randint(len_key, (BATCH,), SEQ // 4, SEQ + 1)
    top_idx = jax.random.randint(top_key, (), 0, BATCH)
    low_idx = (top_idx + jax.random.randint(low_key, (), 1, BATCH)) % BATCH
    positions = jnp.arange(BATCH)
    seq_lens = jnp.where(positions == top_idx, SEQ, seq_lens)
    seq_lens = jnp.where(positions == low_idx, SEQ // 4, seq_lens)
    return seq_lens.astype(jnp.int32)


def setup_inputs(seed: int = 0, part: int = 0) -> dict:
    weight_keys = jax.random.split(jax.random.key(seed), 6)
    part_keys = jax.random.split(jax.random.fold_in(jax.random.key(seed + 1), part), 5)
    act_shape = (BATCH, SEQ, D)
    key_heads = normal_weights(weight_keys[1], (LAYERS, D, KV_HEADS, HEAD), D ** -0.5)
    value_heads = normal_weights(weight_keys[2], (LAYERS, D, KV_HEADS, HEAD), D ** -0.5)
    return {
        'y_one': jax.random.normal(part_keys[0], act_shape, jnp.float32),
        'y_two': jax.random.normal(part_keys[1], act_shape, jnp.float32),
        'dy_one': jax.random.normal(part_keys[2], act_shape, jnp.float32),
        'dy_two': jax.random.normal(part_keys[3], act_shape, jnp.float32),
        'seq_lens': draw_lengths(part_keys[4]),
        'w_query': normal_weights(weight_keys[0], (LAYERS, D, HEADS, HEAD), 2.0 * D ** -0.5),
        'w_key': jnp.repeat(key_heads, REPEAT, axis=2),
        'w_value': jnp.repeat(value_heads, REPEAT, axis=2),
        'w_out': normal_weights(weight_keys[3], (LAYERS, HEADS, HEAD, D), OUT_GAIN * (HEADS * HEAD) ** -0.5),
        'w_up': normal_weights(weight_keys[4], (LAYERS, D, FF), D ** -0.5),
        'w_down': normal_weights(weight_keys[5], (LAYERS, FF, D), 0.6 * FF ** -0.5),
    }


def rms_norm(x_val):
    inv_rms = lax.rsqrt(jnp.mean(x_val * x_val, axis=-1, keepdims=True) + EPS)
    return x_val * inv_rms, inv_rms


def rms_back(normed, inv_rms, grad_norm):
    return inv_rms * (grad_norm - normed * jnp.mean(grad_norm * normed, axis=-1, keepdims=True))


def attend_seq(operands):
    q_seq, k_seq, v_seq, dout_seq, seq_len = operands
    q_grp = q_seq.reshape(SEQ, KV_SLOTS, GROUP, HEAD).astype(jnp.float32)
    k_full = k_seq.astype(jnp.float32)
    v_full = v_seq.astype(jnp.float32)
    dout_grp = dout_seq.reshape(SEQ, KV_SLOTS, GROUP, HEAD).astype(jnp.float32)
    row_pos = jnp.arange(SEQ)[:, None]
    col_pos = jnp.arange(SEQ)[None, :]
    visible = (col_pos <= row_pos) & (col_pos < seq_len)
    scores = jnp.einsum('igre,jge->grij', q_grp, k_full) * SCORE_SCALE
    scores = jnp.where(visible, scores, -1e30)
    attn_probs = jax.nn.softmax(scores, axis=-1)
    probs_b = attn_probs.astype(jnp.bfloat16).astype(jnp.float32)
    attn_out = jnp.einsum('grij,jge->igre', probs_b, v_full).astype(jnp.bfloat16)
    d_value = jnp.einsum('grij,igre->jge', probs_b, dout_grp).astype(jnp.bfloat16)
    d_probs = jnp.einsum('igre,jge->grij', dout_grp, v_full)
    d_scores = attn_probs * (d_probs - jnp.sum(d_probs * attn_probs, axis=-1, keepdims=True)) * SCORE_SCALE
    d_scores = d_scores.astype(jnp.bfloat16).astype(jnp.float32)
    d_query = jnp.einsum('grij,jge->igre', d_scores, k_full).astype(jnp.bfloat16)
    d_key = jnp.einsum('grij,igre->jge', d_scores, q_grp).astype(jnp.bfloat16)
    return attn_out.reshape(SEQ, HEADS, HEAD), d_query.reshape(SEQ, HEADS, HEAD), d_key, d_value


def layer_back(seq_lens, carry, layer_w):
    y_one, y_two, dy_one, dy_two = carry
    w_query, w_key, w_value, w_out, w_up, w_down = layer_w
    norm_g, inv_g = rms_norm(y_one.reshape(TOKENS, D))
    norm_g_b = norm_g.astype(jnp.bfloat16)
    pre_act = jnp.dot(norm_g_b, w_up, preferred_element_type=jnp.float32)
    act_val, gelu_back = jax.vjp(jax.nn.gelu, pre_act)
    act_b = act_val.astype(jnp.bfloat16)
    g_branch = jnp.dot(act_b, w_down, preferred_element_type=jnp.float32)
    x_two = y_two - g_branch.reshape(BATCH, SEQ, D)
    dy2_b = dy_two.reshape(TOKENS, D).astype(jnp.bfloat16)
    d_act = jnp.dot(dy2_b, w_down.T, preferred_element_type=jnp.float32)
    d_pre = gelu_back(d_act)[0].astype(jnp.bfloat16)
    dw_down = jnp.dot(act_b.T, dy2_b, preferred_element_type=jnp.float32)
    dw_up = jnp.dot(norm_g_b.T, d_pre, preferred_element_type=jnp.float32)
    grad_norm_g = jnp.dot(d_pre, w_up.T, preferred_element_type=jnp.float32)
    dy_one = dy_one + rms_back(norm_g, inv_g, grad_norm_g).reshape(BATCH, SEQ, D)

    norm_f, inv_f = rms_norm(x_two.reshape(TOKENS, D))
    norm_f_b = norm_f.astype(jnp.bfloat16)
    wq_flat = w_query.reshape(D, HEADS * HEAD)
    wk_flat = w_key.reshape(D, KV_SLOTS * HEAD)
    wv_flat = w_value.reshape(D, KV_SLOTS * HEAD)
    wo_flat = w_out.reshape(HEADS * HEAD, D)
    q_all = jnp.dot(norm_f_b, wq_flat, preferred_element_type=jnp.float32).astype(jnp.bfloat16).reshape(BATCH, SEQ, HEADS, HEAD)
    k_all = jnp.dot(norm_f_b, wk_flat, preferred_element_type=jnp.float32).astype(jnp.bfloat16).reshape(BATCH, SEQ, KV_SLOTS, HEAD)
    v_all = jnp.dot(norm_f_b, wv_flat, preferred_element_type=jnp.float32).astype(jnp.bfloat16).reshape(BATCH, SEQ, KV_SLOTS, HEAD)
    dy1_b = dy_one.reshape(TOKENS, D).astype(jnp.bfloat16)
    d_attn = jnp.dot(dy1_b, wo_flat.T, preferred_element_type=jnp.float32).astype(jnp.bfloat16).reshape(BATCH, SEQ, HEADS, HEAD)
    attn_out, d_query, d_key, d_value = lax.map(attend_seq, (q_all, k_all, v_all, d_attn, seq_lens))
    out_flat = attn_out.reshape(TOKENS, HEADS * HEAD)
    f_branch = jnp.dot(out_flat, wo_flat, preferred_element_type=jnp.float32)
    x_one = y_one - f_branch.reshape(BATCH, SEQ, D)
    dw_out = jnp.dot(out_flat.T, dy1_b, preferred_element_type=jnp.float32).reshape(HEADS, HEAD, D)
    dq_flat = d_query.reshape(TOKENS, HEADS * HEAD)
    dk_flat = d_key.reshape(TOKENS, KV_SLOTS * HEAD)
    dv_flat = d_value.reshape(TOKENS, KV_SLOTS * HEAD)
    dw_query = jnp.dot(norm_f_b.T, dq_flat, preferred_element_type=jnp.float32).reshape(D, HEADS, HEAD)
    dw_key = jnp.dot(norm_f_b.T, dk_flat, preferred_element_type=jnp.float32).reshape(D, KV_SLOTS, HEAD)
    dw_value = jnp.dot(norm_f_b.T, dv_flat, preferred_element_type=jnp.float32).reshape(D, KV_SLOTS, HEAD)
    grad_norm_f = (jnp.dot(dq_flat, wq_flat.T, preferred_element_type=jnp.float32)
                   + jnp.dot(dk_flat, wk_flat.T, preferred_element_type=jnp.float32)
                   + jnp.dot(dv_flat, wv_flat.T, preferred_element_type=jnp.float32))
    dx_two = dy_two + rms_back(norm_f, inv_f, grad_norm_f).reshape(BATCH, SEQ, D)
    return (x_one, x_two, dy_one, dx_two), (dw_query, dw_key, dw_value, dw_out, dw_up, dw_down)


def reference(y_one, y_two, dy_one, dy_two, seq_lens, w_query, w_key, w_value, w_out, w_up, w_down):
    end_state, layer_grads = lax.scan(functools.partial(layer_back, seq_lens), (y_one, y_two, dy_one, dy_two), (w_query, w_key, w_value, w_out, w_up, w_down), reverse=True)
    return (end_state[0], end_state[1], end_state[2], end_state[3], layer_grads[0], layer_grads[1], layer_grads[2], layer_grads[3], layer_grads[4], layer_grads[5])
```

```python
import jax
import jax.numpy as jnp
from jax import lax
from jax.sharding import PartitionSpec as P

F32 = jnp.float32
BF16 = jnp.bfloat16
EPS = 1e-5
MASK_VALUE = -1e30


def rms_norm(x_val):
    inv_rms = lax.rsqrt(jnp.mean(x_val * x_val, axis=-1, keepdims=True) + EPS)
    return x_val * inv_rms, inv_rms


def rms_back(normed, inv_rms, grad_norm):
    return inv_rms * (grad_norm - normed * jnp.mean(grad_norm * normed, axis=-1, keepdims=True))


def visible_mask(seq_lens, seq_len):
    row_pos = lax.broadcasted_iota(jnp.int32, (seq_len, seq_len), 0)
    col_pos = lax.broadcasted_iota(jnp.int32, (seq_len, seq_len), 1)
    causal = (col_pos <= row_pos)[None, None]
    in_length = col_pos[None, None] < seq_lens[:, None, None, None]
    return causal & in_length


def dot(spec, a, b):
    return jnp.einsum(spec, a, b, preferred_element_type=F32)


def block_back(carry, seq_lens, layer_w, tp_idx):
    y_one, y_two, dy_one, dy_two = carry
    own_q, own_k, own_v, own_o, own_up, own_down = layer_w
    seq_len = y_one.shape[1]
    head_dim = own_q.shape[2]
    score_scale = head_dim ** -0.5

    def gathered(w, axis):
        full = lax.all_gather(w, 'tp', axis=axis, tiled=True)
        size = w.shape[axis]
        return jnp.roll(full, -tp_idx * size, axis=axis)

    w_up, w_down = gathered(own_up, 1), gathered(own_down, 0)
    w_query, w_key, w_value, w_out = gathered(own_q, 1), gathered(own_k, 1), gathered(own_v, 1), gathered(own_o, 0)
    own_ff = own_up.shape[1]

    norm_g, inv_g = rms_norm(y_one)
    norm_g_b = norm_g.astype(BF16)
    pre_act = dot('bsd,df->bsf', norm_g_b, w_up)
    act_val, gelu_back = jax.vjp(jax.nn.gelu, pre_act)
    act_b = act_val.astype(BF16)
    x_two = y_two - dot('bsf,fd->bsd', act_b, w_down)
    dy2_b = dy_two.astype(BF16)
    d_act = dot('bsd,fd->bsf', dy2_b, w_down)
    d_pre = gelu_back(d_act)[0].astype(BF16)
    dw_down = dot('bsf,bsd->fd', act_b[..., :own_ff], dy2_b)
    dw_up = dot('bsd,bsf->df', norm_g_b, d_pre[..., :own_ff])
    grad_norm_g = dot('bsf,df->bsd', d_pre, w_up)
    dy_one = dy_one + rms_back(norm_g, inv_g, grad_norm_g)

    norm_f, inv_f = rms_norm(x_two)
    norm_f_b = norm_f.astype(BF16)
    query = dot('bsd,dhe->bshe', norm_f_b, w_query).astype(BF16)
    key = dot('bsd,dhe->bshe', norm_f_b, w_key).astype(BF16)
    value = dot('bsd,dhe->bshe', norm_f_b, w_value).astype(BF16)
    scores = dot('bihe,bjhe->bhij', query, key) * score_scale
    scores = jnp.where(visible_mask(seq_lens, seq_len), scores, MASK_VALUE)
    probs = jax.nn.softmax(scores, axis=-1)
    probs_b = probs.astype(BF16)
    attn = dot('bhij,bjhe->bihe', probs_b, value).astype(BF16)
    x_one = y_one - dot('bihe,hed->bid', attn, w_out)
    dy1_b = dy_one.astype(BF16)
    dw_out = dot('bihe,bid->hed', attn[:, :, :1], dy1_b)
    d_attn = dot('bid,hed->bihe', dy1_b, w_out).astype(BF16)
    d_value = dot('bhij,bihe->bjhe', probs_b, d_attn).astype(BF16)
    d_probs = dot('bihe,bjhe->bhij', d_attn, value)
    d_scores = (probs * (d_probs - jnp.sum(d_probs * probs, axis=-1, keepdims=True)) * score_scale).astype(BF16)
    d_query = dot('bhij,bjhe->bihe', d_scores, key).astype(BF16)
    d_key = dot('bhij,bihe->bjhe', d_scores, query).astype(BF16)
    dw_query = dot('bsd,bshe->dhe', norm_f_b, d_query[:, :, :1])
    dw_key = dot('bsd,bshe->dhe', norm_f_b, d_key[:, :, :1])
    dw_value = dot('bsd,bshe->dhe', norm_f_b, d_value[:, :, :1])
    grad_norm_f = (dot('bshe,dhe->bsd', d_query, w_query) + dot('bshe,dhe->bsd', d_key, w_key)
                   + dot('bshe,dhe->bsd', d_value, w_value))
    dx_two = dy_two + rms_back(norm_f, inv_f, grad_norm_f)
    return (x_one, x_two, dy_one, dx_two), (dw_query, dw_key, dw_value, dw_out, dw_up, dw_down)


def stack_grads(grads_by_layer):
    return tuple(jnp.stack([layer_grads[grad_pos] for layer_grads in grads_by_layer]) for grad_pos in range(6))


def solution(mesh):
    act_spec = P('dp', None, None)
    w_specs = (P(None, None, 'tp', None), P(None, None, 'tp', None), P(None, None, 'tp', None),
               P(None, 'tp', None, None), P(None, None, 'tp'), P(None, 'tp', None))
    g_specs = (P('dp', None, 'tp', None), P('dp', None, 'tp', None), P('dp', None, 'tp', None),
               P('dp', 'tp', None, None), P('dp', None, 'tp'), P('dp', 'tp', None))

    def local_fn(y_one, y_two, dy_one, dy_two, seq_lens, w_query, w_key, w_value, w_out, w_up, w_down):
        weights = (w_query, w_key, w_value, w_out, w_up, w_down)
        carry = (y_one, y_two, dy_one, dy_two)
        n_layers = w_query.shape[0]
        tp_idx = lax.axis_index('tp')
        grads_by_layer = [None] * n_layers
        for layer_idx in reversed(range(n_layers)):
            layer_w = tuple(w_stack[layer_idx] for w_stack in weights)
            carry, grads_by_layer[layer_idx] = block_back(carry, seq_lens, layer_w, tp_idx)
        return carry + stack_grads(grads_by_layer)

    return jax.shard_map(local_fn, mesh=mesh,
                         in_specs=(act_spec,) * 4 + (P('dp'),) + w_specs,
                         out_specs=(act_spec,) * 4 + g_specs,
                         check_vma=False)
```

```python
import functools

import jax
import jax.numpy as jnp
from jax import lax
from jax.experimental import pallas as pl
from jax.experimental.pallas import tpu as pltpu
from jax.sharding import PartitionSpec as P

F32 = jnp.float32
BF16 = jnp.bfloat16
EPS = 1e-5
MASK_VALUE = -1e30
CORES = 2
GELU_A = 0.7978845608028654
GELU_B = 0.044715


def dot_nt(a, b):
    return lax.dot_general(a, b, (((1,), (1,)), ((), ())), preferred_element_type=F32)


def dot_nn(a, b):
    return lax.dot_general(a, b, (((1,), (0,)), ((), ())), preferred_element_type=F32)


def dot_tn(a, b):
    return lax.dot_general(a, b, (((0,), (0,)), ((), ())), preferred_element_type=F32)


def gelu_and_slope(x):
    sq = x * x
    t = jnp.tanh(GELU_A * (x + GELU_B * (sq * x)))
    half = 0.5 * (1.0 + t)
    slope = half + (0.5 * x) * (1.0 - t * t) * (GELU_A * (1.0 + (3.0 * GELU_B) * sq))
    return x * half, slope


def inv_rms_of(x):
    return lax.rsqrt(jnp.mean(x * x, axis=-1, keepdims=True) + EPS)


class Ring:
    def __init__(self, n_tp):
        self.chips = n_tp // CORES
        me = lax.axis_index('tp')
        self.core = lax.rem(me, CORES)
        chip = lax.div(me, CORES)
        up = lax.rem(chip + 1, self.chips) * CORES + self.core
        down = lax.rem(chip + self.chips - 1, self.chips) * CORES + self.core
        self.toward = (up, down)
        self.sibling = chip * CORES + (1 - self.core)
        self.far = self.chips // 2

    def slot(self, hop, way):
        return 2 * hop - 1 if hop == self.far else 2 * hop - 1 + way

    def rows(self, slot, size):
        return pl.ds(pl.multiple_of((slot * CORES + self.core) * size, 16), size)


def remote(src, dst, send, recv, tp):
    return pltpu.make_async_remote_copy(src_ref=src, dst_ref=dst, send_sem=send, recv_sem=recv,
                                        device_id={'tp': tp}, device_id_type=pl.DeviceIdType.MESH)


def entry_barrier(ring):
    barrier = pltpu.get_barrier_semaphore()
    for peer in (*ring.toward, ring.sibling):
        pl.semaphore_signal(barrier, inc=1, device_id={'tp': peer}, device_id_type=pl.DeviceIdType.MESH)
    pl.semaphore_wait(barrier, 3)


def mlp_kernel(n_tp, tile, y1, y2, dy1, dy2, w1_own, w2_own, x2, dx1, dw1, dw2,
               w1, w2, n1, e, acc_g, acc_d, part, from_sib, in_a, in_b, in_c, out_a, out_b,
               own_sem, ring_send, ring_recv, d2d_send, d2d_recv, in_sem, out_sem, sib_send, sib_recv, dw_send, dw_recv,
               dw_sem):
    ring = Ring(n_tp)
    far = ring.far
    size = w1_own.shape[0]
    rows_own = n1.shape[0]
    base = ring.core * rows_own
    own_w, all_w = (w1_own, w2_own), (w1, w2)
    entry_barrier(ring)

    def ring_copy(mat, way, hop):
        src = own_w[mat] if hop == 1 else all_w[mat].at[ring.rows(ring.slot(hop - 1, way), size)]
        return remote(src, all_w[mat].at[ring.rows(ring.slot(hop, way), size)],
                      ring_send.at[mat, way, hop - 1], ring_recv.at[mat, way, hop - 1], ring.toward[way])

    def has_hop(mat, way, hop):
        return hop < far or (hop == far and mat == way)

    def d2d_copy(mat, slot):
        src = own_w[mat] if slot == 0 else all_w[mat].at[ring.rows(slot, size)]
        return remote(src, all_w[mat].at[ring.rows(slot, size)], d2d_send.at[mat, slot], d2d_recv.at[mat, slot], ring.sibling)

    def own_copy(mat):
        return pltpu.make_async_copy(own_w[mat], all_w[mat].at[ring.rows(0, size)], own_sem.at[mat])

    for mat in range(2):
        for way in range(2):
            ring_copy(mat, way, 1).start()
    for mat in range(2):
        own_copy(mat).start()
        d2d_copy(mat, 0).start()

    n_tiles = rows_own // tile

    def hbm_tile(ref, t):
        return ref.at[pl.ds(pl.multiple_of(base + t * tile, 16), tile)]

    def fetch(src, dst, which, t, slot):
        return pltpu.make_async_copy(hbm_tile(src, t), dst.at[slot], in_sem.at[which, slot])

    def start_norm(t, slot):
        fetch(y1, in_a, 0, t, slot).start()
        fetch(dy2, in_b, 1, t, slot).start()

    start_norm(0, 0)

    def norm_body(t, _):
        slot = lax.rem(t, 2)

        @pl.when(t + 1 < n_tiles)
        def _():
            start_norm(t + 1, 1 - slot)

        fetch(y1, in_a, 0, t, slot).wait()
        fetch(dy2, in_b, 1, t, slot).wait()
        here = pl.ds(pl.multiple_of(t * tile, 16), tile)
        y = in_a[slot]
        n1[here, :] = (y * inv_rms_of(y)).astype(BF16)
        e[here, :] = in_b[slot].astype(BF16)
        return 0

    lax.fori_loop(0, n_tiles, norm_body, 0)

    def products(here, first_row, width):
        cols = pl.ds(first_row, width)
        pre = dot_nt(n1[here, :], w1[cols, :])
        d_act = dot_nt(e[here, :], w2[cols, :])
        act, slope = gelu_and_slope(pre)
        return act.astype(BF16), (d_act * slope).astype(BF16)

    for mat in range(2):
        own_copy(mat).wait()
        d2d_copy(mat, 0).wait_recv()
    big = 2 * tile
    width = CORES * size
    part[...] = jnp.zeros_like(part)

    def own_body(t, _):
        here = pl.ds(pl.multiple_of(t * big, 16), big)
        act, d_pre = products(here, 0, width)
        acc_g[here, :] = dot_nn(act, w2[0:width, :])
        acc_d[here, :] = dot_nn(d_pre, w1[0:width, :])
        part[0] += dot_tn(d_pre, n1[here, :])
        part[1] += dot_tn(act, e[here, :])
        return 0

    lax.fori_loop(0, rows_own // big, own_body, 0)

    def dw_copy(mat):
        return remote(part.at[mat, pl.ds(pl.multiple_of((1 - ring.core) * size, 16), size)], from_sib.at[mat],
                      dw_send.at[mat], dw_recv.at[mat], ring.sibling)

    def pass_on(hop):
        for mat in range(2):
            for way in range(2):
                if has_hop(mat, way, hop):
                    ring_copy(mat, way, hop).wait_recv()
                    if has_hop(mat, way, hop + 1):
                        ring_copy(mat, way, hop + 1).start()
                    d2d_copy(mat, ring.slot(hop, way)).start()
        for mat in range(2):
            for way in range(2):
                if has_hop(mat, way, hop):
                    d2d_copy(mat, ring.slot(hop, way)).wait_recv()

    for hop in range(1, far):
        pass_on(hop)
        first_row = ring.slot(hop, 0) * width

        def pair_body(t, _):
            here = pl.ds(pl.multiple_of(t * big, 16), big)
            act, d_pre = products(here, first_row, 2 * width)
            cols = pl.ds(first_row, 2 * width)
            acc_g[here, :] += dot_nn(act, w2[cols, :])
            acc_d[here, :] += dot_nn(d_pre, w1[cols, :])
            return 0

        lax.fori_loop(0, rows_own // big, pair_body, 0)
        if hop == 1:
            for mat in range(2):
                dw_copy(mat).start()

    def start_last(t, slot):
        for which, (src, dst) in enumerate(((y1, in_a), (y2, in_b), (dy1, in_c))):
            fetch(src, dst, which, t, slot).start()

    start_last(0, 0)
    pass_on(far)
    outs = ((out_a, x2), (out_b, dx1))

    def out_copy(which, t, slot):
        src, dst = outs[which]
        return pltpu.make_async_copy(src.at[slot], hbm_tile(dst, t), out_sem.at[which, slot])

    def sib_copy(which, t, slot):
        src, dst = outs[which]
        return remote(src.at[slot], hbm_tile(dst, t), sib_send.at[which, slot], sib_recv.at[which, t], ring.sibling)

    far_row = ring.slot(far, 0) * width

    def last_body(t, _):
        slot = lax.rem(t, 2)
        here = pl.ds(pl.multiple_of(t * tile, 16), tile)

        @pl.when(t + 1 < n_tiles)
        def _():
            start_last(t + 1, 1 - slot)

        @pl.when(t >= 2)
        def _():
            for which in range(2):
                out_copy(which, t - 2, slot).wait()
                sib_copy(which, t - 2, slot).wait_send()

        act, d_pre = products(here, far_row, width)
        cols = pl.ds(far_row, width)
        total_g = acc_g[here, :] + dot_nn(act, w2[cols, :])
        total_d = acc_d[here, :] + dot_nn(d_pre, w1[cols, :])
        for which, (src, dst) in enumerate(((y1, in_a), (y2, in_b), (dy1, in_c))):
            fetch(src, dst, which, t, slot).wait()
        y = in_a[slot]
        inv = inv_rms_of(y)
        normed = y * inv
        out_a[slot] = in_b[slot] - total_g
        out_b[slot] = in_c[slot] + inv * (total_d - normed * jnp.mean(total_d * normed, axis=-1, keepdims=True))
        for which in range(2):
            out_copy(which, t, slot).start()
            sib_copy(which, t, slot).start()
        return 0

    lax.fori_loop(0, n_tiles, last_body, 0)

    for mat, dst in enumerate((dw1, dw2)):
        dw_copy(mat).wait_recv()
        mine = pl.ds(pl.multiple_of(ring.core * size, 16), size)
        from_sib[mat] = from_sib[mat] + part[mat, mine, :]
        pltpu.make_async_copy(from_sib.at[mat], dst, dw_sem.at[mat]).start()

    for mat, dst in enumerate((dw1, dw2)):
        pltpu.make_async_copy(from_sib.at[mat], dst, dw_sem.at[mat]).wait()
        dw_copy(mat).wait_send()
        for way in range(2):
            for hop in range(1, far + 1):
                if has_hop(mat, way, hop):
                    ring_copy(mat, way, hop).wait_send()
        for slot in range(ring.chips):
            d2d_copy(mat, slot).wait_send()
    for t in range(max(n_tiles - 2, 0), n_tiles):
        for which in range(2):
            out_copy(which, t, t % 2).wait()
            sib_copy(which, t, t % 2).wait_send()
    for t in range(n_tiles):
        for which in range(2):
            sib_copy(which, t, t % 2).wait_recv()


def mlp_back(n_tp, y1, y2, dy1, dy2, w1_own, w2_own, tile=256):
    tokens, d = y1.shape
    size = w1_own.shape[0]
    chips = n_tp // CORES
    half = tokens // CORES
    n_tiles = half // tile
    hidden = n_tp * size
    hbm = pl.BlockSpec(memory_space=pl.ANY)
    dma = pltpu.SemaphoreType.DMA
    flops = 8 * half * d * hidden
    return pl.pallas_call(
        functools.partial(mlp_kernel, n_tp, tile),
        name='mlp_back',
        out_shape=[jax.ShapeDtypeStruct((tokens, d), F32)] * 2 + [jax.ShapeDtypeStruct((size, d), F32)] * 2,
        in_specs=[hbm] * 6,
        out_specs=[hbm] * 4,
        scratch_shapes=[
            pltpu.VMEM((hidden, d), BF16), pltpu.VMEM((hidden, d), BF16),
            pltpu.VMEM((half, d), BF16), pltpu.VMEM((half, d), BF16),
            pltpu.VMEM((half, d), F32), pltpu.VMEM((half, d), F32),
            pltpu.VMEM((2, CORES * size, d), F32), pltpu.VMEM((2, size, d), F32),
            pltpu.VMEM((2, tile, d), F32), pltpu.VMEM((2, tile, d), F32), pltpu.VMEM((2, tile, d), F32),
            pltpu.VMEM((2, tile, d), F32), pltpu.VMEM((2, tile, d), F32),
            dma((2,)), dma((2, 2, chips // 2)), dma((2, 2, chips // 2)), dma((2, chips)), dma((2, chips)),
            dma((3, 2)), dma((2, 2)), dma((2, 2)), dma((2, n_tiles)), dma((2,)), dma((2,)), dma((2,)),
        ],
        compiler_params=pltpu.CompilerParams(collective_id=0, has_side_effects=True, vmem_limit_bytes=60 * 2 ** 20),
        cost_estimate=pl.CostEstimate(flops=flops, bytes_accessed=8 * tokens * d * 4, transcendentals=half * hidden),
    )(y1, y2, dy1, dy2, w1_own, w2_own)


def rms_norm(x_val):
    inv_rms = lax.rsqrt(jnp.mean(x_val * x_val, axis=-1, keepdims=True) + EPS)
    return x_val * inv_rms, inv_rms


def rms_back(normed, inv_rms, grad_norm):
    return inv_rms * (grad_norm - normed * jnp.mean(grad_norm * normed, axis=-1, keepdims=True))


def visible_mask(seq_lens, seq_len):
    row_pos = lax.broadcasted_iota(jnp.int32, (seq_len, seq_len), 0)
    col_pos = lax.broadcasted_iota(jnp.int32, (seq_len, seq_len), 1)
    causal = (col_pos <= row_pos)[None, None]
    in_length = col_pos[None, None] < seq_lens[:, None, None, None]
    return causal & in_length


def dot(spec, a, b):
    return jnp.einsum(spec, a, b, preferred_element_type=F32)


def block_back(carry, seq_lens, layer_w, tp_idx, n_tp):
    y_one, y_two, dy_one, dy_two = carry
    own_q, own_k, own_v, own_o, own_up, own_down = layer_w
    seq_len = y_one.shape[1]
    head_dim = own_q.shape[2]
    score_scale = head_dim ** -0.5

    def gathered(w, axis):
        full = lax.all_gather(w, 'tp', axis=axis, tiled=True)
        size = w.shape[axis]
        return jnp.roll(full, -tp_idx * size, axis=axis)

    w_query, w_key, w_value, w_out = gathered(own_q, 1), gathered(own_k, 1), gathered(own_v, 1), gathered(own_o, 0)
    flat = (-1, y_one.shape[-1])
    x_two, dy_one, dw_up, dw_down = mlp_back(n_tp, y_one.reshape(flat), y_two.reshape(flat), dy_one.reshape(flat),
                                             dy_two.reshape(flat), own_up.T, own_down)
    x_two, dy_one, dw_up = x_two.reshape(y_one.shape), dy_one.reshape(y_one.shape), dw_up.T

    norm_f, inv_f = rms_norm(x_two)
    norm_f_b = norm_f.astype(BF16)
    query = dot('bsd,dhe->bshe', norm_f_b, w_query).astype(BF16)
    key = dot('bsd,dhe->bshe', norm_f_b, w_key).astype(BF16)
    value = dot('bsd,dhe->bshe', norm_f_b, w_value).astype(BF16)
    scores = dot('bihe,bjhe->bhij', query, key) * score_scale
    scores = jnp.where(visible_mask(seq_lens, seq_len), scores, MASK_VALUE)
    probs = jax.nn.softmax(scores, axis=-1)
    probs_b = probs.astype(BF16)
    attn = dot('bhij,bjhe->bihe', probs_b, value).astype(BF16)
    x_one = y_one - dot('bihe,hed->bid', attn, w_out)
    dy1_b = dy_one.astype(BF16)
    dw_out = dot('bihe,bid->hed', attn[:, :, :1], dy1_b)
    d_attn = dot('bid,hed->bihe', dy1_b, w_out).astype(BF16)
    d_value = dot('bhij,bihe->bjhe', probs_b, d_attn).astype(BF16)
    d_probs = dot('bihe,bjhe->bhij', d_attn, value)
    d_scores = (probs * (d_probs - jnp.sum(d_probs * probs, axis=-1, keepdims=True)) * score_scale).astype(BF16)
    d_query = dot('bhij,bjhe->bihe', d_scores, key).astype(BF16)
    d_key = dot('bhij,bihe->bjhe', d_scores, query).astype(BF16)
    dw_query = dot('bsd,bshe->dhe', norm_f_b, d_query[:, :, :1])
    dw_key = dot('bsd,bshe->dhe', norm_f_b, d_key[:, :, :1])
    dw_value = dot('bsd,bshe->dhe', norm_f_b, d_value[:, :, :1])
    grad_norm_f = (dot('bshe,dhe->bsd', d_query, w_query) + dot('bshe,dhe->bsd', d_key, w_key)
                   + dot('bshe,dhe->bsd', d_value, w_value))
    dx_two = dy_two + rms_back(norm_f, inv_f, grad_norm_f)
    return (x_one, x_two, dy_one, dx_two), (dw_query, dw_key, dw_value, dw_out, dw_up, dw_down)


def stack_grads(grads_by_layer):
    return tuple(jnp.stack([layer_grads[grad_pos] for layer_grads in grads_by_layer]) for grad_pos in range(6))


def solution(mesh):
    act_spec = P('dp', None, None)
    w_specs = (P(None, None, 'tp', None), P(None, None, 'tp', None), P(None, None, 'tp', None),
               P(None, 'tp', None, None), P(None, None, 'tp'), P(None, 'tp', None))
    g_specs = (P('dp', None, 'tp', None), P('dp', None, 'tp', None), P('dp', None, 'tp', None),
               P('dp', 'tp', None, None), P('dp', None, 'tp'), P('dp', 'tp', None))

    def local_fn(y_one, y_two, dy_one, dy_two, seq_lens, w_query, w_key, w_value, w_out, w_up, w_down):
        weights = (w_query, w_key, w_value, w_out, w_up, w_down)
        carry = (y_one, y_two, dy_one, dy_two)
        n_layers = w_query.shape[0]
        tp_idx = lax.axis_index('tp')
        grads_by_layer = [None] * n_layers
        for layer_idx in reversed(range(n_layers)):
            layer_w = tuple(w_stack[layer_idx] for w_stack in weights)
            carry, grads_by_layer[layer_idx] = block_back(carry, seq_lens, layer_w, tp_idx, mesh.shape['tp'])
        return carry + stack_grads(grads_by_layer)

    return jax.shard_map(local_fn, mesh=mesh,
                         in_specs=(act_spec,) * 4 + (P('dp'),) + w_specs,
                         out_specs=(act_spec,) * 4 + g_specs,
                         check_vma=False)
```

```python
import functools

import jax
import jax.numpy as jnp
from jax import lax
from jax.experimental import pallas as pl
from jax.experimental.pallas import tpu as pltpu
from jax.sharding import PartitionSpec as P

F32 = jnp.float32
BF16 = jnp.bfloat16
EPS = 1e-5
MASK_VALUE = -1e30
CORES = 2
BLOCK = 128
GELU_A = 0.7978845608028654
GELU_B = 0.044715
LOG2_E = 1.4426950408889634


def dot_nt(a, b):
    return lax.dot_general(a, b, (((1,), (1,)), ((), ())), preferred_element_type=F32)


def dot_nn(a, b):
    return lax.dot_general(a, b, (((1,), (0,)), ((), ())), preferred_element_type=F32)


def dot_tn(a, b):
    return lax.dot_general(a, b, (((0,), (0,)), ((), ())), preferred_element_type=F32)


def gelu_and_slope(x):
    sq = x * x
    t = jnp.tanh(GELU_A * (x + GELU_B * (sq * x)))
    half = 0.5 * (1.0 + t)
    slope = half + (0.5 * x) * (1.0 - t * t) * (GELU_A * (1.0 + (3.0 * GELU_B) * sq))
    return x * half, slope


def inv_rms_of(x):
    return lax.rsqrt(jnp.mean(x * x, axis=-1, keepdims=True) + EPS)


def rms_back(x, grad):
    inv = inv_rms_of(x)
    normed = x * inv
    return inv * (grad - normed * jnp.mean(grad * normed, axis=-1, keepdims=True))


def rows_at(start, size):
    return pl.ds(start if isinstance(start, int) else pl.multiple_of(start, 16), size)


def attn_projections(normed, grad, wq, wkv, wo):
    return dot_nt(normed, wq).astype(BF16), dot_nt(normed, wkv).astype(BF16), dot_nt(grad, wo).astype(BF16)


def attn_scores(span, hd, proj):
    q, kv, da = proj
    out = []
    for first in range(0, span, BLOCK):
        r = slice(first, first + BLOCK)
        q_two = jnp.concatenate([q[r, :hd], q[r, hd:]], axis=0)
        da_two = jnp.concatenate([da[r, :hd], da[r, hd:]], axis=0)
        out.append((dot_nt(q_two, kv[r, :hd]), dot_nt(da_two, kv[r, hd:])))
    return out


def attn_softmax(hd, scores, masks):
    scale = hd ** -0.5
    out = []
    for (s, dp), mask in zip(scores, masks):
        s = jnp.where(jnp.concatenate([mask, mask], axis=0), s, MASK_VALUE)
        ex = jnp.exp2((s - jnp.max(s, axis=-1, keepdims=True)) * (scale * LOG2_E))
        p = ex * (1.0 / jnp.sum(ex, axis=-1, keepdims=True))
        ds = (p * (dp - jnp.sum(dp * p, axis=-1, keepdims=True)) * scale).astype(BF16)
        out.append((p.astype(BF16), ds))
    return out


def attn_grads(span, hd, proj, probs):
    q, kv, da = proj
    a, dq, dkv = [], [], ([], [])
    for first, (p, ds) in zip(range(0, span, BLOCK), probs):
        r = slice(first, first + BLOCK)
        two = dot_nn(p, kv[r, hd:]).astype(BF16)
        a.append(jnp.concatenate([two[:BLOCK], two[BLOCK:]], axis=1))
        two = dot_nn(ds, kv[r, :hd]).astype(BF16)
        dq.append(jnp.concatenate([two[:BLOCK], two[BLOCK:]], axis=1))
        for head in range(CORES):
            own, h = slice(head * BLOCK, (head + 1) * BLOCK), slice(head * hd, (head + 1) * hd)
            dkv[head].append(jnp.concatenate([dot_tn(ds[own], q[r, h]).astype(BF16),
                                              dot_tn(p[own], da[r, h]).astype(BF16)], axis=1))
    return tuple(jnp.concatenate(parts, axis=0) for parts in (a, dq, *dkv))


class Ring:
    def __init__(self, n_tp, paired):
        self.chips = n_tp // CORES
        self.far = self.chips // 2
        me, group = lax.axis_index('tp'), lax.axis_index('dp')
        self.core = lax.rem(me, CORES)
        chip = lax.div(me, CORES)
        up = lax.rem(chip + 1, self.chips) * CORES + self.core
        down = lax.rem(chip + self.chips - 1, self.chips) * CORES + self.core
        self.toward = ({'tp': up}, {'tp': down})
        self.sibling = {'tp': chip * CORES + (1 - self.core)}
        self.paired = paired
        self.parity = lax.rem(group, 2) if paired else 0
        self.partner = {'dp': group + 1 - 2 * self.parity}

    def peers(self):
        return (*self.toward, self.sibling) + ((self.partner,) if self.paired else ())

    def slot(self, hop, way):
        return 2 * hop - 1 if hop == self.far else 2 * hop - 1 + way


def remote(src, dst, send, recv, peer):
    return pltpu.make_async_remote_copy(src_ref=src, dst_ref=dst, send_sem=send, recv_sem=recv,
                                        device_id=peer, device_id_type=pl.DeviceIdType.MESH)


class Shares:
    def __init__(self, ring, pieces, sems):
        self.ring, self.pieces = ring, pieces
        self.send, self.recv, self.pair_send, self.pair_recv, self.d2d_send, self.d2d_recv, self.local = sems

    def lot(self, piece, kind):
        rows, ring_rows = self.pieces[piece][5:7]
        if kind == 'all' or not self.ring.paired:
            return 0, rows
        if kind == 'ring':
            return self.ring.parity * (rows - ring_rows), ring_rows
        return self.ring.parity * ring_rows, rows - ring_rows

    def place(self, piece, slot, kind='all'):
        _, _, full, part, first, *_ = self.pieces[piece]
        low, rows = self.lot(piece, kind)
        return full.at[rows_at((slot * CORES + self.ring.core) * part + first + low, rows)]

    def own(self, piece, kind='all'):
        own, first, *_ = self.pieces[piece]
        if own is None:
            return self.place(piece, 0, kind)
        low, rows = self.lot(piece, kind)
        return own.at[rows_at(first + low, rows)]

    def ways(self, hop):
        return [(piece, way) for piece in range(len(self.pieces)) for way in range(2)
                if hop < self.ring.far or (hop == self.ring.far and self.pieces[piece][-1] == way)]

    def hop_copy(self, piece, way, hop):
        src = self.own(piece, 'ring') if hop == 1 else self.place(piece, self.ring.slot(hop - 1, way), 'ring')
        return remote(src, self.place(piece, self.ring.slot(hop, way), 'ring'), self.send.at[piece, way, hop - 1],
                      self.recv.at[piece, way, hop - 1], self.ring.toward[way])

    def pair_copy(self, piece, slot):
        ref = self.place(piece, slot, 'pair')
        return remote(ref, ref, self.pair_send.at[piece, slot], self.pair_recv.at[piece, slot], self.ring.partner)

    def sibling_copy(self, piece, slot):
        src = self.own(piece) if slot == 0 else self.place(piece, slot)
        return remote(src, self.place(piece, slot), self.d2d_send.at[piece, slot], self.d2d_recv.at[piece, slot],
                      self.ring.sibling)

    def local_copy(self, piece):
        return pltpu.make_async_copy(self.own(piece), self.place(piece, 0), self.local.at[piece])

    def local_pieces(self):
        return [piece for piece in range(len(self.pieces)) if self.pieces[piece][0] is not None]

    def start_local(self):
        for piece in self.local_pieces():
            self.local_copy(piece).start()

    def start(self):
        for piece, way in self.ways(1):
            self.hop_copy(piece, way, 1).start()
        for piece in range(len(self.pieces)):
            self.sibling_copy(piece, 0).start()

    def wait_own(self):
        for piece in self.local_pieces():
            self.local_copy(piece).wait()
        for piece in range(len(self.pieces)):
            self.sibling_copy(piece, 0).wait_recv()

    def take_ring(self, hop):
        later = self.ways(hop + 1)
        for piece, way in self.ways(hop):
            self.hop_copy(piece, way, hop).wait_recv()
            if (piece, way) in later:
                self.hop_copy(piece, way, hop + 1).start()
            if self.ring.paired:
                self.pair_copy(piece, self.ring.slot(hop, way)).start()

    def take_pair(self, hop):
        for piece, way in self.ways(hop):
            if self.ring.paired:
                self.pair_copy(piece, self.ring.slot(hop, way)).wait_recv()
            self.sibling_copy(piece, self.ring.slot(hop, way)).start()

    def take_sibling(self, hop):
        for piece, way in self.ways(hop):
            self.sibling_copy(piece, self.ring.slot(hop, way)).wait_recv()

    def finish(self):
        for hop in range(1, self.ring.far + 1):
            for piece, way in self.ways(hop):
                self.hop_copy(piece, way, hop).wait_send()
                if self.ring.paired:
                    self.pair_copy(piece, self.ring.slot(hop, way)).wait_send()
        for piece in range(len(self.pieces)):
            for slot in range(self.ring.chips):
                self.sibling_copy(piece, slot).wait_send()


def block_kernel(n_tp, paired, tile, big, y1, y2, dy1, dy2, lens, w1_own, w2_own, wq_in, wk_in, wv_in, wo_own,
                 x1, x2, dx1, dx2, dw_mlp, dw_attn,
                 w1, w2, wq, wkv, wo, norm, grad, acc_a, acc_b, part, from_sib, stage, flat_w,
                 mlp_send, mlp_recv, mlp_pair_send, mlp_pair_recv, mlp_d2d_send, mlp_d2d_recv, mlp_local,
                 attn_send, attn_recv, attn_pair_send, attn_pair_recv, attn_d2d_send, attn_d2d_recv, attn_local,
                 norm_sem, stage_sem, out_sem, sib_send, sib_recv, dw_send, dw_recv, dw_sem, flat_sem):
    ring = Ring(n_tp, paired)
    far = ring.far
    size = w1_own.shape[0]
    hd = wo_own.shape[0]
    half_hd = hd // 2
    rows_own = norm.shape[0]
    base = ring.core * rows_own
    n_tiles, n_bigs = rows_own // tile, rows_own // big

    barrier = pltpu.get_barrier_semaphore()
    for peer in ring.peers():
        pl.semaphore_signal(barrier, inc=1, device_id=peer, device_id_type=pl.DeviceIdType.MESH)

    mlp = Shares(ring, ((w1_own, 0, w1, size, 0, size, 2 * size // 3, 0), (w2_own, 0, w2, size, 0, size, 2 * size // 3, 1)),
                 (mlp_send, mlp_recv, mlp_pair_send, mlp_pair_recv, mlp_d2d_send, mlp_d2d_recv, mlp_local))
    attn = Shares(ring, ((None, 0, wq, hd, 0, hd, 5 * hd // 8, 0), (None, 0, wkv, hd, 0, half_hd, 3 * hd // 8, 0),
                         (None, half_hd, wkv, hd, half_hd, half_hd, hd // 4, 1), (wo_own, 0, wo, hd, 0, hd, 5 * hd // 8, 1)),
                  (attn_send, attn_recv, attn_pair_send, attn_pair_recv, attn_d2d_send, attn_d2d_recv, attn_local))

    def hbm_rows(ref, first, rows):
        return ref.at[rows_at(base + first, rows)]

    depth = stage.shape[0]

    def norm_fetch(which, t):
        slot = lax.rem(t, depth)
        return pltpu.make_async_copy(hbm_rows((y1, dy2)[which], t * tile, tile), stage.at[slot, rows_at(which * tile, tile)],
                                     norm_sem.at[which, slot])

    for t in range(min(depth, n_tiles)):
        for which in range(2):
            norm_fetch(which, t).start()

    def flat_copy(which, src):
        return pltpu.make_async_copy(src, flat_w.at[which], flat_sem.at[which])

    flat_copy(0, wq_in).start()

    @pl.when(ring.core == 0)
    def _():
        flat_copy(1, wk_in).start()

    @pl.when(ring.core == 1)
    def _():
        flat_copy(1, wv_in).start()

    mlp.start_local()
    attn.start_local()
    pl.semaphore_wait(barrier, len(ring.peers()))
    mlp.start()

    def norm_body(t, _):
        here = rows_at(t * tile, tile)
        slot = lax.rem(t, depth)
        for which in range(2):
            norm_fetch(which, t).wait()
        y = stage[slot, 0:tile, :]
        norm[here, :] = (y * inv_rms_of(y)).astype(BF16)
        grad[here, :] = stage[slot, tile:2 * tile, :].astype(BF16)

        @pl.when(t + depth < n_tiles)
        def _():
            for which in range(2):
                norm_fetch(which, t + depth).start()

        return 0

    lax.fori_loop(0, n_tiles, norm_body, 0)

    def mlp_hidden(here, cols):
        pre = dot_nt(norm[here, :], w1[cols, :])
        d_act = dot_nt(grad[here, :], w2[cols, :])
        act, slope = gelu_and_slope(pre)
        return act.astype(BF16), (d_act * slope).astype(BF16)

    def serve(shares, t, hop):
        pl.when(t == n_bigs - 2)(lambda: shares.take_ring(hop))
        pl.when(t == n_bigs - 1)(lambda: shares.take_pair(hop))

    width = CORES * size
    mlp.wait_own()
    part[...] = jnp.zeros_like(part)

    def mlp_own(t, _):
        here = rows_at(t * big, big)
        cols = rows_at(0, width)
        act, d_pre = mlp_hidden(here, cols)
        acc_a[here, :] = dot_nn(act, w2[cols, :])
        acc_b[here, :] = dot_nn(d_pre, w1[cols, :])
        part[0:width, :] += dot_tn(d_pre, norm[here, :])
        part[width:2 * width, :] += dot_tn(act, grad[here, :])
        serve(mlp, t, 1)
        return 0

    with jax.named_scope('mlp_own'):
        lax.fori_loop(0, n_bigs, mlp_own, 0)

    eye = (lax.broadcasted_iota(jnp.int32, (hd, hd), 0) == lax.broadcasted_iota(jnp.int32, (hd, hd), 1)).astype(BF16)
    for which, dst in enumerate((wq, wkv)):
        flat_copy(which, wq_in).wait()
        dst[rows_at(ring.core * hd, hd), :] = dot_nt(eye, flat_w[which]).astype(BF16)

    with jax.named_scope('mlp_first_wait'):
        mlp.take_sibling(1)

    def mlp_dw(mat, which):
        core = 1 - ring.core if which else ring.core
        return rows_at(mat * width + core * size, size)

    def mlp_dw_out(mat):
        return pltpu.make_async_copy(from_sib.at[rows_at(mat * size, size)], dw_mlp.at[mat], dw_sem.at[mat])

    def mlp_dw_copy(mat):
        return remote(part.at[mlp_dw(mat, 1)], from_sib.at[rows_at(mat * size, size)], dw_send.at[mat], dw_recv.at[mat],
                      ring.sibling)

    def mlp_pair(hop, _):
        cols = rows_at((2 * hop - 1) * width, 2 * width)

        def body(t, _):
            here = rows_at(t * big, big)
            act, d_pre = mlp_hidden(here, cols)
            acc_a[here, :] += dot_nn(act, w2[cols, :])
            acc_b[here, :] += dot_nn(d_pre, w1[cols, :])
            for h in range(1, far):
                @pl.when((hop == h) & (t == 0))
                def _():
                    mlp.take_ring(h + 1)
                    if h + 1 == far - 1 or far == 2:
                        attn.start()

                @pl.when((hop == h) & (t == n_bigs - 1))
                def _():
                    mlp.take_pair(h + 1)

            return 0

        with jax.named_scope('mlp_pair'):
            lax.fori_loop(0, n_bigs, body, 0)

        @pl.when(hop == 1)
        def _():
            for mat in range(2):
                mlp_dw_copy(mat).start()

        with jax.named_scope('mlp_wait'):
            for h in range(1, far):
                @pl.when(hop == h)
                def _():
                    mlp.take_sibling(h + 1)

        return 0

    lax.fori_loop(1, far, mlp_pair, 0)

    def out_copy(which, ref, src, t):
        return pltpu.make_async_copy(src.at[rows_at(t * big, big)], hbm_rows(ref, t * big, big), out_sem.at[which, t])

    def sib_copy(which, ref, src, t):
        return remote(src.at[rows_at(t * big, big)], hbm_rows(ref, t * big, big), sib_send.at[which, t], sib_recv.at[which, t],
                      ring.sibling)

    def emit(outs, t):
        for which, ref, src in outs:
            out_copy(which, ref, src, t).start()
            sib_copy(which, ref, src, t).start()

    def emitted(outs, t):
        for which, ref, src in outs:
            out_copy(which, ref, src, t).wait()
            sib_copy(which, ref, src, t).wait_send()

    mlp_outs = ((0, x2, acc_a), (1, dx1, acc_b))
    attn_outs = ((2, x1, acc_a), (3, dx2, acc_b))

    def stage_copy(which, src, t):
        return pltpu.make_async_copy(hbm_rows(src, t * big, big), stage.at[which], stage_sem.at[which])

    for mat in range(2):
        mlp_dw_copy(mat).wait_send()
        mlp_dw_copy(mat).wait_recv()
        mine = rows_at(mat * size, size)
        from_sib[mine, :] = from_sib[mine, :] + part[mlp_dw(mat, 0), :]
        mlp_dw_out(mat).start()

    def mlp_last(t, _):
        here = rows_at(t * big, big)
        cols = rows_at((2 * far - 1) * width, width)
        ins = tuple(enumerate((y1, y2, dy1)))
        for which, src in ins:
            stage_copy(which, src, t).start()
        act, d_pre = mlp_hidden(here, cols)
        total_a = acc_a[here, :] + dot_nn(act, w2[cols, :])
        total_b = acc_b[here, :] + dot_nn(d_pre, w1[cols, :])
        for which, src in ins:
            stage_copy(which, src, t).wait()
        x = stage[1] - total_a
        d = stage[2] + rms_back(stage[0], total_b)
        acc_a[here, :] = x
        acc_b[here, :] = d
        norm[here, :] = (x * inv_rms_of(x)).astype(BF16)
        grad[here, :] = d.astype(BF16)
        emit(mlp_outs, t)
        serve(attn, t, 1)
        return 0

    with jax.named_scope('mlp_last'):
        lax.fori_loop(0, n_bigs, mlp_last, 0)

    row_pos = lax.broadcasted_iota(jnp.int32, (BLOCK, BLOCK), 0)
    col_pos = lax.broadcasted_iota(jnp.int32, (BLOCK, BLOCK), 1)
    seq = BLOCK // 2
    causal = (col_pos <= row_pos) & ((col_pos < seq) == (row_pos < seq))
    share = CORES * hd
    first_seq = ring.core * (rows_own // seq)

    def masks_of(t):
        out = []
        for block in range(big // BLOCK):
            at = first_seq + t * (big // seq) + 2 * block
            end = jnp.where(col_pos < seq, lens[at], seq + lens[at + 1])
            out.append(causal & (col_pos < end))
        return out

    def attn_pair(t, j):
        here = rows_at(t * big, big)
        masks = masks_of(t)

        def weights(i):
            r = rows_at((2 * j + i) * share, share)
            return wq[r, :], wkv[r, :], wo[r, :]

        def project(i):
            return attn_projections(norm[here, :], grad[here, :], *weights(i))

        def finish(i, factors):
            q_w, kv_w, o_w = weights(i)
            a, dq, d0, d1 = factors
            return dot_nn(a, o_w), dot_nn(dq, q_w) + dot_nn(d0, kv_w) + dot_nn(d1, kv_w)

        first = project(0)
        scores = attn_scores(big, hd, first)
        second = project(1)
        factors = attn_grads(big, hd, first, attn_softmax(hd, scores, masks))
        scores = attn_scores(big, hd, second)
        f, g = finish(0, factors)
        f2, g2 = finish(1, attn_grads(big, hd, second, attn_softmax(hd, scores, masks)))
        return f + f2, g + g2, factors

    with jax.named_scope('attn_first_wait'):
        attn.wait_own()
        attn.take_sibling(1)
    part[...] = jnp.zeros_like(part)
    own_part = 4 * hd
    for mat in range(2):
        mlp_dw_out(mat).wait()

    def attn_first(t, _):
        here = rows_at(t * big, big)
        f, g, (a, dq, d0, d1) = attn_pair(t, 0)
        for head, dkv in enumerate((d0, d1)):
            cols = slice(head * hd, (head + 1) * hd)
            left = jnp.concatenate([dq[:, cols], dkv], axis=1)
            part[head * own_part:head * own_part + 3 * hd, :] += dot_tn(left, norm[here, :])
            part[head * own_part + 3 * hd:(head + 1) * own_part, :] += dot_tn(a[:, cols], grad[here, :])
        emitted(mlp_outs, t)
        acc_a[here, :] = f
        acc_b[here, :] = g
        serve(attn, t, 2)
        return 0

    with jax.named_scope('attn_first'):
        lax.fori_loop(0, n_bigs, attn_first, 0)
    with jax.named_scope('attn_wait'):
        attn.take_sibling(2)

    def attn_dw(which):
        core = 1 - ring.core if which else ring.core
        return rows_at(core * own_part, own_part)

    def attn_dw_copy():
        return remote(part.at[attn_dw(1)], from_sib.at[rows_at(0, own_part)], dw_send.at[2], dw_recv.at[2], ring.sibling)

    def attn_dw_out():
        return pltpu.make_async_copy(from_sib.at[rows_at(0, own_part)], dw_attn, dw_sem.at[2])

    def attn_middle(j, _):
        def body(t, _):
            here = rows_at(t * big, big)
            f, g, _ = attn_pair(t, j)
            acc_a[here, :] += f
            acc_b[here, :] += g
            for h in range(1, far - 1):
                @pl.when((j == h) & (t == 0))
                def _():
                    attn.take_ring(h + 2)

                @pl.when((j == h) & (t == n_bigs - 1))
                def _():
                    attn.take_pair(h + 2)

            return 0

        with jax.named_scope('attn_pair'):
            lax.fori_loop(0, n_bigs, body, 0)

        @pl.when(j == 1)
        def _():
            attn_dw_copy().start()

        with jax.named_scope('attn_wait'):
            for h in range(1, far - 1):
                @pl.when(j == h)
                def _():
                    attn.take_sibling(h + 2)

        return 0

    lax.fori_loop(1, far - 1, attn_middle, 0)

    attn_dw_copy().wait_send()
    attn_dw_copy().wait_recv()
    mine = rows_at(0, own_part)
    from_sib[mine, :] = from_sib[mine, :] + part[attn_dw(0), :]
    attn_dw_out().start()

    def attn_last(t, _):
        here = rows_at(t * big, big)
        ins = tuple(enumerate((y1, x2, dy2)))
        for which, src in ins:
            stage_copy(which, src, t).start()
        f, g, _ = attn_pair(t, far - 1)
        for which, src in ins:
            stage_copy(which, src, t).wait()
        acc_a[here, :] = stage[0] - (acc_a[here, :] + f)
        acc_b[here, :] = stage[2] + rms_back(stage[1], acc_b[here, :] + g)
        emit(attn_outs, t)
        return 0

    with jax.named_scope('attn_last'):
        lax.fori_loop(0, n_bigs, attn_last, 0)

    mlp.finish()
    attn.finish()
    attn_dw_out().wait()

    def drain(t, _):
        emitted(attn_outs, t)
        for which, ref, src in (*mlp_outs, *attn_outs):
            sib_copy(which, ref, src, t).wait_recv()
        return 0

    with jax.named_scope('drain'):
        lax.fori_loop(0, n_bigs, drain, 0)


def block_back(n_tp, paired, y1, y2, dy1, dy2, lens, w1_own, w2_own, wq_in, wk_in, wv_in, wo_own, tile=256, big=512):
    tokens, d = y1.shape
    size, hd = w1_own.shape[0], wo_own.shape[0]
    chips = n_tp // CORES
    hops = chips // 2
    half = tokens // CORES
    n_bigs = half // big
    hidden, heads = n_tp * size, n_tp * hd
    hbm = pl.BlockSpec(memory_space=pl.ANY)
    dma = pltpu.SemaphoreType.DMA
    flops = 8 * half * d * hidden + 14 * half * d * heads
    part_rows = max(4 * size, CORES * 4 * hd)

    def ring_sems(pieces):
        return [dma((pieces, 2, hops))] * 2 + [dma((pieces, chips))] * 4 + [dma((pieces,))]

    return pl.pallas_call(
        functools.partial(block_kernel, n_tp, paired, tile, big),
        name='block_back',
        out_shape=[jax.ShapeDtypeStruct((tokens, d), F32)] * 4
        + [jax.ShapeDtypeStruct((2, size, d), F32), jax.ShapeDtypeStruct((4 * hd, d), F32)],
        in_specs=[hbm] * 4 + [pl.BlockSpec(memory_space=pltpu.SMEM)] + [hbm] * 6,
        out_specs=[hbm] * 6,
        scratch_shapes=[
            pltpu.VMEM((hidden, d), BF16), pltpu.VMEM((hidden, d), BF16),
            pltpu.VMEM((heads, d), BF16), pltpu.VMEM((heads, d), BF16), pltpu.VMEM((heads, d), BF16),
            pltpu.VMEM((half, d), BF16), pltpu.VMEM((half, d), BF16),
            pltpu.VMEM((half, d), F32), pltpu.VMEM((half, d), F32),
            pltpu.VMEM((part_rows, d), F32), pltpu.VMEM((max(2 * size, 4 * hd), d), F32),
            pltpu.VMEM((3, big, d), F32), pltpu.VMEM((2, d, hd), BF16),
            *ring_sems(2), *ring_sems(4),
            dma((2, 3)), dma((3,)), dma((4, n_bigs)), dma((4, n_bigs)), dma((4, n_bigs)), dma((3,)), dma((3,)), dma((3,)),
            dma((2,)),
        ],
        compiler_params=pltpu.CompilerParams(collective_id=0, has_side_effects=True, vmem_limit_bytes=67043328),
        cost_estimate=pl.CostEstimate(flops=flops, bytes_accessed=10 * tokens * d * 4, transcendentals=half * hidden),
    )(y1, y2, dy1, dy2, lens, w1_own, w2_own, wq_in, wk_in, wv_in, wo_own)


def settle_kernel(chunk, depth, *refs):
    acts_in, (mlp_in, attn_in), acts_out, grads_out = refs[:4], refs[4:6], refs[6:10], refs[10:16]
    buf, mlp_buf, attn_buf, turned, read_sem, write_sem, small_sem = refs[16:]
    size, hd = mlp_buf.shape[1], attn_buf.shape[1]
    jobs = [(act, first) for act in range(4) for first in range(0, acts_in[0].shape[0], chunk)]

    def read(k):
        act, first = jobs[k]
        return pltpu.make_async_copy(acts_in[act].at[pl.ds(first, chunk)], buf.at[k % depth], read_sem.at[k % depth])

    def write(k):
        act, first = jobs[k]
        return pltpu.make_async_copy(buf.at[k % depth], acts_out[act].at[pl.ds(first, chunk)], write_sem.at[k % depth])

    small_reads = [pltpu.make_async_copy(mlp_in, mlp_buf, small_sem.at[0]), pltpu.make_async_copy(attn_in, attn_buf, small_sem.at[1])]
    small_writes = [pltpu.make_async_copy(src, dst, small_sem.at[2 + i]) for i, (src, dst) in enumerate(
        [(turned.at[i], grads_out[i]) for i in range(3)] + [(attn_buf.at[3], grads_out[3]), (mlp_buf.at[0], grads_out[4]),
                                                            (mlp_buf.at[1], grads_out[5])])]
    for copy in small_reads:
        copy.start()
    for k in range(min(depth, len(jobs))):
        read(k).start()
    for copy in small_reads:
        copy.wait()
    for i in range(3):
        turned[i] = attn_buf[i].T
    for copy in small_writes:
        copy.start()
    lag = depth // 2
    for k in range(len(jobs)):
        read(k).wait()
        write(k).start()
        if k >= lag:
            write(k - lag).wait()
            if k - lag + depth < len(jobs):
                read(k - lag + depth).start()
    for k in range(max(len(jobs) - lag, 0), len(jobs)):
        write(k).wait()
    for copy in small_writes:
        copy.wait()


def settle(acts, dw_mlp, dw_attn, chunk=256, depth=24):
    tokens, d = acts[0].shape
    size, hd = dw_mlp.shape[1], dw_attn.shape[1]
    hbm = pl.BlockSpec(memory_space=pl.ANY)
    dma = pltpu.SemaphoreType.DMA
    grads = [(d, hd)] * 3 + [(hd, d), (size, d), (size, d)]
    return pl.pallas_call(
        functools.partial(settle_kernel, chunk, depth),
        name='settle',
        out_shape=[jax.ShapeDtypeStruct((tokens, d), F32)] * 4 + [jax.ShapeDtypeStruct(shape, F32) for shape in grads],
        in_specs=[hbm] * 6,
        out_specs=[hbm] * 10,
        scratch_shapes=[
            pltpu.VMEM((depth, chunk, d), F32), pltpu.VMEM(dw_mlp.shape, F32), pltpu.VMEM(dw_attn.shape, F32),
            pltpu.VMEM((3, d, hd), F32), dma((depth,)), dma((depth,)), dma((8,)),
        ],
        compiler_params=pltpu.CompilerParams(vmem_limit_bytes=60 * 2 ** 20),
        cost_estimate=pl.CostEstimate(flops=0, bytes_accessed=8 * tokens * d * 4, transcendentals=0),
    )(*acts, dw_mlp, dw_attn)


def layer_back(carry, lens, layer_w, n_tp, paired):
    w_query, w_key, w_value, w_out, w_up, w_down = layer_w
    d, _, hd = w_query.shape
    heads = [w.reshape(d, hd) for w in (w_query, w_key, w_value)]
    *carry, dw_mlp, dw_attn = block_back(n_tp, paired, *carry, lens, w_up.T, w_down, *heads, w_out.reshape(hd, d))
    *carry, dwq, dwk, dwv, dwo, dw1, dw2 = settle(carry, dw_mlp, dw_attn.reshape(4, hd, d))
    grads = (dwq.reshape(w_query.shape), dwk.reshape(w_key.shape), dwv.reshape(w_value.shape), dwo.reshape(w_out.shape),
             dw1.T, dw2)
    return tuple(carry), grads


def solution(mesh):
    act_spec = P('dp', None, None)
    w_specs = (P(None, None, 'tp', None), P(None, None, 'tp', None), P(None, None, 'tp', None),
               P(None, 'tp', None, None), P(None, None, 'tp'), P(None, 'tp', None))
    g_specs = (P('dp', None, 'tp', None), P('dp', None, 'tp', None), P('dp', None, 'tp', None),
               P('dp', 'tp', None, None), P('dp', None, 'tp'), P('dp', 'tp', None))
    n_tp = mesh.shape['tp']
    paired = mesh.shape['dp'] % 2 == 0

    def local_fn(y_one, y_two, dy_one, dy_two, seq_lens, *weights):
        n_seqs, seq_len, d = y_one.shape
        carry = tuple(act.reshape(n_seqs * seq_len, d) for act in (y_one, y_two, dy_one, dy_two))
        n_layers = weights[0].shape[0]
        grads_by_layer = [None] * n_layers
        for layer in reversed(range(n_layers)):
            (x1, x2, dx1, dx2), grads_by_layer[layer] = layer_back(carry, seq_lens, [w[layer] for w in weights], n_tp, paired)
            carry = (x1, x2, dx1, dx2)
        stacked = tuple(jnp.stack(grads) for grads in zip(*grads_by_layer))
        return tuple(act.reshape(n_seqs, seq_len, d) for act in carry) + stacked

    return jax.shard_map(local_fn, mesh=mesh,
                         in_specs=(act_spec,) * 4 + (P('dp'),) + w_specs,
                         out_specs=(act_spec,) * 4 + g_specs,
                         check_vma=False)
```

```python
import functools

import jax
import jax.numpy as jnp
from jax import lax
from jax.experimental import pallas as pl
from jax.experimental.pallas import tpu as pltpu
from jax.sharding import PartitionSpec as P

F32 = jnp.float32
BF16 = jnp.bfloat16
EPS = 1e-5
MASK_VALUE = -1e30
CORES = 2
BLOCK = 128
GELU_A = 0.7978845608028654
GELU_B = 0.044715
LOG2_E = 1.4426950408889634


def dot_nt(a, b):
    return lax.dot_general(a, b, (((1,), (1,)), ((), ())), preferred_element_type=F32)


def dot_nn(a, b):
    return lax.dot_general(a, b, (((1,), (0,)), ((), ())), preferred_element_type=F32)


def dot_tn(a, b):
    return lax.dot_general(a, b, (((0,), (0,)), ((), ())), preferred_element_type=F32)


def gelu_and_slope(x):
    sq = x * x
    t = jnp.tanh(GELU_A * (x + GELU_B * (sq * x)))
    half = 0.5 * (1.0 + t)
    slope = half + (0.5 * x) * (1.0 - t * t) * (GELU_A * (1.0 + (3.0 * GELU_B) * sq))
    return x * half, slope


def inv_rms_of(x):
    return lax.rsqrt(jnp.mean(x * x, axis=-1, keepdims=True) + EPS)


def rms_back(x, grad):
    inv = inv_rms_of(x)
    normed = x * inv
    return inv * (grad - normed * jnp.mean(grad * normed, axis=-1, keepdims=True))


def rows_at(start, size):
    return pl.ds(start if isinstance(start, int) else pl.multiple_of(start, 16), size)


def attn_projections(normed, grad, wq, wkv, wo):
    return dot_nt(normed, wq).astype(BF16), dot_nt(normed, wkv).astype(BF16), dot_nt(grad, wo).astype(BF16)


def attn_scores(span, hd, proj):
    q, kv, da = proj
    out = []
    for first in range(0, span, BLOCK):
        r = slice(first, first + BLOCK)
        q_two = jnp.concatenate([q[r, :hd], q[r, hd:]], axis=0)
        da_two = jnp.concatenate([da[r, :hd], da[r, hd:]], axis=0)
        out.append((dot_nt(q_two, kv[r, :hd]), dot_nt(da_two, kv[r, hd:])))
    return out


def attn_softmax(hd, scores, masks):
    scale = hd ** -0.5
    out = []
    for (s, dp), mask in zip(scores, masks):
        s = jnp.where(jnp.concatenate([mask, mask], axis=0), s, MASK_VALUE)
        ex = jnp.exp2((s - jnp.max(s, axis=-1, keepdims=True)) * (scale * LOG2_E))
        p = ex * (1.0 / jnp.sum(ex, axis=-1, keepdims=True))
        ds = (p * (dp - jnp.sum(dp * p, axis=-1, keepdims=True)) * scale).astype(BF16)
        out.append((p.astype(BF16), ds))
    return out


def attn_grads(span, hd, proj, probs):
    q, kv, da = proj
    a, dq, dkv = [], [], ([], [])
    for first, (p, ds) in zip(range(0, span, BLOCK), probs):
        r = slice(first, first + BLOCK)
        two = dot_nn(p, kv[r, hd:]).astype(BF16)
        a.append(jnp.concatenate([two[:BLOCK], two[BLOCK:]], axis=1))
        two = dot_nn(ds, kv[r, :hd]).astype(BF16)
        dq.append(jnp.concatenate([two[:BLOCK], two[BLOCK:]], axis=1))
        for head in range(CORES):
            own, h = slice(head * BLOCK, (head + 1) * BLOCK), slice(head * hd, (head + 1) * hd)
            dkv[head].append(jnp.concatenate([dot_tn(ds[own], q[r, h]).astype(BF16),
                                              dot_tn(p[own], da[r, h]).astype(BF16)], axis=1))
    return tuple(jnp.concatenate(parts, axis=0) for parts in (a, dq, *dkv))


def when_do(condition, step):
    @pl.when(condition)
    def _():
        step()


class Ring:
    def __init__(self, n_tp, paired):
        self.chips = n_tp // CORES
        self.far = self.chips // 2
        me, group = lax.axis_index('tp'), lax.axis_index('dp')
        self.core = lax.rem(me, CORES)
        chip = lax.div(me, CORES)
        up = lax.rem(chip + 1, self.chips) * CORES + self.core
        down = lax.rem(chip + self.chips - 1, self.chips) * CORES + self.core
        self.toward = ({'tp': up}, {'tp': down})
        self.sibling = {'tp': chip * CORES + (1 - self.core)}
        self.paired = paired
        self.parity = lax.rem(group, 2) if paired else 0
        self.partner = {'dp': group + 1 - 2 * self.parity}

    def peers(self):
        return (*self.toward, self.sibling) + ((self.partner,) if self.paired else ())

    def slot(self, hop, way):
        return 2 * hop - 1 if hop == self.far else 2 * hop - 1 + way


def remote(src, dst, send, recv, peer):
    return pltpu.make_async_remote_copy(src_ref=src, dst_ref=dst, send_sem=send, recv_sem=recv,
                                        device_id=peer, device_id_type=pl.DeviceIdType.MESH)


class Shares:
    def __init__(self, ring, pieces, sems):
        self.ring, self.pieces = ring, pieces
        self.send, self.recv, self.pair_send, self.pair_recv, self.d2d_send, self.d2d_recv, self.local = sems

    def lot(self, piece, kind):
        rows, ring_rows = self.pieces[piece][5:7]
        if kind == 'all' or not self.ring.paired:
            return 0, rows
        if kind == 'ring':
            return self.ring.parity * (rows - ring_rows), ring_rows
        return self.ring.parity * ring_rows, rows - ring_rows

    def place(self, piece, slot, kind='all'):
        _, _, full, part, first, *_ = self.pieces[piece]
        low, rows = self.lot(piece, kind)
        return full.at[rows_at((slot * CORES + self.ring.core) * part + first + low, rows)]

    def own(self, piece, kind='all'):
        own, first, *_ = self.pieces[piece]
        if own is None:
            return self.place(piece, 0, kind)
        low, rows = self.lot(piece, kind)
        return own.at[rows_at(first + low, rows)]

    def ways(self, hop):
        return [(piece, way) for piece in range(len(self.pieces)) for way in range(2)
                if hop < self.ring.far or (hop == self.ring.far and self.pieces[piece][-1] == way)]

    def hop_copy(self, piece, way, hop):
        src = self.own(piece, 'ring') if hop == 1 else self.place(piece, self.ring.slot(hop - 1, way), 'ring')
        return remote(src, self.place(piece, self.ring.slot(hop, way), 'ring'), self.send.at[piece, way, hop - 1],
                      self.recv.at[piece, way, hop - 1], self.ring.toward[way])

    def pair_copy(self, piece, slot):
        ref = self.place(piece, slot, 'pair')
        return remote(ref, ref, self.pair_send.at[piece, slot], self.pair_recv.at[piece, slot], self.ring.partner)

    def sibling_copy(self, piece, slot):
        src = self.own(piece) if slot == 0 else self.place(piece, slot)
        return remote(src, self.place(piece, slot), self.d2d_send.at[piece, slot], self.d2d_recv.at[piece, slot],
                      self.ring.sibling)

    def local_copy(self, piece):
        return pltpu.make_async_copy(self.own(piece), self.place(piece, 0), self.local.at[piece])

    def local_pieces(self):
        return [piece for piece in range(len(self.pieces)) if self.pieces[piece][0] is not None]

    def start_local(self):
        for piece in self.local_pieces():
            self.local_copy(piece).start()

    def start(self):
        for piece, way in self.ways(1):
            self.hop_copy(piece, way, 1).start()
        for piece in range(len(self.pieces)):
            self.sibling_copy(piece, 0).start()

    def wait_own(self):
        for piece in self.local_pieces():
            self.local_copy(piece).wait()
        for piece in range(len(self.pieces)):
            self.sibling_copy(piece, 0).wait_recv()

    def bundle(self, hop, part):
        return [(piece, way) for piece, way in self.ways(hop) if self.pieces[piece][-1] == part]

    def take_ring(self, hop, part):
        later = self.ways(hop + 1)
        for piece, way in self.bundle(hop, part):
            self.hop_copy(piece, way, hop).wait_recv()
            if (piece, way) in later:
                self.hop_copy(piece, way, hop + 1).start()
            if self.ring.paired:
                self.pair_copy(piece, self.ring.slot(hop, way)).start()

    def take_pair(self, hop, part):
        for piece, way in self.bundle(hop, part):
            if self.ring.paired:
                self.pair_copy(piece, self.ring.slot(hop, way)).wait_recv()
            self.sibling_copy(piece, self.ring.slot(hop, way)).start()

    def take_sibling(self, hop):
        for piece, way in self.ways(hop):
            self.sibling_copy(piece, self.ring.slot(hop, way)).wait_recv()

    def finish(self):
        for hop in range(1, self.ring.far + 1):
            for piece, way in self.ways(hop):
                self.hop_copy(piece, way, hop).wait_send()
                if self.ring.paired:
                    self.pair_copy(piece, self.ring.slot(hop, way)).wait_send()
        for piece in range(len(self.pieces)):
            for slot in range(self.ring.chips):
                self.sibling_copy(piece, slot).wait_send()


def block_kernel(n_tp, paired, tile, big, y1, y2, dy1, dy2, lens, w1_own, w2_own, wq_in, wk_in, wv_in, wo_own,
                 x1, x2, dx1, dx2, dw_mlp, dw_attn,
                 w1, w2, wq, wkv, wo, norm, grad, acc_a, acc_b, part, from_sib, stage, flat_w,
                 mlp_send, mlp_recv, mlp_pair_send, mlp_pair_recv, mlp_d2d_send, mlp_d2d_recv, mlp_local,
                 attn_send, attn_recv, attn_pair_send, attn_pair_recv, attn_d2d_send, attn_d2d_recv, attn_local,
                 norm_sem, stage_sem, out_sem, sib_send, sib_recv, dw_send, dw_recv, dw_sem, flat_sem):
    ring = Ring(n_tp, paired)
    far = ring.far
    size = w1_own.shape[0]
    hd = wo_own.shape[0]
    half_hd = hd // 2
    rows_own = norm.shape[0]
    base = ring.core * rows_own
    n_tiles, n_bigs = rows_own // tile, rows_own // big

    barrier = pltpu.get_barrier_semaphore()
    for peer in ring.peers():
        pl.semaphore_signal(barrier, inc=1, device_id=peer, device_id_type=pl.DeviceIdType.MESH)

    mlp = Shares(ring, ((w1_own, 0, w1, size, 0, size, 2 * size // 3, 0), (w2_own, 0, w2, size, 0, size, 2 * size // 3, 1)),
                 (mlp_send, mlp_recv, mlp_pair_send, mlp_pair_recv, mlp_d2d_send, mlp_d2d_recv, mlp_local))
    attn = Shares(ring, ((None, 0, wq, hd, 0, hd, 5 * hd // 8, 0), (None, 0, wkv, hd, 0, half_hd, 3 * hd // 8, 0),
                         (None, half_hd, wkv, hd, half_hd, half_hd, hd // 4, 1), (wo_own, 0, wo, hd, 0, hd, 5 * hd // 8, 1)),
                  (attn_send, attn_recv, attn_pair_send, attn_pair_recv, attn_d2d_send, attn_d2d_recv, attn_local))

    def hbm_rows(ref, first, rows):
        return ref.at[rows_at(base + first, rows)]

    depth = stage.shape[0]

    def norm_fetch(which, t):
        slot = lax.rem(t, depth)
        return pltpu.make_async_copy(hbm_rows((y1, dy2)[which], t * tile, tile), stage.at[slot, rows_at(which * tile, tile)],
                                     norm_sem.at[which, slot])

    for t in range(min(depth, n_tiles)):
        for which in range(2):
            norm_fetch(which, t).start()

    def flat_copy(which, src):
        return pltpu.make_async_copy(src, flat_w.at[which], flat_sem.at[which])

    flat_copy(0, wq_in).start()

    @pl.when(ring.core == 0)
    def _():
        flat_copy(1, wk_in).start()

    @pl.when(ring.core == 1)
    def _():
        flat_copy(1, wv_in).start()

    mlp.start_local()
    attn.start_local()
    pl.semaphore_wait(barrier, len(ring.peers()))
    mlp.start()

    def norm_body(t, _):
        here = rows_at(t * tile, tile)
        slot = lax.rem(t, depth)
        for which in range(2):
            norm_fetch(which, t).wait()
        y = stage[slot, 0:tile, :]
        norm[here, :] = (y * inv_rms_of(y)).astype(BF16)
        grad[here, :] = stage[slot, tile:2 * tile, :].astype(BF16)

        @pl.when(t + depth < n_tiles)
        def _():
            for which in range(2):
                norm_fetch(which, t + depth).start()

        return 0

    lax.fori_loop(0, n_tiles, norm_body, 0)

    def mlp_hidden(here, cols):
        pre = dot_nt(norm[here, :], w1[cols, :])
        d_act = dot_nt(grad[here, :], w2[cols, :])
        act, slope = gelu_and_slope(pre)
        return act.astype(BF16), (d_act * slope).astype(BF16)

    def r(shares, hop, part):
        with jax.named_scope('ring'):
            shares.take_ring(hop, part)

    def y(shares, hop, part):
        with jax.named_scope('pair'):
            shares.take_pair(hop, part)

    def both(step, shares, hop):
        step(shares, hop, 0)
        step(shares, hop, 1)

    plan = {
        ('own', 0): lambda: r(mlp, 1, 0),
        ('own', 2): lambda: r(mlp, 1, 1),
        ('mlp1', -1): lambda: (y(mlp, 1, 0), r(mlp, 2, 0), y(mlp, 1, 1), r(mlp, 2, 1), mlp.take_sibling(1)),
        ('mlp1', 0): lambda: y(mlp, 2, 0),
        ('mlp1', 1): lambda: r(mlp, 3, 0),
        ('mlp1', 2): lambda: y(mlp, 2, 1),
        ('mlp2', -1): lambda: (r(mlp, 3, 1), attn.start(), mlp.take_sibling(2)),
        ('mlp2', 0): lambda: y(mlp, 3, 0),
        ('mlp2', 1): lambda: both(r, mlp, 4),
        ('mlp2', 2): lambda: y(mlp, 3, 1),
        ('mlp3', -1): lambda: mlp.take_sibling(3),
        ('mlp3', 0): lambda: both(y, mlp, 4),
        ('mlp3', 1): lambda: r(attn, 1, 0),
        ('mlp3', 2): lambda: r(attn, 1, 1),
        ('last', -1): lambda: mlp.take_sibling(4),
        ('last', 0): lambda: (y(attn, 1, 0), r(attn, 2, 0)),
        ('last', 1): lambda: (y(attn, 1, 1), r(attn, 2, 1)),
        ('last', 2): lambda: r(attn, 3, 0),
        ('attn0', -1): lambda: (attn.wait_own(), attn.take_sibling(1)),
        ('attn0', 0): lambda: (y(attn, 2, 0), r(attn, 3, 1)),
        ('attn0', 1): lambda: (y(attn, 2, 1), both(r, attn, 4)),
        ('attn0', 2): lambda: both(y, attn, 3),
        ('attn1', -1): lambda: attn.take_sibling(2),
        ('attn1', 0): lambda: both(y, attn, 4),
        ('attn2', -1): lambda: attn.take_sibling(3),
        ('attn3', -1): lambda: attn.take_sibling(4),
    }

    def serve(phase, t):
        for (name, at), step in plan.items():
            if name == phase and at >= 0:
                when_do(t == at, step)

    def serve_loop(kind, index, indices, t=None):
        for i in indices:
            if t is None and (f'{kind}{i}', -1) in plan:
                when_do(index == i, plan[f'{kind}{i}', -1])
            for at in range(n_bigs if t is not None else 0):
                if (f'{kind}{i}', at) in plan:
                    when_do((index == i) & (t == at), plan[f'{kind}{i}', at])

    width = CORES * size
    mlp.wait_own()
    part[...] = jnp.zeros_like(part)

    def mlp_own(t, _):
        here = rows_at(t * big, big)
        cols = rows_at(0, width)
        act, d_pre = mlp_hidden(here, cols)
        acc_a[here, :] = dot_nn(act, w2[cols, :])
        acc_b[here, :] = dot_nn(d_pre, w1[cols, :])
        part[0:width, :] += dot_tn(d_pre, norm[here, :])
        part[width:2 * width, :] += dot_tn(act, grad[here, :])
        serve('own', t)
        return 0

    with jax.named_scope('mlp_own'):
        lax.fori_loop(0, n_bigs, mlp_own, 0)

    eye = (lax.broadcasted_iota(jnp.int32, (hd, hd), 0) == lax.broadcasted_iota(jnp.int32, (hd, hd), 1)).astype(BF16)
    for which, dst in enumerate((wq, wkv)):
        flat_copy(which, wq_in).wait()
        dst[rows_at(ring.core * hd, hd), :] = dot_nt(eye, flat_w[which]).astype(BF16)

    def mlp_dw(mat, which):
        core = 1 - ring.core if which else ring.core
        return rows_at(mat * width + core * size, size)

    def mlp_dw_out(mat):
        return pltpu.make_async_copy(from_sib.at[rows_at(mat * size, size)], dw_mlp.at[mat], dw_sem.at[mat])

    def mlp_dw_copy(mat):
        return remote(part.at[mlp_dw(mat, 1)], from_sib.at[rows_at(mat * size, size)], dw_send.at[mat], dw_recv.at[mat],
                      ring.sibling)

    def mlp_pair(hop, _):
        with jax.named_scope('mlp_wait'):
            serve_loop('mlp', hop, range(1, far))
        cols = rows_at((2 * hop - 1) * width, 2 * width)

        def body(t, _):
            here = rows_at(t * big, big)
            act, d_pre = mlp_hidden(here, cols)
            acc_a[here, :] += dot_nn(act, w2[cols, :])
            acc_b[here, :] += dot_nn(d_pre, w1[cols, :])
            serve_loop('mlp', hop, range(1, far), t)
            return 0

        with jax.named_scope('mlp_pair'):
            lax.fori_loop(0, n_bigs, body, 0)

        @pl.when(hop == 1)
        def _():
            for mat in range(2):
                mlp_dw_copy(mat).start()

        return 0

    lax.fori_loop(1, far, mlp_pair, 0)

    def out_copy(which, ref, src, t):
        return pltpu.make_async_copy(src.at[rows_at(t * big, big)], hbm_rows(ref, t * big, big), out_sem.at[which, t])

    def sib_copy(which, ref, src, t):
        return remote(src.at[rows_at(t * big, big)], hbm_rows(ref, t * big, big), sib_send.at[which, t], sib_recv.at[which, t],
                      ring.sibling)

    def emit(outs, t):
        for which, ref, src in outs:
            out_copy(which, ref, src, t).start()
            sib_copy(which, ref, src, t).start()

    def emitted(outs, t):
        for which, ref, src in outs:
            out_copy(which, ref, src, t).wait()
            sib_copy(which, ref, src, t).wait_send()

    mlp_outs = ((0, x2, acc_a), (1, dx1, acc_b))
    attn_outs = ((2, x1, acc_a), (3, dx2, acc_b))

    def stage_copy(which, src, t):
        return pltpu.make_async_copy(hbm_rows(src, t * big, big), stage.at[which], stage_sem.at[which])

    with jax.named_scope('mlp_wait'):
        plan['last', -1]()
    for mat in range(2):
        mlp_dw_copy(mat).wait_send()
        mlp_dw_copy(mat).wait_recv()
        mine = rows_at(mat * size, size)
        from_sib[mine, :] = from_sib[mine, :] + part[mlp_dw(mat, 0), :]
        mlp_dw_out(mat).start()

    def mlp_last(t, _):
        here = rows_at(t * big, big)
        cols = rows_at((2 * far - 1) * width, width)
        ins = tuple(enumerate((y1, y2, dy1)))
        for which, src in ins:
            stage_copy(which, src, t).start()
        act, d_pre = mlp_hidden(here, cols)
        total_a = acc_a[here, :] + dot_nn(act, w2[cols, :])
        total_b = acc_b[here, :] + dot_nn(d_pre, w1[cols, :])
        for which, src in ins:
            stage_copy(which, src, t).wait()
        x = stage[1] - total_a
        d = stage[2] + rms_back(stage[0], total_b)
        acc_a[here, :] = x
        acc_b[here, :] = d
        norm[here, :] = (x * inv_rms_of(x)).astype(BF16)
        grad[here, :] = d.astype(BF16)
        emit(mlp_outs, t)
        serve('last', t)
        return 0

    with jax.named_scope('mlp_last'):
        lax.fori_loop(0, n_bigs, mlp_last, 0)

    row_pos = lax.broadcasted_iota(jnp.int32, (BLOCK, BLOCK), 0)
    col_pos = lax.broadcasted_iota(jnp.int32, (BLOCK, BLOCK), 1)
    seq = BLOCK // 2
    causal = (col_pos <= row_pos) & ((col_pos < seq) == (row_pos < seq))
    share = CORES * hd
    first_seq = ring.core * (rows_own // seq)

    def masks_of(t):
        out = []
        for block in range(big // BLOCK):
            at = first_seq + t * (big // seq) + 2 * block
            end = jnp.where(col_pos < seq, lens[at], seq + lens[at + 1])
            out.append(causal & (col_pos < end))
        return out

    def attn_pair(t, j):
        here = rows_at(t * big, big)
        masks = masks_of(t)

        def weights(i):
            r = rows_at((2 * j + i) * share, share)
            return wq[r, :], wkv[r, :], wo[r, :]

        def project(i):
            return attn_projections(norm[here, :], grad[here, :], *weights(i))

        def finish(i, factors):
            q_w, kv_w, o_w = weights(i)
            a, dq, d0, d1 = factors
            return dot_nn(a, o_w), dot_nn(dq, q_w) + dot_nn(d0, kv_w) + dot_nn(d1, kv_w)

        first = project(0)
        scores = attn_scores(big, hd, first)
        second = project(1)
        factors = attn_grads(big, hd, first, attn_softmax(hd, scores, masks))
        scores = attn_scores(big, hd, second)
        f, g = finish(0, factors)
        f2, g2 = finish(1, attn_grads(big, hd, second, attn_softmax(hd, scores, masks)))
        return f + f2, g + g2, factors

    with jax.named_scope('attn_first_wait'):
        plan['attn0', -1]()
    part[...] = jnp.zeros_like(part)
    own_part = 4 * hd
    for mat in range(2):
        mlp_dw_out(mat).wait()

    def attn_first(t, _):
        here = rows_at(t * big, big)
        f, g, (a, dq, d0, d1) = attn_pair(t, 0)
        for head, dkv in enumerate((d0, d1)):
            cols = slice(head * hd, (head + 1) * hd)
            left = jnp.concatenate([dq[:, cols], dkv], axis=1)
            part[head * own_part:head * own_part + 3 * hd, :] += dot_tn(left, norm[here, :])
            part[head * own_part + 3 * hd:(head + 1) * own_part, :] += dot_tn(a[:, cols], grad[here, :])
        emitted(mlp_outs, t)
        acc_a[here, :] = f
        acc_b[here, :] = g
        serve('attn0', t)
        return 0

    with jax.named_scope('attn_first'):
        lax.fori_loop(0, n_bigs, attn_first, 0)
    def attn_dw(which):
        core = 1 - ring.core if which else ring.core
        return rows_at(core * own_part, own_part)

    def attn_dw_copy():
        return remote(part.at[attn_dw(1)], from_sib.at[rows_at(0, own_part)], dw_send.at[2], dw_recv.at[2], ring.sibling)

    def attn_dw_out():
        return pltpu.make_async_copy(from_sib.at[rows_at(0, own_part)], dw_attn, dw_sem.at[2])

    def attn_middle(j, _):
        with jax.named_scope('attn_wait'):
            serve_loop('attn', j, range(1, far - 1))

        def body(t, _):
            here = rows_at(t * big, big)
            f, g, _ = attn_pair(t, j)
            acc_a[here, :] += f
            acc_b[here, :] += g
            serve_loop('attn', j, range(1, far - 1), t)
            return 0

        with jax.named_scope('attn_pair'):
            lax.fori_loop(0, n_bigs, body, 0)

        @pl.when(j == 1)
        def _():
            attn_dw_copy().start()

        return 0

    lax.fori_loop(1, far - 1, attn_middle, 0)

    with jax.named_scope('attn_wait'):
        plan['attn3', -1]()
    attn_dw_copy().wait_send()
    attn_dw_copy().wait_recv()
    mine = rows_at(0, own_part)
    from_sib[mine, :] = from_sib[mine, :] + part[attn_dw(0), :]
    attn_dw_out().start()

    def attn_last(t, _):
        here = rows_at(t * big, big)
        ins = tuple(enumerate((y1, x2, dy2)))
        for which, src in ins:
            stage_copy(which, src, t).start()
        f, g, _ = attn_pair(t, far - 1)
        for which, src in ins:
            stage_copy(which, src, t).wait()
        acc_a[here, :] = stage[0] - (acc_a[here, :] + f)
        acc_b[here, :] = stage[2] + rms_back(stage[1], acc_b[here, :] + g)
        emit(attn_outs, t)
        return 0

    with jax.named_scope('attn_last'):
        lax.fori_loop(0, n_bigs, attn_last, 0)

    mlp.finish()
    attn.finish()
    attn_dw_out().wait()

    def drain(t, _):
        emitted(attn_outs, t)
        for which, ref, src in (*mlp_outs, *attn_outs):
            sib_copy(which, ref, src, t).wait_recv()
        return 0

    with jax.named_scope('drain'):
        lax.fori_loop(0, n_bigs, drain, 0)


def block_back(n_tp, paired, y1, y2, dy1, dy2, lens, w1_own, w2_own, wq_in, wk_in, wv_in, wo_own, tile=256, big=512):
    tokens, d = y1.shape
    size, hd = w1_own.shape[0], wo_own.shape[0]
    chips = n_tp // CORES
    hops = chips // 2
    half = tokens // CORES
    n_bigs = half // big
    hidden, heads = n_tp * size, n_tp * hd
    hbm = pl.BlockSpec(memory_space=pl.ANY)
    dma = pltpu.SemaphoreType.DMA
    flops = 8 * half * d * hidden + 14 * half * d * heads
    part_rows = max(4 * size, CORES * 4 * hd)

    def ring_sems(pieces):
        return [dma((pieces, 2, hops))] * 2 + [dma((pieces, chips))] * 4 + [dma((pieces,))]

    return pl.pallas_call(
        functools.partial(block_kernel, n_tp, paired, tile, big),
        name='block_back',
        out_shape=[jax.ShapeDtypeStruct((tokens, d), F32)] * 4
        + [jax.ShapeDtypeStruct((2, size, d), F32), jax.ShapeDtypeStruct((4 * hd, d), F32)],
        in_specs=[hbm] * 4 + [pl.BlockSpec(memory_space=pltpu.SMEM)] + [hbm] * 6,
        out_specs=[hbm] * 6,
        scratch_shapes=[
            pltpu.VMEM((hidden, d), BF16), pltpu.VMEM((hidden, d), BF16),
            pltpu.VMEM((heads, d), BF16), pltpu.VMEM((heads, d), BF16), pltpu.VMEM((heads, d), BF16),
            pltpu.VMEM((half, d), BF16), pltpu.VMEM((half, d), BF16),
            pltpu.VMEM((half, d), F32), pltpu.VMEM((half, d), F32),
            pltpu.VMEM((part_rows, d), F32), pltpu.VMEM((max(2 * size, 4 * hd), d), F32),
            pltpu.VMEM((3, big, d), F32), pltpu.VMEM((2, d, hd), BF16),
            *ring_sems(2), *ring_sems(4),
            dma((2, 3)), dma((3,)), dma((4, n_bigs)), dma((4, n_bigs)), dma((4, n_bigs)), dma((3,)), dma((3,)), dma((3,)),
            dma((2,)),
        ],
        compiler_params=pltpu.CompilerParams(collective_id=0, has_side_effects=True, vmem_limit_bytes=67043328),
        cost_estimate=pl.CostEstimate(flops=flops, bytes_accessed=10 * tokens * d * 4, transcendentals=half * hidden),
    )(y1, y2, dy1, dy2, lens, w1_own, w2_own, wq_in, wk_in, wv_in, wo_own)


def settle_kernel(chunk, depth, *refs):
    acts_in, (mlp_in, attn_in), acts_out, grads_out = refs[:4], refs[4:6], refs[6:10], refs[10:16]
    buf, mlp_buf, attn_buf, turned, read_sem, write_sem, small_sem = refs[16:]
    size, hd = mlp_buf.shape[1], attn_buf.shape[1]
    jobs = [(act, first) for act in range(4) for first in range(0, acts_in[0].shape[0], chunk)]

    def read(k):
        act, first = jobs[k]
        return pltpu.make_async_copy(acts_in[act].at[pl.ds(first, chunk)], buf.at[k % depth], read_sem.at[k % depth])

    def write(k):
        act, first = jobs[k]
        return pltpu.make_async_copy(buf.at[k % depth], acts_out[act].at[pl.ds(first, chunk)], write_sem.at[k % depth])

    small_reads = [pltpu.make_async_copy(mlp_in, mlp_buf, small_sem.at[0]), pltpu.make_async_copy(attn_in, attn_buf, small_sem.at[1])]
    small_writes = [pltpu.make_async_copy(src, dst, small_sem.at[2 + i]) for i, (src, dst) in enumerate(
        [(turned.at[i], grads_out[i]) for i in range(3)] + [(attn_buf.at[3], grads_out[3]), (mlp_buf.at[0], grads_out[4]),
                                                            (mlp_buf.at[1], grads_out[5])])]
    for copy in small_reads:
        copy.start()
    for k in range(min(depth, len(jobs))):
        read(k).start()
    for copy in small_reads:
        copy.wait()
    for i in range(3):
        turned[i] = attn_buf[i].T
    for copy in small_writes:
        copy.start()
    lag = depth // 2
    for k in range(len(jobs)):
        read(k).wait()
        write(k).start()
        if k >= lag:
            write(k - lag).wait()
            if k - lag + depth < len(jobs):
                read(k - lag + depth).start()
    for k in range(max(len(jobs) - lag, 0), len(jobs)):
        write(k).wait()
    for copy in small_writes:
        copy.wait()


def settle(acts, dw_mlp, dw_attn, chunk=256, depth=24):
    tokens, d = acts[0].shape
    size, hd = dw_mlp.shape[1], dw_attn.shape[1]
    hbm = pl.BlockSpec(memory_space=pl.ANY)
    dma = pltpu.SemaphoreType.DMA
    grads = [(d, hd)] * 3 + [(hd, d), (size, d), (size, d)]
    return pl.pallas_call(
        functools.partial(settle_kernel, chunk, depth),
        name='settle',
        out_shape=[jax.ShapeDtypeStruct((tokens, d), F32)] * 4 + [jax.ShapeDtypeStruct(shape, F32) for shape in grads],
        in_specs=[hbm] * 6,
        out_specs=[hbm] * 10,
        scratch_shapes=[
            pltpu.VMEM((depth, chunk, d), F32), pltpu.VMEM(dw_mlp.shape, F32), pltpu.VMEM(dw_attn.shape, F32),
            pltpu.VMEM((3, d, hd), F32), dma((depth,)), dma((depth,)), dma((8,)),
        ],
        compiler_params=pltpu.CompilerParams(vmem_limit_bytes=60 * 2 ** 20),
        cost_estimate=pl.CostEstimate(flops=0, bytes_accessed=8 * tokens * d * 4, transcendentals=0),
    )(*acts, dw_mlp, dw_attn)


def layer_back(carry, lens, layer_w, n_tp, paired):
    w_query, w_key, w_value, w_out, w_up, w_down = layer_w
    d, _, hd = w_query.shape
    heads = [w.reshape(d, hd) for w in (w_query, w_key, w_value)]
    *carry, dw_mlp, dw_attn = block_back(n_tp, paired, *carry, lens, w_up.T, w_down, *heads, w_out.reshape(hd, d))
    *carry, dwq, dwk, dwv, dwo, dw1, dw2 = settle(carry, dw_mlp, dw_attn.reshape(4, hd, d))
    grads = (dwq.reshape(w_query.shape), dwk.reshape(w_key.shape), dwv.reshape(w_value.shape), dwo.reshape(w_out.shape),
             dw1.T, dw2)
    return tuple(carry), grads


def solution(mesh):
    act_spec = P('dp', None, None)
    w_specs = (P(None, None, 'tp', None), P(None, None, 'tp', None), P(None, None, 'tp', None),
               P(None, 'tp', None, None), P(None, None, 'tp'), P(None, 'tp', None))
    g_specs = (P('dp', None, 'tp', None), P('dp', None, 'tp', None), P('dp', None, 'tp', None),
               P('dp', 'tp', None, None), P('dp', None, 'tp'), P('dp', 'tp', None))
    n_tp = mesh.shape['tp']
    paired = mesh.shape['dp'] % 2 == 0

    def local_fn(y_one, y_two, dy_one, dy_two, seq_lens, *weights):
        n_seqs, seq_len, d = y_one.shape
        carry = tuple(act.reshape(n_seqs * seq_len, d) for act in (y_one, y_two, dy_one, dy_two))
        n_layers = weights[0].shape[0]
        grads_by_layer = [None] * n_layers
        for layer in reversed(range(n_layers)):
            (x1, x2, dx1, dx2), grads_by_layer[layer] = layer_back(carry, seq_lens, [w[layer] for w in weights], n_tp, paired)
            carry = (x1, x2, dx1, dx2)
        stacked = tuple(jnp.stack(grads) for grads in zip(*grads_by_layer))
        return tuple(act.reshape(n_seqs, seq_len, d) for act in carry) + stacked

    return jax.shard_map(local_fn, mesh=mesh,
                         in_specs=(act_spec,) * 4 + (P('dp'),) + w_specs,
                         out_specs=(act_spec,) * 4 + g_specs,
                         check_vma=False)
```

```python
import functools

import jax
import jax.numpy as jnp
from jax import lax
from jax.experimental import pallas as pl
from jax.experimental.pallas import tpu as pltpu
from jax.sharding import PartitionSpec as P

F32 = jnp.float32
BF16 = jnp.bfloat16
EPS = 1e-5
MASK_VALUE = -1e30
CORES = 2
BLOCK = 128
GELU_A = 0.7978845608028654
GELU_B = 0.044715
LOG2_E = 1.4426950408889634


def dot_nt(a, b):
    return lax.dot_general(a, b, (((1,), (1,)), ((), ())), preferred_element_type=F32)


def dot_nn(a, b):
    return lax.dot_general(a, b, (((1,), (0,)), ((), ())), preferred_element_type=F32)


def dot_tn(a, b):
    return lax.dot_general(a, b, (((0,), (0,)), ((), ())), preferred_element_type=F32)


def gelu_and_slope(x):
    sq = x * x
    t = jnp.tanh(GELU_A * (x + GELU_B * (sq * x)))
    half = 0.5 * (1.0 + t)
    slope = half + (0.5 * x) * (1.0 - t * t) * (GELU_A * (1.0 + (3.0 * GELU_B) * sq))
    return x * half, slope


def inv_rms_of(x):
    return lax.rsqrt(jnp.mean(x * x, axis=-1, keepdims=True) + EPS)


def rms_back(x, grad):
    inv = inv_rms_of(x)
    normed = x * inv
    return inv * (grad - normed * jnp.mean(grad * normed, axis=-1, keepdims=True))


def rows_at(start, size):
    return pl.ds(start if isinstance(start, int) else pl.multiple_of(start, 16), size)


def attn_projections(normed, grad, wq, wkv, wo):
    return dot_nt(normed, wq).astype(BF16), dot_nt(normed, wkv).astype(BF16), dot_nt(grad, wo).astype(BF16)


def attn_scores(span, hd, proj):
    q, kv, da = proj
    out = []
    for first in range(0, span, BLOCK):
        r = slice(first, first + BLOCK)
        q_two = jnp.concatenate([q[r, :hd], q[r, hd:]], axis=0)
        da_two = jnp.concatenate([da[r, :hd], da[r, hd:]], axis=0)
        out.append((dot_nt(q_two, kv[r, :hd]), dot_nt(da_two, kv[r, hd:])))
    return out


def attn_softmax(hd, scores, masks):
    scale = hd ** -0.5
    out = []
    for (s, dp), mask in zip(scores, masks):
        s = jnp.where(jnp.concatenate([mask, mask], axis=0), s, MASK_VALUE)
        ex = jnp.exp2((s - jnp.max(s, axis=-1, keepdims=True)) * (scale * LOG2_E))
        p = ex * (1.0 / jnp.sum(ex, axis=-1, keepdims=True))
        ds = (p * (dp - jnp.sum(dp * p, axis=-1, keepdims=True)) * scale).astype(BF16)
        out.append((p.astype(BF16), ds))
    return out


def attn_grads(span, hd, proj, probs):
    q, kv, da = proj
    a, dq, dkv = [], [], ([], [])
    for first, (p, ds) in zip(range(0, span, BLOCK), probs):
        r = slice(first, first + BLOCK)
        two = dot_nn(p, kv[r, hd:]).astype(BF16)
        a.append(jnp.concatenate([two[:BLOCK], two[BLOCK:]], axis=1))
        two = dot_nn(ds, kv[r, :hd]).astype(BF16)
        dq.append(jnp.concatenate([two[:BLOCK], two[BLOCK:]], axis=1))
        for head in range(CORES):
            own, h = slice(head * BLOCK, (head + 1) * BLOCK), slice(head * hd, (head + 1) * hd)
            dkv[head].append(jnp.concatenate([dot_tn(ds[own], q[r, h]).astype(BF16),
                                              dot_tn(p[own], da[r, h]).astype(BF16)], axis=1))
    return tuple(jnp.concatenate(parts, axis=0) for parts in (a, dq, *dkv))


def when_do(condition, step):
    @pl.when(condition)
    def _():
        step()


class Ring:
    def __init__(self, n_tp, paired):
        self.chips = n_tp // CORES
        self.far = self.chips // 2
        me, group = lax.axis_index('tp'), lax.axis_index('dp')
        self.core = lax.rem(me, CORES)
        chip = lax.div(me, CORES)
        up = lax.rem(chip + 1, self.chips) * CORES + self.core
        down = lax.rem(chip + self.chips - 1, self.chips) * CORES + self.core
        self.toward = ({'tp': up}, {'tp': down})
        self.sibling = {'tp': chip * CORES + (1 - self.core)}
        self.paired = paired
        self.parity = lax.rem(group, 2) if paired else 0
        self.partner = {'dp': group + 1 - 2 * self.parity}

    def peers(self):
        return (*self.toward, self.sibling) + ((self.partner,) if self.paired else ())

    def slot(self, hop, way):
        return 2 * hop - 1 if hop == self.far else 2 * hop - 1 + way


def remote(src, dst, send, recv, peer):
    return pltpu.make_async_remote_copy(src_ref=src, dst_ref=dst, send_sem=send, recv_sem=recv,
                                        device_id=peer, device_id_type=pl.DeviceIdType.MESH)


class Shares:
    def __init__(self, ring, pieces, sems):
        self.ring, self.pieces = ring, pieces
        self.send, self.recv, self.pair_send, self.pair_recv, self.d2d_send, self.d2d_recv, self.local = sems

    def lot(self, piece, kind):
        rows, ring_rows = self.pieces[piece][5:7]
        if kind == 'all' or not self.ring.paired:
            return 0, rows
        if kind == 'ring':
            return self.ring.parity * (rows - ring_rows), ring_rows
        return self.ring.parity * ring_rows, rows - ring_rows

    def place(self, piece, slot, kind='all'):
        _, _, full, part, first, *_ = self.pieces[piece]
        low, rows = self.lot(piece, kind)
        return full.at[rows_at((slot * CORES + self.ring.core) * part + first + low, rows)]

    def own(self, piece, kind='all'):
        own, first, *_ = self.pieces[piece]
        if own is None:
            return self.place(piece, 0, kind)
        low, rows = self.lot(piece, kind)
        return own.at[rows_at(first + low, rows)]

    def ways(self, hop):
        return [(piece, way) for piece in range(len(self.pieces)) for way in range(2)
                if hop < self.ring.far or (hop == self.ring.far and self.pieces[piece][-1] == way)]

    def hop_copy(self, piece, way, hop):
        src = self.own(piece, 'ring') if hop == 1 else self.place(piece, self.ring.slot(hop - 1, way), 'ring')
        return remote(src, self.place(piece, self.ring.slot(hop, way), 'ring'), self.send.at[piece, way, hop - 1],
                      self.recv.at[piece, way, hop - 1], self.ring.toward[way])

    def pair_copy(self, piece, slot):
        ref = self.place(piece, slot, 'pair')
        return remote(ref, ref, self.pair_send.at[piece, slot], self.pair_recv.at[piece, slot], self.ring.partner)

    def sibling_copy(self, piece, slot):
        src = self.own(piece) if slot == 0 else self.place(piece, slot)
        return remote(src, self.place(piece, slot), self.d2d_send.at[piece, slot], self.d2d_recv.at[piece, slot],
                      self.ring.sibling)

    def local_copy(self, piece):
        return pltpu.make_async_copy(self.own(piece), self.place(piece, 0), self.local.at[piece])

    def local_pieces(self):
        return [piece for piece in range(len(self.pieces)) if self.pieces[piece][0] is not None]

    def start_local(self):
        for piece in self.local_pieces():
            self.local_copy(piece).start()

    def start(self, part):
        for piece, way in self.bundle(1, part):
            self.hop_copy(piece, way, 1).start()
            if way == part:
                self.sibling_copy(piece, 0).start()

    def wait_own(self):
        for piece in self.local_pieces():
            self.local_copy(piece).wait()
        for piece in range(len(self.pieces)):
            self.sibling_copy(piece, 0).wait_recv()

    def bundle(self, hop, part):
        return [(piece, way) for piece, way in self.ways(hop) if self.pieces[piece][-1] == part]

    def take_ring(self, hop, part):
        later = self.ways(hop + 1)
        for piece, way in self.bundle(hop, part):
            self.hop_copy(piece, way, hop).wait_recv()
            if (piece, way) in later:
                self.hop_copy(piece, way, hop + 1).start()
            if self.ring.paired:
                self.pair_copy(piece, self.ring.slot(hop, way)).start()

    def take_pair(self, hop, part):
        for piece, way in self.bundle(hop, part):
            if self.ring.paired:
                self.pair_copy(piece, self.ring.slot(hop, way)).wait_recv()
            self.sibling_copy(piece, self.ring.slot(hop, way)).start()

    def take_sibling(self, hop):
        for piece, way in self.ways(hop):
            self.sibling_copy(piece, self.ring.slot(hop, way)).wait_recv()

    def finish(self):
        for hop in range(1, self.ring.far + 1):
            for piece, way in self.ways(hop):
                self.hop_copy(piece, way, hop).wait_send()
                if self.ring.paired:
                    self.pair_copy(piece, self.ring.slot(hop, way)).wait_send()
        for piece in range(len(self.pieces)):
            for slot in range(self.ring.chips):
                self.sibling_copy(piece, slot).wait_send()


def block_kernel(n_tp, paired, tile, big, y1, y2, dy1, dy2, lens, w1_own, w2_own, wq_in, wk_in, wv_in, wo_own,
                 x1_sib, x2, dx1, dx2_sib, dw_mlp, dw_attn, acc_a, acc_b,
                 w1, w2, wq, wkv, wo, norm, grad, part, stage,
                 mlp_send, mlp_recv, mlp_pair_send, mlp_pair_recv, mlp_d2d_send, mlp_d2d_recv, mlp_local,
                 attn_send, attn_recv, attn_pair_send, attn_pair_recv, attn_d2d_send, attn_d2d_recv, attn_local,
                 norm_sem, stage_sem, out_sem, sib_send, sib_recv, dw_send, dw_recv, dw_sem, flat_sem):
    ring = Ring(n_tp, paired)
    far = ring.far
    size = w1_own.shape[0]
    hd = wo_own.shape[0]
    half_hd = hd // 2
    rows_own = norm.shape[0]
    base = ring.core * rows_own
    n_tiles, n_bigs = rows_own // tile, rows_own // big

    barrier = pltpu.get_barrier_semaphore()
    for peer in ring.peers():
        pl.semaphore_signal(barrier, inc=1, device_id=peer, device_id_type=pl.DeviceIdType.MESH)

    mlp = Shares(ring, ((w1_own, 0, w1, size, 0, size, 2 * size // 3, 0), (w2_own, 0, w2, size, 0, size, 2 * size // 3, 1)),
                 (mlp_send, mlp_recv, mlp_pair_send, mlp_pair_recv, mlp_d2d_send, mlp_d2d_recv, mlp_local))
    attn = Shares(ring, ((None, 0, wq, hd, 0, hd, 5 * hd // 8, 0), (None, 0, wkv, hd, 0, half_hd, 3 * hd // 8, 0),
                         (None, half_hd, wkv, hd, half_hd, half_hd, hd // 4, 1), (wo_own, 0, wo, hd, 0, hd, 5 * hd // 8, 1)),
                  (attn_send, attn_recv, attn_pair_send, attn_pair_recv, attn_d2d_send, attn_d2d_recv, attn_local))

    def hbm_rows(ref, first, rows):
        return ref.at[rows_at(base + first, rows)]

    depth = stage.shape[0]

    def norm_fetch(which, t):
        slot = lax.rem(t, depth)
        return pltpu.make_async_copy(hbm_rows((y1, dy2)[which], t * tile, tile), stage.at[slot, rows_at(which * tile, tile)],
                                     norm_sem.at[which, slot])

    for t in range(min(depth, n_tiles)):
        for which in range(2):
            norm_fetch(which, t).start()

    depth_w, places = w1.shape[1], (wo, wkv)
    flat = (slice(wo.shape[0] - depth_w, wo.shape[0]), slice(0, hd))

    def flat_copy(which, src):
        return pltpu.make_async_copy(src, places[which].at[flat], flat_sem.at[which])

    flat_copy(0, wq_in).start()

    @pl.when(ring.core == 0)
    def _():
        flat_copy(1, wk_in).start()

    @pl.when(ring.core == 1)
    def _():
        flat_copy(1, wv_in).start()

    mlp.start_local()
    attn.start_local()
    pl.semaphore_wait(barrier, len(ring.peers()))
    mlp.start(0)

    def norm_body(t, _):
        here = rows_at(t * tile, tile)
        slot = lax.rem(t, depth)
        for which in range(2):
            norm_fetch(which, t).wait()
        y = stage[slot, 0:tile, :]
        norm[here, :] = (y * inv_rms_of(y)).astype(BF16)
        grad[here, :] = stage[slot, tile:2 * tile, :].astype(BF16)

        @pl.when(t + depth < n_tiles)
        def _():
            for which in range(2):
                norm_fetch(which, t + depth).start()

        when_do(t == n_tiles // 3, lambda: mlp.start(1))
        return 0

    lax.fori_loop(0, n_tiles, norm_body, 0)

    def mlp_hidden(here, cols):
        pre = dot_nt(norm[here, :], w1[cols, :])
        d_act = dot_nt(grad[here, :], w2[cols, :])
        act, slope = gelu_and_slope(pre)
        return act.astype(BF16), (d_act * slope).astype(BF16)

    def r(shares, hop, part):
        with jax.named_scope('ring'):
            shares.take_ring(hop, part)

    def y(shares, hop, part):
        with jax.named_scope('pair'):
            shares.take_pair(hop, part)

    def both(step, shares, hop):
        step(shares, hop, 0)
        step(shares, hop, 1)

    plan = {
        ('own', 0): lambda: r(mlp, 1, 0),
        ('own', 1): lambda: r(mlp, 1, 1),
        ('mlp1', -1): lambda: (y(mlp, 1, 0), r(mlp, 2, 0), y(mlp, 1, 1), r(mlp, 2, 1), mlp.take_sibling(1)),
        ('mlp1', 0): lambda: y(mlp, 2, 0),
        ('mlp1', 1): lambda: (r(mlp, 3, 0), y(mlp, 2, 1)),
        ('mlp2', -1): lambda: (r(mlp, 3, 1), attn.start(0), attn.start(1), mlp.take_sibling(2)),
        ('mlp2', 0): lambda: y(mlp, 3, 0),
        ('mlp2', 1): lambda: (both(r, mlp, 4), y(mlp, 3, 1)),
        ('mlp3', -1): lambda: mlp.take_sibling(3),
        ('mlp3', 0): lambda: (both(y, mlp, 4), r(attn, 1, 0)),
        ('mlp3', 1): lambda: r(attn, 1, 1),
        ('mlp3', 2): lambda: (y(attn, 1, 0), r(attn, 2, 0)),
        ('last', -1): lambda: mlp.take_sibling(4),
        ('last', 0): lambda: (y(attn, 1, 1), r(attn, 2, 1)),
        ('last', 1): lambda: (y(attn, 2, 0), r(attn, 3, 0)),
        ('last', 2): lambda: y(attn, 2, 1),
        ('attn0', -1): lambda: (attn.wait_own(), attn.take_sibling(1)),
        ('attn0', 0): lambda: (r(attn, 3, 1), y(attn, 3, 0)),
        ('attn0', 1): lambda: (both(r, attn, 4), y(attn, 3, 1)),
        ('attn1', -1): lambda: attn.take_sibling(2),
        ('attn1', 0): lambda: both(y, attn, 4),
        ('attn2', -1): lambda: attn.take_sibling(3),
        ('attn3', -1): lambda: attn.take_sibling(4),
    }

    def serve(phase, t):
        for (name, at), step in plan.items():
            if name == phase and at >= 0:
                when_do(t == at, step)

    def serve_loop(kind, index, indices, t=None):
        for i in indices:
            if t is None and (f'{kind}{i}', -1) in plan:
                when_do(index == i, plan[f'{kind}{i}', -1])
            for at in range(n_bigs if t is not None else 0):
                if (f'{kind}{i}', at) in plan:
                    when_do((index == i) & (t == at), plan[f'{kind}{i}', at])

    width = CORES * size
    mlp.wait_own()
    part[...] = jnp.zeros_like(part)

    def mlp_own(t, _):
        here = rows_at(t * big, big)
        cols = rows_at(0, width)
        act, d_pre = mlp_hidden(here, cols)
        acc_a[here, :] = dot_nn(act, w2[cols, :])
        acc_b[here, :] = dot_nn(d_pre, w1[cols, :])
        part[0:width, :] += dot_tn(d_pre, norm[here, :])
        part[width:2 * width, :] += dot_tn(act, grad[here, :])
        serve('own', t)
        return 0

    with jax.named_scope('mlp_own'):
        lax.fori_loop(0, n_bigs, mlp_own, 0)

    eye = (lax.broadcasted_iota(jnp.int32, (hd, hd), 0) == lax.broadcasted_iota(jnp.int32, (hd, hd), 1)).astype(BF16)
    for which, dst in enumerate((wq, wkv)):
        flat_copy(which, wq_in).wait()
        dst[rows_at(ring.core * hd, hd), :] = dot_nt(eye, places[which][flat]).astype(BF16)

    def mlp_dw(mat, which):
        core = 1 - ring.core if which else ring.core
        return rows_at(mat * width + core * size, size)

    def mlp_dw_out(mat):
        return pltpu.make_async_copy(dw_attn.at[rows_at(mat * size, size)], dw_mlp.at[mat], dw_sem.at[mat])

    def mlp_dw_copy(mat):
        return remote(part.at[mlp_dw(mat, 1)], dw_attn.at[rows_at(mat * size, size)], dw_send.at[mat], dw_recv.at[mat],
                      ring.sibling)

    def mlp_pair(hop, _):
        with jax.named_scope('mlp_wait'):
            serve_loop('mlp', hop, range(1, far))
        cols = rows_at((2 * hop - 1) * width, 2 * width)

        def body(t, _):
            here = rows_at(t * big, big)
            act, d_pre = mlp_hidden(here, cols)
            acc_a[here, :] += dot_nn(act, w2[cols, :])
            acc_b[here, :] += dot_nn(d_pre, w1[cols, :])
            serve_loop('mlp', hop, range(1, far), t)
            return 0

        with jax.named_scope('mlp_pair'):
            lax.fori_loop(0, n_bigs, body, 0)

        @pl.when(hop == 1)
        def _():
            for mat in range(2):
                mlp_dw_copy(mat).start()

        return 0

    lax.fori_loop(1, far, mlp_pair, 0)

    def out_copy(which, t):
        return pltpu.make_async_copy((acc_a, acc_b)[which].at[rows_at(t * big, big)], hbm_rows((x2, dx1)[which], t * big, big),
                                     out_sem.at[which, t])

    def sib_copy(which, t):
        here = rows_at(t * big, big)
        dst = (hbm_rows(x2, t * big, big), hbm_rows(dx1, t * big, big), x1_sib.at[here], dx2_sib.at[here])[which]
        return remote((acc_a, acc_b)[which % 2].at[here], dst, sib_send.at[which, t], sib_recv.at[which, t], ring.sibling)

    def stage_copy(which, src, t):
        return pltpu.make_async_copy(hbm_rows(src, t * big, big), stage.at[which], stage_sem.at[which])

    with jax.named_scope('mlp_wait'):
        plan['last', -1]()
    for mat in range(2):
        mlp_dw_copy(mat).wait_send()
        mlp_dw_copy(mat).wait_recv()
        mine = rows_at(mat * size, size)
        dw_attn[mine, :] = dw_attn[mine, :] + part[mlp_dw(mat, 0), :]
        mlp_dw_out(mat).start()

    mlp_ins = (y1, y2, dy1)

    def mlp_far(t):
        here = rows_at(t * big, big)
        cols = rows_at((2 * far - 1) * width, width)
        act, d_pre = mlp_hidden(here, cols)
        acc_a[here, :] += dot_nn(act, w2[cols, :])
        acc_b[here, :] += dot_nn(d_pre, w1[cols, :])

    def mlp_ends(t):
        here = rows_at(t * big, big)
        for which, src in enumerate(mlp_ins):
            stage_copy(which, src, t).wait()
        x = stage[1] - acc_a[here, :]
        d = stage[2] + rms_back(stage[0], acc_b[here, :])
        acc_a[here, :] = x
        acc_b[here, :] = d
        norm[here, :] = (x * inv_rms_of(x)).astype(BF16)
        grad[here, :] = d.astype(BF16)

    def mlp_sent(t):
        for which in range(2):
            out_copy(which, t).start()
            sib_copy(which, t).start()

    def start_stage(ins, t):
        for which, src in enumerate(ins):
            stage_copy(which, src, t).start()

    def mlp_last(t, _):
        mlp_ends(t - 1)
        mlp_far(t)
        serve('last', t - 1)
        mlp_sent(t - 1)
        start_stage(mlp_ins, t)
        return 0

    with jax.named_scope('mlp_last'):
        start_stage(mlp_ins, 0)
        mlp_far(0)
        lax.fori_loop(1, n_bigs, mlp_last, 0)
        mlp_ends(n_bigs - 1)
        for mat in range(2):
            mlp_dw_out(mat).wait()
        plan['last', n_bigs - 1]()
        mlp_sent(n_bigs - 1)

    row_pos = lax.broadcasted_iota(jnp.int32, (BLOCK, BLOCK), 0)
    col_pos = lax.broadcasted_iota(jnp.int32, (BLOCK, BLOCK), 1)
    seq = BLOCK // 2
    causal = (col_pos <= row_pos) & ((col_pos < seq) == (row_pos < seq))
    share = CORES * hd
    first_seq = ring.core * (rows_own // seq)

    def masks_of(t):
        out = []
        for block in range(big // BLOCK):
            at = first_seq + t * (big // seq) + 2 * block
            end = jnp.where(col_pos < seq, lens[at], seq + lens[at + 1])
            out.append(causal & (col_pos < end))
        return out

    def attn_pair(t, j, use_f):
        here = rows_at(t * big, big)
        masks = masks_of(t)

        def weights(i):
            r = rows_at((2 * j + i) * share, share)
            return wq[r, :], wkv[r, :], wo[r, :]

        def project(i):
            return attn_projections(norm[here, :], grad[here, :], *weights(i))

        def grad_sum(i, factors):
            q_w, kv_w, _ = weights(i)
            _, dq, d0, d1 = factors
            return dot_nn(dq, q_w) + dot_nn(d0, kv_w) + dot_nn(d1, kv_w)

        first = project(0)
        scores = attn_scores(big, hd, first)
        second = project(1)
        factors = attn_grads(big, hd, first, attn_softmax(hd, scores, masks))
        scores = attn_scores(big, hd, second)
        f = dot_nn(factors[0], weights(0)[2])
        g = grad_sum(0, factors)
        more = attn_grads(big, hd, second, attn_softmax(hd, scores, masks))
        f = f + dot_nn(more[0], weights(1)[2])
        use_f(f)
        return g + grad_sum(1, more), factors

    part[...] = jnp.zeros_like(part)
    own_part = 4 * hd
    mlp.finish()

    def attn_dw(which):
        core = 1 - ring.core if which else ring.core
        return rows_at(core * own_part, own_part)

    def attn_dw_copy():
        return remote(part.at[attn_dw(1)], dw_attn.at[rows_at(0, own_part)], dw_send.at[2], dw_recv.at[2], ring.sibling)

    per_band = w1.shape[1] // hd

    def kept_at(k):
        return slice(k // per_band * big, (k // per_band + 1) * big), slice(k % per_band * hd, (k % per_band + 1) * hd)

    def attn_pairs(j, _):
        with jax.named_scope('attn_wait'):
            serve_loop('attn', j, range(far - 1))

        def body(t, _):
            here = rows_at(t * big, big)

            @pl.when(j == 0)
            def _():
                for which in range(2):
                    out_copy(which, t).wait()
                    sib_copy(which, t).wait_send()
                acc_a[here, :] = jnp.zeros((big, acc_a.shape[1]), F32)
                acc_b[here, :] = jnp.zeros((big, acc_b.shape[1]), F32)

            kept = []
            g, own_factors = attn_pair(t, j, kept.append)
            acc_a[here, :] += kept[0]
            acc_b[here, :] += g
            a, dq, *dkv = own_factors
            for head in range(CORES):
                cols = slice(head * hd, (head + 1) * hd)
                for which, factor in enumerate((dq[:, cols], dkv[head][:, :hd], dkv[head][:, hd:], a[:, cols])):
                    r, c = kept_at(4 * head + which)
                    w1[r, c] = factor

            @pl.when(j == 0)
            def _():
                for head in range(CORES):
                    for which in range(4):
                        r, c = kept_at(4 * head + which)
                        rows = slice(head * own_part + which * hd, head * own_part + (which + 1) * hd)
                        part[rows, :] += dot_tn(w1[r, c], (norm if which < 3 else grad)[here, :])

            serve_loop('attn', j, range(far - 1), t)
            return 0

        with jax.named_scope('attn_pair'):
            lax.fori_loop(0, n_bigs, body, 0)

        @pl.when(j == 1)
        def _():
            attn_dw_copy().start()

        return 0

    lax.fori_loop(0, far - 1, attn_pairs, 0)

    with jax.named_scope('attn_wait'):
        plan['attn3', -1]()
    attn_dw_copy().wait_send()
    attn_dw_copy().wait_recv()
    mine = rows_at(0, own_part)
    dw_attn[mine, :] = dw_attn[mine, :] + part[attn_dw(0), :]

    attn_ins = (y1, x2, dy2)

    def attn_last(t, _):
        here = rows_at(t * big, big)
        start_stage(attn_ins, t)

        def x1_ends(f):
            stage_copy(0, y1, t).wait()
            acc_a[here, :] = stage[0] - (acc_a[here, :] + f)
            sib_copy(2, t).start()

        g, _ = attn_pair(t, far - 1, x1_ends)
        stage_copy(1, x2, t).wait()
        stage_copy(2, dy2, t).wait()
        acc_b[here, :] = stage[2] + rms_back(stage[1], acc_b[here, :] + g)
        sib_copy(3, t).start()
        return 0

    with jax.named_scope('attn_last'):
        lax.fori_loop(0, n_bigs, attn_last, 0)

    attn.finish()

    def drain(t, _):
        for which in range(2, 4):
            sib_copy(which, t).wait_send()
        for which in range(4):
            sib_copy(which, t).wait_recv()
        return 0

    with jax.named_scope('drain'):
        lax.fori_loop(0, n_bigs, drain, 0)


def block_back(n_tp, paired, y1, y2, dy1, dy2, lens, w1_own, w2_own, wq_in, wk_in, wv_in, wo_own, tile=256, big=512):
    tokens, d = y1.shape
    size, hd = w1_own.shape[0], wo_own.shape[0]
    chips = n_tp // CORES
    hops = chips // 2
    half = tokens // CORES
    n_bigs = half // big
    hidden, heads = n_tp * size, n_tp * hd
    hbm = pl.BlockSpec(memory_space=pl.ANY)
    dma = pltpu.SemaphoreType.DMA
    flops = 8 * half * d * hidden + 14 * half * d * heads
    part_rows = max(4 * size, CORES * 4 * hd)
    own_rows = max(2 * size, 4 * hd)

    def ring_sems(pieces):
        return [dma((pieces, 2, hops))] * 2 + [dma((pieces, chips))] * 4 + [dma((pieces,))]

    return pl.pallas_call(
        functools.partial(block_kernel, n_tp, paired, tile, big),
        name='block_back',
        out_shape=[jax.ShapeDtypeStruct(shape, F32) for shape in ((half, d), (tokens, d), (tokens, d), (half, d), (2, size, d))]
        + [pltpu.VMEM((rows, d), F32) for rows in (own_rows, half, half)],
        in_specs=[hbm] * 4 + [pl.BlockSpec(memory_space=pltpu.SMEM)] + [hbm] * 6,
        out_specs=[hbm] * 5 + [pl.BlockSpec(memory_space=pltpu.VMEM)] * 3,
        scratch_shapes=[
            pltpu.VMEM((hidden, d), BF16), pltpu.VMEM((hidden, d), BF16),
            pltpu.VMEM((heads, d), BF16), pltpu.VMEM((heads, d), BF16), pltpu.VMEM((heads, d), BF16),
            pltpu.VMEM((half, d), BF16), pltpu.VMEM((half, d), BF16),
            pltpu.VMEM((part_rows, d), F32),
            pltpu.VMEM((3, big, d), F32),
            *ring_sems(2), *ring_sems(4),
            dma((2, 3)), dma((3,)), dma((2, n_bigs)), dma((4, n_bigs)), dma((4, n_bigs)), dma((3,)), dma((3,)), dma((2,)), dma((2,)),
        ],
        compiler_params=pltpu.CompilerParams(collective_id=0, has_side_effects=True, vmem_limit_bytes=67043328 - 4 * d * (2 * half + own_rows)),
        cost_estimate=pl.CostEstimate(flops=flops, bytes_accessed=10 * tokens * d * 4, transcendentals=half * hidden),
    )(y1, y2, dy1, dy2, lens, w1_own, w2_own, wq_in, wk_in, wv_in, wo_own)


def settle_kernel(chunk, depth, *refs):
    x1_sib, x2_in, dx1_in, dx2_sib, mlp_in, attn_buf, x1_own, dx2_own = refs[:8]
    x1, x2, dx1, dx2, *grads_out = refs[8:18]
    buf, mlp_buf, turned, read_sem, write_sem, small_sem, own_sem = refs[18:]
    tokens, half, hd = x2.shape[0], x1_own.shape[0], turned.shape[2]
    core = lax.rem(lax.axis_index('tp'), CORES)
    jobs = []
    for first in range(0, tokens, chunk):
        jobs += [(x2_in, first, x2, first), (dx1_in, first, dx1, first)]
    for first in range(0, half, chunk):
        jobs += [(x1_sib, first, x1, (1 - core) * half + first), (dx2_sib, first, dx2, (1 - core) * half + first)]

    def read(k):
        src, first, _, _ = jobs[k]
        return pltpu.make_async_copy(src.at[rows_at(first, chunk)], buf.at[k % depth], read_sem.at[k % depth])

    def write(k):
        _, _, dst, first = jobs[k]
        return pltpu.make_async_copy(buf.at[k % depth], dst.at[rows_at(first, chunk)], write_sem.at[k % depth])

    own = [pltpu.make_async_copy(src, dst.at[rows_at(core * half, half)], own_sem.at[i])
           for i, (src, dst) in enumerate(((x1_own, x1), (dx2_own, dx2)))]
    small_writes = [pltpu.make_async_copy(src, dst, small_sem.at[i]) for i, (src, dst) in enumerate(
        [(turned.at[i], grads_out[i]) for i in range(3)] + [(attn_buf.at[rows_at(3 * hd, hd)], grads_out[3]),
                                                            (mlp_buf.at[0], grads_out[4]), (mlp_buf.at[1], grads_out[5])])]
    mlp_read = pltpu.make_async_copy(mlp_in, mlp_buf, small_sem.at[6])
    mlp_read.start()
    for k in range(min(depth, len(jobs))):
        read(k).start()
    for copy in own:
        copy.start()
    for i in range(3):
        turned[i] = attn_buf[i * hd:(i + 1) * hd, :].T
    mlp_read.wait()
    for copy in small_writes:
        copy.start()
    lag = depth // 2
    for k in range(len(jobs)):
        read(k).wait()
        write(k).start()
        if k >= lag:
            write(k - lag).wait()
            if k - lag + depth < len(jobs):
                read(k - lag + depth).start()
    for k in range(max(len(jobs) - lag, 0), len(jobs)):
        write(k).wait()
    for copy in own + small_writes:
        copy.wait()


def settle(hd, x1_sib, x2, dx1, dx2_sib, dw_mlp, dw_attn, x1_own, dx2_own, chunk=256, depth=24):
    tokens, d = x2.shape
    size = dw_mlp.shape[1]
    hbm, vmem = pl.BlockSpec(memory_space=pl.ANY), pl.BlockSpec(memory_space=pltpu.VMEM)
    dma = pltpu.SemaphoreType.DMA
    grads = [(d, hd)] * 3 + [(hd, d), (size, d), (size, d)]
    return pl.pallas_call(
        functools.partial(settle_kernel, chunk, depth),
        name='settle',
        out_shape=[jax.ShapeDtypeStruct((tokens, d), F32)] * 4 + [jax.ShapeDtypeStruct(shape, F32) for shape in grads],
        in_specs=[hbm] * 5 + [vmem] * 3,
        out_specs=[hbm] * 10,
        scratch_shapes=[
            pltpu.VMEM((depth, chunk, d), F32), pltpu.VMEM((2, size, d), F32), pltpu.VMEM((3, d, hd), F32),
            dma((depth,)), dma((depth,)), dma((7,)), dma((2,)),
        ],
        compiler_params=pltpu.CompilerParams(vmem_limit_bytes=36 * 2 ** 20),
        cost_estimate=pl.CostEstimate(flops=0, bytes_accessed=8 * tokens * d * 4, transcendentals=0),
    )(x1_sib, x2, dx1, dx2_sib, pltpu.with_memory_space_constraint(dw_mlp, pltpu.HBM),
      *(pltpu.with_memory_space_constraint(ref, pltpu.VMEM) for ref in (dw_attn, x1_own, dx2_own)))


def layer_back(carry, lens, layer_w, n_tp, paired):
    w_query, w_key, w_value, w_out, w_up, w_down = layer_w
    d, _, hd = w_query.shape
    heads = [w.reshape(d, hd) for w in (w_query, w_key, w_value)]
    *acts, dw_mlp, dw_attn, x1_own, dx2_own = block_back(n_tp, paired, *carry, lens, w_up.T, w_down, *heads,
                                                         w_out.reshape(hd, d))
    *carry, dwq, dwk, dwv, dwo, dw1, dw2 = settle(hd, *acts, dw_mlp, dw_attn, x1_own, dx2_own)
    grads = (dwq.reshape(w_query.shape), dwk.reshape(w_key.shape), dwv.reshape(w_value.shape), dwo.reshape(w_out.shape),
             dw1.T, dw2)
    return tuple(carry), grads


def solution(mesh):
    act_spec = P('dp', None, None)
    w_specs = (P(None, None, 'tp', None), P(None, None, 'tp', None), P(None, None, 'tp', None),
               P(None, 'tp', None, None), P(None, None, 'tp'), P(None, 'tp', None))
    g_specs = (P('dp', None, 'tp', None), P('dp', None, 'tp', None), P('dp', None, 'tp', None),
               P('dp', 'tp', None, None), P('dp', None, 'tp'), P('dp', 'tp', None))
    n_tp = mesh.shape['tp']
    paired = mesh.shape['dp'] % 2 == 0

    def local_fn(y_one, y_two, dy_one, dy_two, seq_lens, *weights):
        n_seqs, seq_len, d = y_one.shape
        carry = tuple(act.reshape(n_seqs * seq_len, d) for act in (y_one, y_two, dy_one, dy_two))
        n_layers = weights[0].shape[0]
        grads_by_layer = [None] * n_layers
        for layer in reversed(range(n_layers)):
            (x1, x2, dx1, dx2), grads_by_layer[layer] = layer_back(carry, seq_lens, [w[layer] for w in weights], n_tp, paired)
            carry = (x1, x2, dx1, dx2)
        stacked = tuple(jnp.stack(grads) for grads in zip(*grads_by_layer))
        return tuple(act.reshape(n_seqs, seq_len, d) for act in carry) + stacked

    return jax.shard_map(local_fn, mesh=mesh,
                         in_specs=(act_spec,) * 4 + (P('dp'),) + w_specs,
                         out_specs=(act_spec,) * 4 + g_specs,
                         check_vma=False)
```

```python
import functools

import jax
import jax.numpy as jnp
from jax import lax
from jax.experimental import pallas as pl
from jax.experimental.pallas import tpu as pltpu
from jax.sharding import PartitionSpec as P

F32 = jnp.float32
BF16 = jnp.bfloat16
EPS = 1e-5
MASK_VALUE = -1e30
CORES = 2
BLOCK = 128
GELU_A = 0.7978845608028654
GELU_B = 0.044715
LOG2_E = 1.4426950408889634


def dot_nt(a, b):
    return lax.dot_general(a, b, (((1,), (1,)), ((), ())), preferred_element_type=F32)


def dot_nn(a, b):
    return lax.dot_general(a, b, (((1,), (0,)), ((), ())), preferred_element_type=F32)


def dot_tn(a, b):
    return lax.dot_general(a, b, (((0,), (0,)), ((), ())), preferred_element_type=F32)


def gelu_and_slope(x):
    sq = x * x
    t = jnp.tanh(GELU_A * (x + GELU_B * (sq * x)))
    half = 0.5 * (1.0 + t)
    slope = half + (0.5 * x) * (1.0 - t * t) * (GELU_A * (1.0 + (3.0 * GELU_B) * sq))
    return x * half, slope


def inv_rms_of(x):
    return lax.rsqrt(jnp.mean(x * x, axis=-1, keepdims=True) + EPS)


def rms_back(x, grad):
    inv = inv_rms_of(x)
    normed = x * inv
    return inv * (grad - normed * jnp.mean(grad * normed, axis=-1, keepdims=True))


def rows_at(start, size):
    return pl.ds(start if isinstance(start, int) else pl.multiple_of(start, 16), size)


def attn_projections(normed, grad, wq, wkv, wo):
    return dot_nt(normed, wq).astype(BF16), dot_nt(normed, wkv).astype(BF16), dot_nt(grad, wo).astype(BF16)


def attn_scores(span, hd, proj):
    q, kv, da = proj
    out = []
    for first in range(0, span, BLOCK):
        r = slice(first, first + BLOCK)
        q_two = jnp.concatenate([q[r, :hd], q[r, hd:]], axis=0)
        da_two = jnp.concatenate([da[r, :hd], da[r, hd:]], axis=0)
        out.append((dot_nt(q_two, kv[r, :hd]), dot_nt(da_two, kv[r, hd:])))
    return out


def attn_softmax(hd, scores, masks):
    scale = hd ** -0.5
    out = []
    for (s, dp), mask in zip(scores, masks):
        s = jnp.where(jnp.concatenate([mask, mask], axis=0), s, MASK_VALUE)
        ex = jnp.exp2((s - jnp.max(s, axis=-1, keepdims=True)) * (scale * LOG2_E))
        p = ex * (1.0 / jnp.sum(ex, axis=-1, keepdims=True))
        ds = (p * (dp - jnp.sum(dp * p, axis=-1, keepdims=True)) * scale).astype(BF16)
        out.append((p.astype(BF16), ds))
    return out


def attn_grads(span, hd, proj, probs):
    q, kv, da = proj
    a, dq, dkv = [], [], ([], [])
    for first, (p, ds) in zip(range(0, span, BLOCK), probs):
        r = slice(first, first + BLOCK)
        two = dot_nn(p, kv[r, hd:]).astype(BF16)
        a.append(jnp.concatenate([two[:BLOCK], two[BLOCK:]], axis=1))
        two = dot_nn(ds, kv[r, :hd]).astype(BF16)
        dq.append(jnp.concatenate([two[:BLOCK], two[BLOCK:]], axis=1))
        for head in range(CORES):
            own, h = slice(head * BLOCK, (head + 1) * BLOCK), slice(head * hd, (head + 1) * hd)
            dkv[head].append(jnp.concatenate([dot_tn(ds[own], q[r, h]).astype(BF16),
                                              dot_tn(p[own], da[r, h]).astype(BF16)], axis=1))
    return tuple(jnp.concatenate(parts, axis=0) for parts in (a, dq, *dkv))


def when_do(condition, step):
    @pl.when(condition)
    def _():
        step()


class Ring:
    def __init__(self, n_tp, paired):
        self.chips = n_tp // CORES
        self.far = self.chips // 2
        me, group = lax.axis_index('tp'), lax.axis_index('dp')
        self.core = lax.rem(me, CORES)
        chip = lax.div(me, CORES)
        up = lax.rem(chip + 1, self.chips) * CORES + self.core
        down = lax.rem(chip + self.chips - 1, self.chips) * CORES + self.core
        self.toward = ({'tp': up}, {'tp': down})
        self.sibling = {'tp': chip * CORES + (1 - self.core)}
        self.paired = paired
        self.parity = lax.rem(group, 2) if paired else 0
        self.partner = {'dp': group + 1 - 2 * self.parity}

    def peers(self):
        return (*self.toward, self.sibling) + ((self.partner,) if self.paired else ())

    def slot(self, hop, way):
        return 2 * hop - 1 if hop == self.far else 2 * hop - 1 + way


def remote(src, dst, send, recv, peer):
    return pltpu.make_async_remote_copy(src_ref=src, dst_ref=dst, send_sem=send, recv_sem=recv,
                                        device_id=peer, device_id_type=pl.DeviceIdType.MESH)


class Shares:
    def __init__(self, ring, refs, rows, ring_rows, sems):
        self.ring, self.refs, self.rows = ring, refs, rows
        self.ring_rows = ring_rows if ring.paired else rows
        self.recv, self.pair_recv, self.d2d_recv, self.sent = sems

    def place(self, piece, slot, kind='all'):
        full, part, first = self.refs[piece]
        low, rows = 0, self.rows
        if kind == 'ring':
            low, rows = self.ring.parity * (self.rows - self.ring_rows), self.ring_rows
        elif kind == 'pair':
            low, rows = self.ring.parity * self.ring_rows, self.rows - self.ring_rows
        return full.at[rows_at((slot * CORES + self.ring.core) * part + first + low, rows)]

    def bundle(self, hop, piece):
        far = self.ring.far
        return () if hop > far else (piece,) if hop == far else (0, 1)

    def hop_copy(self, piece, way, hop):
        slot = 0 if hop == 1 else self.ring.slot(hop - 1, way)
        return remote(self.place(piece, slot, 'ring'), self.place(piece, self.ring.slot(hop, way), 'ring'),
                      self.sent.at[0], self.recv.at[piece, way, hop - 1], self.ring.toward[way])

    def pair_copy(self, piece, slot):
        ref = self.place(piece, slot, 'pair')
        return remote(ref, ref, self.sent.at[1], self.pair_recv.at[piece, slot], self.ring.partner)

    def sibling_copy(self, piece, slot):
        ref = self.place(piece, slot)
        return remote(ref, ref, self.sent.at[2], self.d2d_recv.at[piece, slot], self.ring.sibling)

    def start(self, piece):
        for way in self.bundle(1, piece):
            self.hop_copy(piece, way, 1).start()
        self.sibling_copy(piece, 0).start()

    def wait_own(self):
        for piece in range(2):
            self.sibling_copy(piece, 0).wait_recv()

    def take_ring(self, hop, piece):
        for way in self.bundle(hop, piece):
            self.hop_copy(piece, way, hop).wait_recv()
            if way in self.bundle(hop + 1, piece):
                self.hop_copy(piece, way, hop + 1).start()
            if self.ring.paired:
                self.pair_copy(piece, self.ring.slot(hop, way)).start()

    def take_pair(self, hop, piece):
        for way in self.bundle(hop, piece):
            if self.ring.paired:
                self.pair_copy(piece, self.ring.slot(hop, way)).wait_recv()
            self.sibling_copy(piece, self.ring.slot(hop, way)).start()

    def take_sibling(self, hop):
        for piece in range(2):
            for way in self.bundle(hop, piece):
                self.sibling_copy(piece, self.ring.slot(hop, way)).wait_recv()

    def finish(self, like):
        ring = self.ring
        counts = ((2 * (ring.chips - 1), self.ring_rows), (2 * (ring.chips - 1), self.rows - self.ring_rows),
                  (2 * ring.chips, self.rows))
        for kind, (copies, rows) in enumerate(counts):
            if copies * rows:
                ref = like.at[pl.ds(0, copies * rows)]
                pltpu.make_async_copy(ref, ref, self.sent.at[kind]).wait()


def block_kernel(n_tp, paired, tile, big, y1, y2, dy1, dy2, lens_in, w1_own, w2_own, wq_in, wk_in, wv_in, wo_own,
                 x1_sib, x2, dx1, dx2_sib, dw_mlp, dw_attn, acc_a, acc_b,
                 lens, w1, w2, wa, norm, grad, part, stage,
                 mlp_recv, mlp_pair_recv, mlp_d2d_recv, mlp_sent, attn_recv, attn_pair_recv, attn_d2d_recv, attn_sent,
                 norm_sem, stage_sem, out_sem, sib_send, sib_recv, dw_send, dw_recv, dw_sem, local_sem):
    ring = Ring(n_tp, paired)
    far = ring.far
    size = w1_own.shape[0]
    hd = wo_own.shape[0]
    rows_own = norm.shape[0]
    base = ring.core * rows_own
    n_tiles, n_bigs = rows_own // tile, rows_own // big

    barrier = pltpu.get_barrier_semaphore()
    for peer in ring.peers():
        pl.semaphore_signal(barrier, inc=1, device_id=peer, device_id_type=pl.DeviceIdType.MESH)

    a_part = 3 * hd
    mlp = Shares(ring, ((w1, size, 0), (w2, size, 0)), size, 2 * size // 3,
                 (mlp_recv, mlp_pair_recv, mlp_d2d_recv, mlp_sent))
    attn = Shares(ring, ((wa, a_part, 0), (wa, a_part, a_part // 2)), a_part // 2, hd,
                  (attn_recv, attn_pair_recv, attn_d2d_recv, attn_sent))

    def hbm_rows(ref, first, rows):
        return ref.at[rows_at(base + first, rows)]

    depth = stage.shape[0]

    def norm_fetch(which, t):
        slot = lax.rem(t, depth)
        return pltpu.make_async_copy(hbm_rows((y1, dy2)[which], t * tile, tile), stage.at[slot, rows_at(which * tile, tile)],
                                     norm_sem.at[which, slot])

    for t in range(min(depth, n_tiles)):
        for which in range(2):
            norm_fetch(which, t).start()

    depth_w = w1.shape[1]
    flat = [(slice(wa.shape[0] - (2 - i) * depth_w, wa.shape[0] - (1 - i) * depth_w), slice(0, hd)) for i in range(2)]
    own_a = ring.core * a_part

    def local_copy(i, src=None):
        src = (w1_own, w2_own, wo_own, lens_in, wq_in, src)[i]
        dst = (mlp.place(0, 0), mlp.place(1, 0), wa.at[rows_at(own_a + 2 * hd, hd)], lens, wa.at[flat[0]], wa.at[flat[1]])[i]
        return pltpu.make_async_copy(src, dst, local_sem.at[i])

    for i in range(5):
        local_copy(i).start()
    when_do(ring.core == 0, lambda: local_copy(5, wk_in).start())
    when_do(ring.core == 1, lambda: local_copy(5, wv_in).start())
    local_copy(0).wait()
    local_copy(1).wait()
    pl.semaphore_wait(barrier, len(ring.peers()))
    mlp.start(0)

    def norm_body(t, _):
        here = rows_at(t * tile, tile)
        slot = lax.rem(t, depth)
        for which in range(2):
            norm_fetch(which, t).wait()
        y = stage[slot, 0:tile, :]
        norm[here, :] = (y * inv_rms_of(y)).astype(BF16)
        grad[here, :] = stage[slot, tile:2 * tile, :].astype(BF16)

        @pl.when(t + depth < n_tiles)
        def _():
            for which in range(2):
                norm_fetch(which, t + depth).start()

        when_do(t == n_tiles // 3, lambda: mlp.start(1))
        return 0

    lax.fori_loop(0, n_tiles, norm_body, 0)

    def mlp_hidden(here, cols):
        pre = dot_nt(norm[here, :], w1[cols, :])
        d_act = dot_nt(grad[here, :], w2[cols, :])
        act, slope = gelu_and_slope(pre)
        return act.astype(BF16), (d_act * slope).astype(BF16)

    def r(shares, hop, piece):
        with jax.named_scope('ring'):
            shares.take_ring(hop, piece)

    def y(shares, hop, piece):
        with jax.named_scope('pair'):
            shares.take_pair(hop, piece)

    def both(step, shares, hop):
        step(shares, hop, 0)
        step(shares, hop, 1)

    plan = {
        ('own', 0): lambda: r(mlp, 1, 0),
        ('own', 1): lambda: r(mlp, 1, 1),
        ('mlp1', -1): lambda: (y(mlp, 1, 0), r(mlp, 2, 0), y(mlp, 1, 1), mlp.take_sibling(1)),
        ('mlp1', 0): lambda: (r(mlp, 2, 1), y(mlp, 2, 0)),
        ('mlp1', 1): lambda: r(mlp, 3, 0),
        ('mlp1', 2): lambda: y(mlp, 2, 1),
        ('mlp2', -1): lambda: (r(mlp, 3, 1), attn.start(0), attn.start(1), mlp.take_sibling(2)),
        ('mlp2', 0): lambda: y(mlp, 3, 0),
        ('mlp2', 1): lambda: both(r, mlp, 4),
        ('mlp2', 2): lambda: y(mlp, 3, 1),
        ('mlp3', -1): lambda: mlp.take_sibling(3),
        ('mlp3', 0): lambda: (both(y, mlp, 4), r(attn, 1, 0)),
        ('mlp3', 1): lambda: r(attn, 1, 1),
        ('mlp3', 2): lambda: (y(attn, 1, 0), r(attn, 2, 0)),
        ('last', -1): lambda: mlp.take_sibling(4),
        ('last', 0): lambda: (y(attn, 1, 1), r(attn, 2, 1)),
        ('last', 1): lambda: (y(attn, 2, 0), r(attn, 3, 0)),
        ('last', 2): lambda: y(attn, 2, 1),
        ('attn0', -1): lambda: (attn.wait_own(), attn.take_sibling(1)),
        ('attn0', 0): lambda: (r(attn, 3, 1), y(attn, 3, 0)),
        ('attn0', 1): lambda: (both(r, attn, 4), y(attn, 3, 1)),
        ('attn1', -1): lambda: attn.take_sibling(2),
        ('attn1', 0): lambda: both(y, attn, 4),
        ('attn2', -1): lambda: attn.take_sibling(3),
        ('attn3', -1): lambda: attn.take_sibling(4),
    }

    def serve(phase, t):
        for (name, at), step in plan.items():
            if name == phase and at >= 0:
                when_do(t == at, step)

    def serve_loop(kind, index, indices, t=None):
        for i in indices:
            if t is None and (f'{kind}{i}', -1) in plan:
                when_do(index == i, plan[f'{kind}{i}', -1])
            for at in range(n_bigs if t is not None else 0):
                if (f'{kind}{i}', at) in plan:
                    when_do((index == i) & (t == at), plan[f'{kind}{i}', at])

    width = CORES * size
    mlp.wait_own()
    part[...] = jnp.zeros_like(part)

    def mlp_own(t, _):
        here = rows_at(t * big, big)
        cols = rows_at(0, width)
        act, d_pre = mlp_hidden(here, cols)
        acc_a[here, :] = dot_nn(act, w2[cols, :])
        acc_b[here, :] = dot_nn(d_pre, w1[cols, :])
        part[0:width, :] += dot_tn(d_pre, norm[here, :])
        part[width:2 * width, :] += dot_tn(act, grad[here, :])
        serve('own', t)
        return 0

    with jax.named_scope('mlp_own'):
        lax.fori_loop(0, n_bigs, mlp_own, 0)

    eye = (lax.broadcasted_iota(jnp.int32, (hd, hd), 0) == lax.broadcasted_iota(jnp.int32, (hd, hd), 1)).astype(BF16)
    for i in range(2):
        local_copy(4 + i, wk_in).wait()
        wa[rows_at(own_a + i * hd, hd), :] = dot_nt(eye, wa[flat[i]]).astype(BF16)
    local_copy(2).wait()
    local_copy(3).wait()

    def mlp_dw(mat, which):
        core = 1 - ring.core if which else ring.core
        return rows_at(mat * width + core * size, size)

    def mlp_dw_out(mat):
        return pltpu.make_async_copy(dw_attn.at[rows_at(mat * size, size)], dw_mlp.at[mat], dw_sem.at[mat])

    def mlp_dw_copy(mat):
        return remote(part.at[mlp_dw(mat, 1)], dw_attn.at[rows_at(mat * size, size)], dw_send.at[mat], dw_recv.at[mat],
                      ring.sibling)

    def mlp_pair(hop, _):
        with jax.named_scope('mlp_wait'):
            serve_loop('mlp', hop, range(1, far))
        cols = rows_at((2 * hop - 1) * width, 2 * width)

        def body(t, _):
            here = rows_at(t * big, big)
            act, d_pre = mlp_hidden(here, cols)
            acc_a[here, :] += dot_nn(act, w2[cols, :])
            acc_b[here, :] += dot_nn(d_pre, w1[cols, :])
            serve_loop('mlp', hop, range(1, far), t)
            return 0

        with jax.named_scope('mlp_pair'):
            lax.fori_loop(0, n_bigs, body, 0)

        @pl.when(hop == 1)
        def _():
            for mat in range(2):
                mlp_dw_copy(mat).start()

        return 0

    lax.fori_loop(1, far, mlp_pair, 0)

    def out_copy(which, t):
        return pltpu.make_async_copy((acc_a, acc_b)[which].at[rows_at(t * big, big)], hbm_rows((x2, dx1)[which], t * big, big),
                                     out_sem.at[which, t])

    def sib_copy(which, t):
        here = rows_at(t * big, big)
        dst = (hbm_rows(x2, t * big, big), hbm_rows(dx1, t * big, big), x1_sib.at[here], dx2_sib.at[here])[which]
        return remote((acc_a, acc_b)[which % 2].at[here], dst, sib_send.at[which, t], sib_recv.at[which, t], ring.sibling)

    def stage_copy(which, src, t):
        return pltpu.make_async_copy(hbm_rows(src, t * big, big), stage.at[which], stage_sem.at[which])

    with jax.named_scope('mlp_wait'):
        plan['last', -1]()
    for mat in range(2):
        mlp_dw_copy(mat).wait_send()
        mlp_dw_copy(mat).wait_recv()
        mine = rows_at(mat * size, size)
        dw_attn[mine, :] = dw_attn[mine, :] + part[mlp_dw(mat, 0), :]
        mlp_dw_out(mat).start()

    def start_stage(ins, t):
        for which, src in enumerate(ins):
            stage_copy(which, src, t).start()

    mlp_ins = (y1, y2, dy1)

    def mlp_last(t, _):
        here = rows_at(t * big, big)
        cols = rows_at((2 * far - 1) * width, width)
        start_stage(mlp_ins, t)
        act, d_pre = mlp_hidden(here, cols)
        acc_a[here, :] += dot_nn(act, w2[cols, :])
        acc_b[here, :] += dot_nn(d_pre, w1[cols, :])
        for which, src in enumerate(mlp_ins):
            stage_copy(which, src, t).wait()
        x = stage[1] - acc_a[here, :]
        d = stage[2] + rms_back(stage[0], acc_b[here, :])
        acc_a[here, :] = x
        acc_b[here, :] = d
        norm[here, :] = (x * inv_rms_of(x)).astype(BF16)
        grad[here, :] = d.astype(BF16)

        @pl.when(t == n_bigs - 1)
        def _():
            for mat in range(2):
                mlp_dw_out(mat).wait()

        serve('last', t)
        for which in range(2):
            out_copy(which, t).start()
            sib_copy(which, t).start()
        return 0

    with jax.named_scope('mlp_last'):
        lax.fori_loop(0, n_bigs, mlp_last, 0)

    row_pos = lax.broadcasted_iota(jnp.int32, (BLOCK, BLOCK), 0)
    col_pos = lax.broadcasted_iota(jnp.int32, (BLOCK, BLOCK), 1)
    seq = BLOCK // 2
    causal = (col_pos <= row_pos) & ((col_pos < seq) == (row_pos < seq))
    first_seq = ring.core * (rows_own // seq)

    def masks_of(t):
        out = []
        for block in range(big // BLOCK):
            at = first_seq + t * (big // seq) + 2 * block
            end = jnp.where(col_pos < seq, lens[at], seq + lens[at + 1])
            out.append(causal & (col_pos < end))
        return out

    def attn_pair(t, j, use_f):
        here = rows_at(t * big, big)
        masks = masks_of(t)

        def weights(i):
            first = (2 * j + i) * CORES * a_part
            return [jnp.concatenate([wa[rows_at(first + core * a_part + which * hd, hd), :] for core in range(CORES)], axis=0)
                    for which in range(3)]

        def project(i):
            return attn_projections(norm[here, :], grad[here, :], *weights(i))

        def grad_sum(i, factors):
            q_w, kv_w, _ = weights(i)
            _, dq, d0, d1 = factors
            return dot_nn(dq, q_w) + dot_nn(d0, kv_w) + dot_nn(d1, kv_w)

        first = project(0)
        scores = attn_scores(big, hd, first)
        second = project(1)
        factors = attn_grads(big, hd, first, attn_softmax(hd, scores, masks))
        scores = attn_scores(big, hd, second)
        f = dot_nn(factors[0], weights(0)[2])
        g = grad_sum(0, factors)
        more = attn_grads(big, hd, second, attn_softmax(hd, scores, masks))
        f = f + dot_nn(more[0], weights(1)[2])
        use_f(f)
        return g + grad_sum(1, more), factors

    part[...] = jnp.zeros_like(part)
    own_part = 4 * hd
    mlp.finish(w1)

    def attn_dw(which):
        core = 1 - ring.core if which else ring.core
        return rows_at(core * own_part, own_part)

    def attn_dw_copy():
        return remote(part.at[attn_dw(1)], dw_attn.at[rows_at(0, own_part)], dw_send.at[2], dw_recv.at[2], ring.sibling)

    per_band = w1.shape[1] // hd

    def kept_at(k):
        return slice(k // per_band * big, (k // per_band + 1) * big), slice(k % per_band * hd, (k % per_band + 1) * hd)

    def attn_pairs(j, _):
        with jax.named_scope('attn_wait'):
            serve_loop('attn', j, range(far - 1))

        def body(t, _):
            here = rows_at(t * big, big)

            @pl.when(j == 0)
            def _():
                for which in range(2):
                    out_copy(which, t).wait()
                    sib_copy(which, t).wait_send()
                acc_a[here, :] = jnp.zeros((big, acc_a.shape[1]), F32)
                acc_b[here, :] = jnp.zeros((big, acc_b.shape[1]), F32)

            kept = []
            g, own_factors = attn_pair(t, j, kept.append)
            acc_a[here, :] += kept[0]
            acc_b[here, :] += g
            a, dq, *dkv = own_factors
            for head in range(CORES):
                cols = slice(head * hd, (head + 1) * hd)
                for which, factor in enumerate((dq[:, cols], dkv[head][:, :hd], dkv[head][:, hd:], a[:, cols])):
                    r, c = kept_at(4 * head + which)
                    w1[r, c] = factor

            @pl.when(j == 0)
            def _():
                for head in range(CORES):
                    for which in range(4):
                        r, c = kept_at(4 * head + which)
                        rows = slice(head * own_part + which * hd, head * own_part + (which + 1) * hd)
                        part[rows, :] += dot_tn(w1[r, c], (norm if which < 3 else grad)[here, :])

            serve_loop('attn', j, range(far - 1), t)
            return 0

        with jax.named_scope('attn_pair'):
            lax.fori_loop(0, n_bigs, body, 0)

        @pl.when(j == 1)
        def _():
            attn_dw_copy().start()

        return 0

    lax.fori_loop(0, far - 1, attn_pairs, 0)

    with jax.named_scope('attn_wait'):
        plan['attn3', -1]()
    attn_dw_copy().wait_send()
    attn_dw_copy().wait_recv()
    mine = rows_at(0, own_part)
    dw_attn[mine, :] = dw_attn[mine, :] + part[attn_dw(0), :]

    attn_ins = (y1, x2, dy2)

    def attn_last(t, _):
        here = rows_at(t * big, big)
        start_stage(attn_ins, t)

        def x1_ends(f):
            stage_copy(0, y1, t).wait()
            acc_a[here, :] = stage[0] - (acc_a[here, :] + f)
            sib_copy(2, t).start()

        g, _ = attn_pair(t, far - 1, x1_ends)
        stage_copy(1, x2, t).wait()
        stage_copy(2, dy2, t).wait()
        acc_b[here, :] = stage[2] + rms_back(stage[1], acc_b[here, :] + g)
        sib_copy(3, t).start()
        return 0

    with jax.named_scope('attn_last'):
        lax.fori_loop(0, n_bigs, attn_last, 0)

    attn.finish(wa)

    def drain(t, _):
        for which in range(2, 4):
            sib_copy(which, t).wait_send()
        for which in range(4):
            sib_copy(which, t).wait_recv()
        return 0

    with jax.named_scope('drain'):
        lax.fori_loop(0, n_bigs, drain, 0)


def block_back(n_tp, paired, y1, y2, dy1, dy2, lens, w1_own, w2_own, wq_in, wk_in, wv_in, wo_own, tile=256, big=512):
    tokens, d = y1.shape
    size, hd = w1_own.shape[0], wo_own.shape[0]
    chips = n_tp // CORES
    hops = chips // 2
    half = tokens // CORES
    n_bigs = half // big
    hidden, heads = n_tp * size, n_tp * hd
    hbm = pl.BlockSpec(memory_space=pl.ANY)
    dma = pltpu.SemaphoreType.DMA
    flops = 8 * half * d * hidden + 14 * half * d * heads
    part_rows = max(4 * size, CORES * 4 * hd)
    own_rows = max(2 * size, 4 * hd)

    ring_sems = [dma((2, 2, hops)), dma((2, chips)), dma((2, chips)), dma((3,))]

    return pl.pallas_call(
        functools.partial(block_kernel, n_tp, paired, tile, big),
        name='block_back',
        out_shape=[jax.ShapeDtypeStruct(shape, F32) for shape in ((half, d), (tokens, d), (tokens, d), (half, d), (2, size, d))]
        + [pltpu.VMEM((rows, d), F32) for rows in (own_rows, half, half)],
        in_specs=[hbm] * 11,
        out_specs=[hbm] * 5 + [pl.BlockSpec(memory_space=pltpu.VMEM)] * 3,
        scratch_shapes=[
            pltpu.SMEM(lens.shape, jnp.int32), pltpu.VMEM((hidden, d), BF16), pltpu.VMEM((hidden, d), BF16),
            pltpu.VMEM((3 * heads, d), BF16),
            pltpu.VMEM((half, d), BF16), pltpu.VMEM((half, d), BF16),
            pltpu.VMEM((part_rows, d), F32),
            pltpu.VMEM((3, big, d), F32),
            *ring_sems, *ring_sems,
            dma((2, 3)), dma((3,)), dma((2, n_bigs)), dma((4, n_bigs)), dma((4, n_bigs)), dma((3,)), dma((3,)), dma((2,)), dma((6,)),
        ],
        compiler_params=pltpu.CompilerParams(collective_id=0, has_side_effects=True, vmem_limit_bytes=67043328 - 4 * d * (2 * half + own_rows)),
        cost_estimate=pl.CostEstimate(flops=flops, bytes_accessed=10 * tokens * d * 4, transcendentals=half * hidden),
    )(y1, y2, dy1, dy2, lens, w1_own, w2_own, wq_in, wk_in, wv_in, wo_own)


def settle_kernel(chunk, depth, *refs):
    x1_sib, x2_in, dx1_in, dx2_sib, mlp_in, attn_buf, x1_own, dx2_own = refs[:8]
    x1, x2, dx1, dx2, *grads_out = refs[8:18]
    buf, mlp_buf, turned, read_sem, write_sem, small_sem, own_sem = refs[18:]
    tokens, half, hd = x2.shape[0], x1_own.shape[0], turned.shape[2]
    core = lax.rem(lax.axis_index('tp'), CORES)
    jobs = []
    for first in range(0, tokens, chunk):
        jobs += [(x2_in, first, x2, first), (dx1_in, first, dx1, first)]
    for first in range(0, half, chunk):
        jobs += [(x1_sib, first, x1, (1 - core) * half + first), (dx2_sib, first, dx2, (1 - core) * half + first)]

    def read(k):
        src, first, _, _ = jobs[k]
        return pltpu.make_async_copy(src.at[rows_at(first, chunk)], buf.at[k % depth], read_sem.at[k % depth])

    def write(k):
        _, _, dst, first = jobs[k]
        return pltpu.make_async_copy(buf.at[k % depth], dst.at[rows_at(first, chunk)], write_sem.at[k % depth])

    own = [pltpu.make_async_copy(src, dst.at[rows_at(core * half, half)], own_sem.at[i])
           for i, (src, dst) in enumerate(((x1_own, x1), (dx2_own, dx2)))]
    small_writes = [pltpu.make_async_copy(src, dst, small_sem.at[i]) for i, (src, dst) in enumerate(
        [(turned.at[i], grads_out[i]) for i in range(3)] + [(attn_buf.at[rows_at(3 * hd, hd)], grads_out[3]),
                                                            (mlp_buf.at[0], grads_out[4]), (mlp_buf.at[1], grads_out[5])])]
    mlp_read = pltpu.make_async_copy(mlp_in, mlp_buf, small_sem.at[6])
    mlp_read.start()
    for k in range(min(depth, len(jobs))):
        read(k).start()
    for copy in own:
        copy.start()
    for i in range(3):
        turned[i] = attn_buf[i * hd:(i + 1) * hd, :].T
    mlp_read.wait()
    for copy in small_writes:
        copy.start()
    lag = depth // 2
    for k in range(len(jobs)):
        read(k).wait()
        write(k).start()
        if k >= lag:
            write(k - lag).wait()
            if k - lag + depth < len(jobs):
                read(k - lag + depth).start()
    for k in range(max(len(jobs) - lag, 0), len(jobs)):
        write(k).wait()
    for copy in own + small_writes:
        copy.wait()


def settle(hd, x1_sib, x2, dx1, dx2_sib, dw_mlp, dw_attn, x1_own, dx2_own, chunk=256, depth=24):
    tokens, d = x2.shape
    size = dw_mlp.shape[1]
    hbm, vmem = pl.BlockSpec(memory_space=pl.ANY), pl.BlockSpec(memory_space=pltpu.VMEM)
    dma = pltpu.SemaphoreType.DMA
    grads = [(d, hd)] * 3 + [(hd, d), (size, d), (size, d)]
    return pl.pallas_call(
        functools.partial(settle_kernel, chunk, depth),
        name='settle',
        out_shape=[jax.ShapeDtypeStruct((tokens, d), F32)] * 4 + [jax.ShapeDtypeStruct(shape, F32) for shape in grads],
        in_specs=[hbm] * 5 + [vmem] * 3,
        out_specs=[hbm] * 10,
        scratch_shapes=[
            pltpu.VMEM((depth, chunk, d), F32), pltpu.VMEM((2, size, d), F32), pltpu.VMEM((3, d, hd), F32),
            dma((depth,)), dma((depth,)), dma((7,)), dma((2,)),
        ],
        compiler_params=pltpu.CompilerParams(vmem_limit_bytes=36 * 2 ** 20),
        cost_estimate=pl.CostEstimate(flops=0, bytes_accessed=8 * tokens * d * 4, transcendentals=0),
    )(x1_sib, x2, dx1, dx2_sib, pltpu.with_memory_space_constraint(dw_mlp, pltpu.HBM),
      *(pltpu.with_memory_space_constraint(ref, pltpu.VMEM) for ref in (dw_attn, x1_own, dx2_own)))


def layer_back(carry, lens, layer_w, n_tp, paired):
    w_query, w_key, w_value, w_out, w_up, w_down = layer_w
    d, _, hd = w_query.shape
    heads = [w.reshape(d, hd) for w in (w_query, w_key, w_value)]
    *acts, dw_mlp, dw_attn, x1_own, dx2_own = block_back(n_tp, paired, *carry, lens, w_up.T, w_down, *heads,
                                                         w_out.reshape(hd, d))
    *carry, dwq, dwk, dwv, dwo, dw1, dw2 = settle(hd, *acts, dw_mlp, dw_attn, x1_own, dx2_own)
    grads = (dwq.reshape(w_query.shape), dwk.reshape(w_key.shape), dwv.reshape(w_value.shape), dwo.reshape(w_out.shape),
             dw1.T, dw2)
    return tuple(carry), grads


def solution(mesh):
    act_spec = P('dp', None, None)
    w_specs = (P(None, None, 'tp', None), P(None, None, 'tp', None), P(None, None, 'tp', None),
               P(None, 'tp', None, None), P(None, None, 'tp'), P(None, 'tp', None))
    g_specs = (P('dp', None, 'tp', None), P('dp', None, 'tp', None), P('dp', None, 'tp', None),
               P('dp', 'tp', None, None), P('dp', None, 'tp'), P('dp', 'tp', None))
    n_tp = mesh.shape['tp']
    paired = mesh.shape['dp'] % 2 == 0

    def local_fn(y_one, y_two, dy_one, dy_two, seq_lens, *weights):
        n_seqs, seq_len, d = y_one.shape
        carry = tuple(act.reshape(n_seqs * seq_len, d) for act in (y_one, y_two, dy_one, dy_two))
        n_layers = weights[0].shape[0]
        grads_by_layer = [None] * n_layers
        for layer in reversed(range(n_layers)):
            (x1, x2, dx1, dx2), grads_by_layer[layer] = layer_back(carry, seq_lens, [w[layer] for w in weights], n_tp, paired)
            carry = (x1, x2, dx1, dx2)
        stacked = tuple(jnp.stack(grads) for grads in zip(*grads_by_layer))
        return tuple(act.reshape(n_seqs, seq_len, d) for act in carry) + stacked

    return jax.shard_map(local_fn, mesh=mesh,
                         in_specs=(act_spec,) * 4 + (P('dp'),) + w_specs,
                         out_specs=(act_spec,) * 4 + g_specs,
                         check_vma=False)
```

```python
import functools
import math

import jax
import jax.numpy as jnp
from jax import lax
from jax.experimental import pallas as pl
from jax.experimental.pallas import tpu as pltpu
from jax.sharding import PartitionSpec as P

F32 = jnp.float32
BF16 = jnp.bfloat16
EPS = 1e-5
MASK_VALUE = -1e30
CORES = 2
BLOCK = 128
GELU_A = 0.7978845608028654
GELU_B = 0.044715
LOG2_E = 1.4426950408889634


def dot_nt(a, b):
    return lax.dot_general(a, b, (((1,), (1,)), ((), ())), preferred_element_type=F32)


def dot_nn(a, b):
    return lax.dot_general(a, b, (((1,), (0,)), ((), ())), preferred_element_type=F32)


def dot_tn(a, b):
    return lax.dot_general(a, b, (((0,), (0,)), ((), ())), preferred_element_type=F32)


def gelu_and_slope(x):
    sq = x * x
    t = jnp.tanh(GELU_A * (x + GELU_B * (sq * x)))
    half = 0.5 * (1.0 + t)
    slope = half + (0.5 * x) * (1.0 - t * t) * (GELU_A * (1.0 + (3.0 * GELU_B) * sq))
    return x * half, slope


def inv_rms_of(x):
    return lax.rsqrt(jnp.mean(x * x, axis=-1, keepdims=True) + EPS)


def rms_back(x, grad):
    inv = inv_rms_of(x)
    normed = x * inv
    return inv * (grad - normed * jnp.mean(grad * normed, axis=-1, keepdims=True))


def rows_at(start, size):
    return pl.ds(start if isinstance(start, int) else pl.multiple_of(start, 16), size)


def attn_projections(normed, grad, wq, wkv, wo):
    return dot_nt(normed, wq).astype(BF16), dot_nt(normed, wkv).astype(BF16), dot_nt(grad, wo).astype(BF16)


def attn_scores(span, hd, proj):
    q, kv, da = proj
    out = []
    for first in range(0, span, BLOCK):
        r = slice(first, first + BLOCK)
        q_two = jnp.concatenate([q[r, :hd], q[r, hd:]], axis=0)
        da_two = jnp.concatenate([da[r, :hd], da[r, hd:]], axis=0)
        out.append((dot_nt(q_two, kv[r, :hd]), dot_nt(da_two, kv[r, hd:])))
    return out


def attn_softmax(hd, scores, masks):
    scale = hd ** -0.5
    out = []
    for (s, dp), mask in zip(scores, masks):
        s = jnp.where(jnp.concatenate([mask, mask], axis=0), s, MASK_VALUE)
        ex = jnp.exp2((s - jnp.max(s, axis=-1, keepdims=True)) * (scale * LOG2_E))
        p = ex * (1.0 / jnp.sum(ex, axis=-1, keepdims=True))
        ds = (p * (dp - jnp.sum(dp * p, axis=-1, keepdims=True)) * scale).astype(BF16)
        out.append((p.astype(BF16), ds))
    return out


def attn_grads(span, hd, proj, probs):
    q, kv, da = proj
    a, dq, dkv = [], [], ([], [])
    for first, (p, ds) in zip(range(0, span, BLOCK), probs):
        r = slice(first, first + BLOCK)
        two = dot_nn(p, kv[r, hd:]).astype(BF16)
        a.append(jnp.concatenate([two[:BLOCK], two[BLOCK:]], axis=1))
        two = dot_nn(ds, kv[r, :hd]).astype(BF16)
        dq.append(jnp.concatenate([two[:BLOCK], two[BLOCK:]], axis=1))
        for head in range(CORES):
            own, h = slice(head * BLOCK, (head + 1) * BLOCK), slice(head * hd, (head + 1) * hd)
            dkv[head].append(jnp.concatenate([dot_tn(ds[own], q[r, h]).astype(BF16),
                                              dot_tn(p[own], da[r, h]).astype(BF16)], axis=1))
    return tuple(jnp.concatenate(parts, axis=0) for parts in (a, dq, *dkv))


def when_do(condition, step):
    @pl.when(condition)
    def _():
        step()


class Ring:
    def __init__(self, n_tp, side):
        self.chips = n_tp // CORES
        self.far = self.chips // 2
        me, group = lax.axis_index('tp'), lax.axis_index('dp')
        self.core = lax.rem(me, CORES)
        chip = lax.div(me, CORES)
        up = lax.rem(chip + 1, self.chips) * CORES + self.core
        down = lax.rem(chip + self.chips - 1, self.chips) * CORES + self.core
        self.toward = ({'tp': up}, {'tp': down})
        self.sibling = {'tp': chip * CORES + (1 - self.core)}
        self.shared = side > 0
        if self.shared:
            over, down = lax.div(group, side), lax.rem(group, side)
            self.parity = lax.rem(over + down, 2)
            self.partners = ({'dp': group + 1 - 2 * lax.rem(down, 2)}, {'dp': group + side * (1 - 2 * lax.rem(over, 2))})

    def peers(self):
        return (*self.toward, self.sibling) + (self.partners if self.shared else ())

    def slot(self, hop, way):
        return 2 * hop - 1 if hop == self.far else 2 * hop - 1 + way


def remote(src, dst, send, recv, peer):
    return pltpu.make_async_remote_copy(src_ref=src, dst_ref=dst, send_sem=send, recv_sem=recv,
                                        device_id=peer, device_id_type=pl.DeviceIdType.MESH)


class Shares:
    def __init__(self, ring, refs, rows, sems):
        self.ring, self.refs, self.rows = ring, refs, rows
        self.recv, self.pair_recv, self.d2d_recv, self.sent = sems

    def place(self, piece, slot, low=0, rows=None):
        full, part, first = self.refs[piece]
        return full.at[rows_at((slot * CORES + self.ring.core) * part + first + low, rows or self.rows)]

    def ring_place(self, piece, slot):
        if not self.ring.shared:
            return self.place(piece, slot)
        return self.place(piece, slot, self.ring.parity * (self.rows // 2), self.rows // 2)

    def bundle(self, hop, piece):
        far = self.ring.far
        return () if hop > far else (piece,) if hop == far else (0, 1)

    def hop_copy(self, piece, way, hop):
        slot = 0 if hop == 1 else self.ring.slot(hop - 1, way)
        return remote(self.ring_place(piece, slot), self.ring_place(piece, self.ring.slot(hop, way)), self.sent.at[0],
                      self.recv.at[piece, way, hop - 1], self.ring.toward[way])

    def pair_copies(self, piece, slot):
        if not self.ring.shared:
            return ()
        quarter = self.rows // 4
        refs = [self.place(piece, slot, self.ring.parity * (self.rows // 2) + i * quarter, quarter) for i in range(2)]
        return [remote(ref, ref, self.sent.at[1], self.pair_recv.at[i, piece, slot], self.ring.partners[i])
                for i, ref in enumerate(refs)]

    def sibling_copy(self, piece, slot):
        ref = self.place(piece, slot)
        return remote(ref, ref, self.sent.at[2], self.d2d_recv.at[piece, slot], self.ring.sibling)

    def start(self, piece):
        for way in self.bundle(1, piece):
            self.hop_copy(piece, way, 1).start()
        self.sibling_copy(piece, 0).start()

    def wait_own(self):
        for piece in range(2):
            self.sibling_copy(piece, 0).wait_recv()

    def take_ring(self, hop, piece):
        for way in self.bundle(hop, piece):
            self.hop_copy(piece, way, hop).wait_recv()
            if way in self.bundle(hop + 1, piece):
                self.hop_copy(piece, way, hop + 1).start()
            for copy in self.pair_copies(piece, self.ring.slot(hop, way)):
                copy.start()

    def take_pair(self, hop, piece):
        for way in self.bundle(hop, piece):
            for copy in self.pair_copies(piece, self.ring.slot(hop, way)):
                copy.wait_recv()
            self.sibling_copy(piece, self.ring.slot(hop, way)).start()

    def take_sibling(self, hop):
        for piece in range(2):
            for way in self.bundle(hop, piece):
                self.sibling_copy(piece, self.ring.slot(hop, way)).wait_recv()

    def finish(self, like):
        ring = self.ring
        hops = 2 * (ring.chips - 1)
        counts = (hops * self.rows // 2, hops * self.rows // 2) if ring.shared else (hops * self.rows, 0)
        for kind, rows in enumerate((*counts, 2 * ring.chips * self.rows)):
            if rows:
                ref = like.at[pl.ds(0, rows)]
                pltpu.make_async_copy(ref, ref, self.sent.at[kind]).wait()


def block_kernel(n_tp, side, tile, big, y1, y2, dy1, dy2, lens_in, w1_own, w2_own, wq_in, wk_in, wv_in, wo_own,
                 x1_sib, x2, dx1, dx2_sib, dw_mlp, dw_attn, acc_a, acc_b,
                 lens, w1, w2, wa, norm, grad, part, stage,
                 mlp_recv, mlp_pair_recv, mlp_d2d_recv, mlp_sent, attn_recv, attn_pair_recv, attn_d2d_recv, attn_sent,
                 norm_sem, stage_sem, out_sem, sib_send, sib_recv, dw_send, dw_recv, dw_sem, local_sem):
    ring = Ring(n_tp, side)
    far = ring.far
    size = w1_own.shape[0]
    hd = wo_own.shape[0]
    rows_own = norm.shape[0]
    base = ring.core * rows_own
    n_tiles, n_bigs = rows_own // tile, rows_own // big

    barrier = pltpu.get_barrier_semaphore()
    for peer in ring.peers():
        pl.semaphore_signal(barrier, inc=1, device_id=peer, device_id_type=pl.DeviceIdType.MESH)

    a_part = 3 * hd
    mlp = Shares(ring, ((w1, size, 0), (w2, size, 0)), size,
                 (mlp_recv, mlp_pair_recv, mlp_d2d_recv, mlp_sent))
    attn = Shares(ring, ((wa, a_part, 0), (wa, a_part, a_part // 2)), a_part // 2,
                  (attn_recv, attn_pair_recv, attn_d2d_recv, attn_sent))

    def hbm_rows(ref, first, rows):
        return ref.at[rows_at(base + first, rows)]

    depth = stage.shape[0]

    def norm_fetch(which, t):
        slot = lax.rem(t, depth)
        return pltpu.make_async_copy(hbm_rows((y1, dy2)[which], t * tile, tile), stage.at[slot, rows_at(which * tile, tile)],
                                     norm_sem.at[which, slot])

    for t in range(min(depth, n_tiles)):
        for which in range(2):
            norm_fetch(which, t).start()

    depth_w = w1.shape[1]
    flat = [(slice(wa.shape[0] - (2 - i) * depth_w, wa.shape[0] - (1 - i) * depth_w), slice(0, hd)) for i in range(2)]
    own_a = ring.core * a_part

    def local_copy(i, src=None):
        src = (w1_own, w2_own, wo_own, lens_in, wq_in, src)[i]
        dst = (mlp.place(0, 0), mlp.place(1, 0), wa.at[rows_at(own_a + 2 * hd, hd)], lens, wa.at[flat[0]], wa.at[flat[1]])[i]
        return pltpu.make_async_copy(src, dst, local_sem.at[i])

    for i in range(5):
        local_copy(i).start()
    when_do(ring.core == 0, lambda: local_copy(5, wk_in).start())
    when_do(ring.core == 1, lambda: local_copy(5, wv_in).start())
    local_copy(0).wait()
    local_copy(1).wait()
    pl.semaphore_wait(barrier, len(ring.peers()))
    mlp.start(0)

    def norm_body(t, _):
        here = rows_at(t * tile, tile)
        slot = lax.rem(t, depth)
        for which in range(2):
            norm_fetch(which, t).wait()
        y = stage[slot, 0:tile, :]
        norm[here, :] = (y * inv_rms_of(y)).astype(BF16)
        grad[here, :] = stage[slot, tile:2 * tile, :].astype(BF16)

        @pl.when(t + depth < n_tiles)
        def _():
            for which in range(2):
                norm_fetch(which, t + depth).start()

        when_do(t == n_tiles // 3, lambda: mlp.start(1))
        return 0

    lax.fori_loop(0, n_tiles, norm_body, 0)

    def mlp_hidden(here, cols):
        pre = dot_nt(norm[here, :], w1[cols, :])
        d_act = dot_nt(grad[here, :], w2[cols, :])
        act, slope = gelu_and_slope(pre)
        return act.astype(BF16), (d_act * slope).astype(BF16)

    def r(shares, hop, piece):
        with jax.named_scope('ring'):
            shares.take_ring(hop, piece)

    def y(shares, hop, piece):
        with jax.named_scope('pair'):
            shares.take_pair(hop, piece)

    def both(step, shares, hop):
        step(shares, hop, 0)
        step(shares, hop, 1)

    plan = {
        ('own', 0): lambda: r(mlp, 1, 0),
        ('own', 1): lambda: r(mlp, 1, 1),
        ('own', 2): lambda: y(mlp, 1, 0),
        ('mlp1', -1): lambda: (r(mlp, 2, 0), y(mlp, 1, 1), mlp.take_sibling(1)),
        ('mlp1', 0): lambda: (r(mlp, 2, 1), y(mlp, 2, 0)),
        ('mlp1', 1): lambda: r(mlp, 3, 0),
        ('mlp1', 2): lambda: (y(mlp, 2, 1), r(mlp, 3, 1)),
        ('mlp2', -1): lambda: mlp.take_sibling(2),
        ('mlp2', 0): lambda: (y(mlp, 3, 0), r(mlp, 4, 0)),
        ('mlp2', 1): lambda: (r(mlp, 4, 1), y(mlp, 3, 1), attn.start(0), attn.start(1)),
        ('mlp2', 2): lambda: y(mlp, 4, 0),
        ('mlp3', -1): lambda: mlp.take_sibling(3),
        ('mlp3', 0): lambda: y(mlp, 4, 1),
        ('mlp3', 1): lambda: r(attn, 1, 0),
        ('mlp3', 2): lambda: r(attn, 1, 1),
        ('last', -1): lambda: mlp.take_sibling(4),
        ('last', 0): lambda: (both(y, attn, 1), r(attn, 2, 0)),
        ('last', 1): lambda: r(attn, 2, 1),
        ('last', 2): lambda: (both(y, attn, 2), r(attn, 3, 0)),
        ('attn0', -1): lambda: (attn.wait_own(), attn.take_sibling(1)),
        ('attn0', 0): lambda: (r(attn, 3, 1), y(attn, 3, 0)),
        ('attn0', 1): lambda: (both(r, attn, 4), y(attn, 3, 1)),
        ('attn1', -1): lambda: attn.take_sibling(2),
        ('attn1', 0): lambda: both(y, attn, 4),
        ('attn2', -1): lambda: attn.take_sibling(3),
        ('attn3', -1): lambda: attn.take_sibling(4),
    }

    def serve(phase, t):
        for (name, at), step in plan.items():
            if name == phase and at >= 0:
                when_do(t == at, step)

    def serve_loop(kind, index, indices, t=None):
        for i in indices:
            if t is None and (f'{kind}{i}', -1) in plan:
                when_do(index == i, plan[f'{kind}{i}', -1])
            for at in range(n_bigs if t is not None else 0):
                if (f'{kind}{i}', at) in plan:
                    when_do((index == i) & (t == at), plan[f'{kind}{i}', at])

    width = CORES * size
    mlp.wait_own()
    part[...] = jnp.zeros_like(part)

    def mlp_own(t, _):
        here = rows_at(t * big, big)
        cols = rows_at(0, width)
        act, d_pre = mlp_hidden(here, cols)
        acc_a[here, :] = dot_nn(act, w2[cols, :])
        acc_b[here, :] = dot_nn(d_pre, w1[cols, :])
        part[0:width, :] += dot_tn(d_pre, norm[here, :])
        part[width:2 * width, :] += dot_tn(act, grad[here, :])
        serve('own', t)
        return 0

    with jax.named_scope('mlp_own'):
        lax.fori_loop(0, n_bigs, mlp_own, 0)

    eye = (lax.broadcasted_iota(jnp.int32, (hd, hd), 0) == lax.broadcasted_iota(jnp.int32, (hd, hd), 1)).astype(BF16)
    for i in range(2):
        local_copy(4 + i, wk_in).wait()
        wa[rows_at(own_a + i * hd, hd), :] = dot_nt(eye, wa[flat[i]]).astype(BF16)
    local_copy(2).wait()
    local_copy(3).wait()

    def mlp_dw(mat, which):
        core = 1 - ring.core if which else ring.core
        return rows_at(mat * width + core * size, size)

    def mlp_dw_out(mat):
        return pltpu.make_async_copy(dw_attn.at[rows_at(mat * size, size)], dw_mlp.at[mat], dw_sem.at[mat])

    def mlp_dw_copy(mat):
        return remote(part.at[mlp_dw(mat, 1)], dw_attn.at[rows_at(mat * size, size)], dw_send.at[mat], dw_recv.at[mat],
                      ring.sibling)

    def mlp_pair(hop, _):
        with jax.named_scope('mlp_wait'):
            serve_loop('mlp', hop, range(1, far))
        cols = rows_at((2 * hop - 1) * width, 2 * width)

        def body(t, _):
            here = rows_at(t * big, big)
            act, d_pre = mlp_hidden(here, cols)
            acc_a[here, :] += dot_nn(act, w2[cols, :])
            acc_b[here, :] += dot_nn(d_pre, w1[cols, :])
            serve_loop('mlp', hop, range(1, far), t)
            return 0

        with jax.named_scope('mlp_pair'):
            lax.fori_loop(0, n_bigs, body, 0)

        @pl.when(hop == 1)
        def _():
            for mat in range(2):
                mlp_dw_copy(mat).start()

        return 0

    lax.fori_loop(1, far, mlp_pair, 0)

    def out_copy(which, t):
        return pltpu.make_async_copy((acc_a, acc_b)[which].at[rows_at(t * big, big)], hbm_rows((x2, dx1)[which], t * big, big),
                                     out_sem.at[which, t])

    def sib_copy(which, t):
        here = rows_at(t * big, big)
        dst = (hbm_rows(x2, t * big, big), hbm_rows(dx1, t * big, big), x1_sib.at[here], dx2_sib.at[here])[which]
        return remote((acc_a, acc_b)[which % 2].at[here], dst, sib_send.at[which, t], sib_recv.at[which, t], ring.sibling)

    def stage_copy(which, src, t):
        return pltpu.make_async_copy(hbm_rows(src, t * big, big), stage.at[which], stage_sem.at[which])

    with jax.named_scope('mlp_wait'):
        plan['last', -1]()
    for mat in range(2):
        mlp_dw_copy(mat).wait_send()
        mlp_dw_copy(mat).wait_recv()
        mine = rows_at(mat * size, size)
        dw_attn[mine, :] = dw_attn[mine, :] + part[mlp_dw(mat, 0), :]
        mlp_dw_out(mat).start()

    def start_stage(ins, t):
        for which, src in enumerate(ins):
            stage_copy(which, src, t).start()

    mlp_ins = (y1, y2, dy1)

    def mlp_last(t, _):
        here = rows_at(t * big, big)
        cols = rows_at((2 * far - 1) * width, width)
        start_stage(mlp_ins, t)
        act, d_pre = mlp_hidden(here, cols)
        acc_a[here, :] += dot_nn(act, w2[cols, :])
        acc_b[here, :] += dot_nn(d_pre, w1[cols, :])
        for which, src in enumerate(mlp_ins):
            stage_copy(which, src, t).wait()
        x = stage[1] - acc_a[here, :]
        d = stage[2] + rms_back(stage[0], acc_b[here, :])
        acc_a[here, :] = x
        acc_b[here, :] = d
        norm[here, :] = (x * inv_rms_of(x)).astype(BF16)
        grad[here, :] = d.astype(BF16)

        @pl.when(t == n_bigs - 1)
        def _():
            for mat in range(2):
                mlp_dw_out(mat).wait()

        serve('last', t)
        for which in range(2):
            out_copy(which, t).start()
            sib_copy(which, t).start()
        return 0

    with jax.named_scope('mlp_last'):
        lax.fori_loop(0, n_bigs, mlp_last, 0)

    row_pos = lax.broadcasted_iota(jnp.int32, (BLOCK, BLOCK), 0)
    col_pos = lax.broadcasted_iota(jnp.int32, (BLOCK, BLOCK), 1)
    seq = BLOCK // 2
    causal = (col_pos <= row_pos) & ((col_pos < seq) == (row_pos < seq))
    first_seq = ring.core * (rows_own // seq)

    def masks_of(t):
        out = []
        for block in range(big // BLOCK):
            at = first_seq + t * (big // seq) + 2 * block
            end = jnp.where(col_pos < seq, lens[at], seq + lens[at + 1])
            out.append(causal & (col_pos < end))
        return out

    def attn_pair(t, j, use_f):
        here = rows_at(t * big, big)
        masks = masks_of(t)

        def weights(i):
            first = (2 * j + i) * CORES * a_part
            return [jnp.concatenate([wa[rows_at(first + core * a_part + which * hd, hd), :] for core in range(CORES)], axis=0)
                    for which in range(3)]

        def project(i):
            return attn_projections(norm[here, :], grad[here, :], *weights(i))

        def grad_sum(i, factors):
            q_w, kv_w, _ = weights(i)
            _, dq, d0, d1 = factors
            return dot_nn(dq, q_w) + dot_nn(d0, kv_w) + dot_nn(d1, kv_w)

        first = project(0)
        scores = attn_scores(big, hd, first)
        second = project(1)
        factors = attn_grads(big, hd, first, attn_softmax(hd, scores, masks))
        scores = attn_scores(big, hd, second)
        f = dot_nn(factors[0], weights(0)[2])
        g = grad_sum(0, factors)
        more = attn_grads(big, hd, second, attn_softmax(hd, scores, masks))
        f = f + dot_nn(more[0], weights(1)[2])
        use_f(f)
        return g + grad_sum(1, more), factors

    part[...] = jnp.zeros_like(part)
    own_part = 4 * hd
    mlp.finish(w1)

    def attn_dw(which):
        core = 1 - ring.core if which else ring.core
        return rows_at(core * own_part, own_part)

    def attn_dw_copy():
        return remote(part.at[attn_dw(1)], dw_attn.at[rows_at(0, own_part)], dw_send.at[2], dw_recv.at[2], ring.sibling)

    per_band = w1.shape[1] // hd

    def kept_at(k):
        return slice(k // per_band * big, (k // per_band + 1) * big), slice(k % per_band * hd, (k % per_band + 1) * hd)

    def attn_pairs(j, _):
        with jax.named_scope('attn_wait'):
            serve_loop('attn', j, range(far - 1))

        def body(t, _):
            here = rows_at(t * big, big)

            @pl.when(j == 0)
            def _():
                for which in range(2):
                    out_copy(which, t).wait()
                    sib_copy(which, t).wait_send()
                acc_a[here, :] = jnp.zeros((big, acc_a.shape[1]), F32)
                acc_b[here, :] = jnp.zeros((big, acc_b.shape[1]), F32)

            kept = []
            g, own_factors = attn_pair(t, j, kept.append)
            acc_a[here, :] += kept[0]
            acc_b[here, :] += g
            a, dq, *dkv = own_factors
            for head in range(CORES):
                cols = slice(head * hd, (head + 1) * hd)
                for which, factor in enumerate((dq[:, cols], dkv[head][:, :hd], dkv[head][:, hd:], a[:, cols])):
                    r, c = kept_at(4 * head + which)
                    w1[r, c] = factor

            @pl.when(j == 0)
            def _():
                for head in range(CORES):
                    for which in range(4):
                        r, c = kept_at(4 * head + which)
                        rows = slice(head * own_part + which * hd, head * own_part + (which + 1) * hd)
                        part[rows, :] += dot_tn(w1[r, c], (norm if which < 3 else grad)[here, :])

            serve_loop('attn', j, range(far - 1), t)
            return 0

        with jax.named_scope('attn_pair'):
            lax.fori_loop(0, n_bigs, body, 0)

        @pl.when(j == 1)
        def _():
            attn_dw_copy().start()

        return 0

    lax.fori_loop(0, far - 1, attn_pairs, 0)

    with jax.named_scope('attn_wait'):
        plan['attn3', -1]()
    attn_dw_copy().wait_send()
    attn_dw_copy().wait_recv()
    mine = rows_at(0, own_part)
    dw_attn[mine, :] = dw_attn[mine, :] + part[attn_dw(0), :]

    attn_ins = (y1, x2, dy2)

    def attn_last(t, _):
        here = rows_at(t * big, big)
        start_stage(attn_ins, t)

        def x1_ends(f):
            stage_copy(0, y1, t).wait()
            acc_a[here, :] = stage[0] - (acc_a[here, :] + f)
            sib_copy(2, t).start()

        g, _ = attn_pair(t, far - 1, x1_ends)
        stage_copy(1, x2, t).wait()
        stage_copy(2, dy2, t).wait()
        acc_b[here, :] = stage[2] + rms_back(stage[1], acc_b[here, :] + g)
        sib_copy(3, t).start()
        return 0

    with jax.named_scope('attn_last'):
        lax.fori_loop(0, n_bigs, attn_last, 0)

    attn.finish(wa)

    def drain(t, _):
        for which in range(2, 4):
            sib_copy(which, t).wait_send()
        for which in range(4):
            sib_copy(which, t).wait_recv()
        return 0

    with jax.named_scope('drain'):
        lax.fori_loop(0, n_bigs, drain, 0)


def block_back(n_tp, side, y1, y2, dy1, dy2, lens, w1_own, w2_own, wq_in, wk_in, wv_in, wo_own, tile=256, big=512):
    tokens, d = y1.shape
    size, hd = w1_own.shape[0], wo_own.shape[0]
    chips = n_tp // CORES
    hops = chips // 2
    half = tokens // CORES
    n_bigs = half // big
    hidden, heads = n_tp * size, n_tp * hd
    hbm = pl.BlockSpec(memory_space=pl.ANY)
    dma = pltpu.SemaphoreType.DMA
    flops = 8 * half * d * hidden + 14 * half * d * heads
    part_rows = max(4 * size, CORES * 4 * hd)
    own_rows = max(2 * size, 4 * hd)

    ring_sems = [dma((2, 2, hops)), dma((2, 2, chips)), dma((2, chips)), dma((3,))]

    return pl.pallas_call(
        functools.partial(block_kernel, n_tp, side, tile, big),
        name='block_back',
        out_shape=[jax.ShapeDtypeStruct(shape, F32) for shape in ((half, d), (tokens, d), (tokens, d), (half, d), (2, size, d))]
        + [pltpu.VMEM((rows, d), F32) for rows in (own_rows, half, half)],
        in_specs=[hbm] * 11,
        out_specs=[hbm] * 5 + [pl.BlockSpec(memory_space=pltpu.VMEM)] * 3,
        scratch_shapes=[
            pltpu.SMEM(lens.shape, jnp.int32), pltpu.VMEM((hidden, d), BF16), pltpu.VMEM((hidden, d), BF16),
            pltpu.VMEM((3 * heads, d), BF16),
            pltpu.VMEM((half, d), BF16), pltpu.VMEM((half, d), BF16),
            pltpu.VMEM((part_rows, d), F32),
            pltpu.VMEM((3, big, d), F32),
            *ring_sems, *ring_sems,
            dma((2, 3)), dma((3,)), dma((2, n_bigs)), dma((4, n_bigs)), dma((4, n_bigs)), dma((3,)), dma((3,)), dma((2,)), dma((6,)),
        ],
        compiler_params=pltpu.CompilerParams(collective_id=0, has_side_effects=True, vmem_limit_bytes=67043328 - 4 * d * (2 * half + own_rows)),
        cost_estimate=pl.CostEstimate(flops=flops, bytes_accessed=10 * tokens * d * 4, transcendentals=half * hidden),
    )(y1, y2, dy1, dy2, lens, w1_own, w2_own, wq_in, wk_in, wv_in, wo_own)


def settle_kernel(chunk, depth, *refs):
    x1_sib, x2_in, dx1_in, dx2_sib, mlp_in, attn_buf, x1_own, dx2_own = refs[:8]
    x1, x2, dx1, dx2, *grads_out = refs[8:18]
    buf, mlp_buf, turned, read_sem, write_sem, small_sem, own_sem = refs[18:]
    tokens, half, hd = x2.shape[0], x1_own.shape[0], turned.shape[2]
    core = lax.rem(lax.axis_index('tp'), CORES)
    jobs = []
    for first in range(0, tokens, chunk):
        jobs += [(x2_in, first, x2, first), (dx1_in, first, dx1, first)]
    for first in range(0, half, chunk):
        jobs += [(x1_sib, first, x1, (1 - core) * half + first), (dx2_sib, first, dx2, (1 - core) * half + first)]

    def read(k):
        src, first, _, _ = jobs[k]
        return pltpu.make_async_copy(src.at[rows_at(first, chunk)], buf.at[k % depth], read_sem.at[k % depth])

    def write(k):
        _, _, dst, first = jobs[k]
        return pltpu.make_async_copy(buf.at[k % depth], dst.at[rows_at(first, chunk)], write_sem.at[k % depth])

    own = [pltpu.make_async_copy(src, dst.at[rows_at(core * half, half)], own_sem.at[i])
           for i, (src, dst) in enumerate(((x1_own, x1), (dx2_own, dx2)))]
    small_writes = [pltpu.make_async_copy(src, dst, small_sem.at[i]) for i, (src, dst) in enumerate(
        [(turned.at[i], grads_out[i]) for i in range(3)] + [(attn_buf.at[rows_at(3 * hd, hd)], grads_out[3]),
                                                            (mlp_buf.at[0], grads_out[4]), (mlp_buf.at[1], grads_out[5])])]
    mlp_read = pltpu.make_async_copy(mlp_in, mlp_buf, small_sem.at[6])
    mlp_read.start()
    for k in range(min(depth, len(jobs))):
        read(k).start()
    for copy in own:
        copy.start()
    for i in range(3):
        turned[i] = attn_buf[i * hd:(i + 1) * hd, :].T
    mlp_read.wait()
    for copy in small_writes:
        copy.start()
    lag = depth // 2
    for k in range(len(jobs)):
        read(k).wait()
        write(k).start()
        if k >= lag:
            write(k - lag).wait()
            if k - lag + depth < len(jobs):
                read(k - lag + depth).start()
    for k in range(max(len(jobs) - lag, 0), len(jobs)):
        write(k).wait()
    for copy in own + small_writes:
        copy.wait()


def settle(hd, x1_sib, x2, dx1, dx2_sib, dw_mlp, dw_attn, x1_own, dx2_own, chunk=256, depth=24):
    tokens, d = x2.shape
    size = dw_mlp.shape[1]
    hbm, vmem = pl.BlockSpec(memory_space=pl.ANY), pl.BlockSpec(memory_space=pltpu.VMEM)
    dma = pltpu.SemaphoreType.DMA
    grads = [(d, hd)] * 3 + [(hd, d), (size, d), (size, d)]
    return pl.pallas_call(
        functools.partial(settle_kernel, chunk, depth),
        name='settle',
        out_shape=[jax.ShapeDtypeStruct((tokens, d), F32)] * 4 + [jax.ShapeDtypeStruct(shape, F32) for shape in grads],
        in_specs=[hbm] * 5 + [vmem] * 3,
        out_specs=[hbm] * 10,
        scratch_shapes=[
            pltpu.VMEM((depth, chunk, d), F32), pltpu.VMEM((2, size, d), F32), pltpu.VMEM((3, d, hd), F32),
            dma((depth,)), dma((depth,)), dma((7,)), dma((2,)),
        ],
        compiler_params=pltpu.CompilerParams(vmem_limit_bytes=36 * 2 ** 20),
        cost_estimate=pl.CostEstimate(flops=0, bytes_accessed=8 * tokens * d * 4, transcendentals=0),
    )(x1_sib, x2, dx1, dx2_sib, pltpu.with_memory_space_constraint(dw_mlp, pltpu.HBM),
      *(pltpu.with_memory_space_constraint(ref, pltpu.VMEM) for ref in (dw_attn, x1_own, dx2_own)))


def layer_back(carry, lens, layer_w, n_tp, side):
    w_query, w_key, w_value, w_out, w_up, w_down = layer_w
    d, _, hd = w_query.shape
    heads = [w.reshape(d, hd) for w in (w_query, w_key, w_value)]
    *acts, dw_mlp, dw_attn, x1_own, dx2_own = block_back(n_tp, side, *carry, lens, w_up.T, w_down, *heads,
                                                         w_out.reshape(hd, d))
    *carry, dwq, dwk, dwv, dwo, dw1, dw2 = settle(hd, *acts, dw_mlp, dw_attn, x1_own, dx2_own)
    grads = (dwq.reshape(w_query.shape), dwk.reshape(w_key.shape), dwv.reshape(w_value.shape), dwo.reshape(w_out.shape),
             dw1.T, dw2)
    return tuple(carry), grads


def solution(mesh):
    act_spec = P('dp', None, None)
    w_specs = (P(None, None, 'tp', None), P(None, None, 'tp', None), P(None, None, 'tp', None),
               P(None, 'tp', None, None), P(None, None, 'tp'), P(None, 'tp', None))
    g_specs = (P('dp', None, 'tp', None), P('dp', None, 'tp', None), P('dp', None, 'tp', None),
               P('dp', 'tp', None, None), P('dp', None, 'tp'), P('dp', 'tp', None))
    n_tp = mesh.shape['tp']
    side = math.isqrt(mesh.shape['dp'])
    if side % 2 or side * side != mesh.shape['dp']:
        side = 0

    def local_fn(y_one, y_two, dy_one, dy_two, seq_lens, *weights):
        n_seqs, seq_len, d = y_one.shape
        carry = tuple(act.reshape(n_seqs * seq_len, d) for act in (y_one, y_two, dy_one, dy_two))
        n_layers = weights[0].shape[0]
        grads_by_layer = [None] * n_layers
        for layer in reversed(range(n_layers)):
            (x1, x2, dx1, dx2), grads_by_layer[layer] = layer_back(carry, seq_lens, [w[layer] for w in weights], n_tp, side)
            carry = (x1, x2, dx1, dx2)
        stacked = tuple(jnp.stack(grads) for grads in zip(*grads_by_layer))
        return tuple(act.reshape(n_seqs, seq_len, d) for act in carry) + stacked

    return jax.shard_map(local_fn, mesh=mesh,
                         in_specs=(act_spec,) * 4 + (P('dp'),) + w_specs,
                         out_specs=(act_spec,) * 4 + g_specs,
                         check_vma=False)
```

```python
import functools
import math

import jax
import jax.numpy as jnp
from jax import lax
from jax.experimental import pallas as pl
from jax.experimental.pallas import tpu as pltpu
from jax.sharding import PartitionSpec as P

F32 = jnp.float32
BF16 = jnp.bfloat16
EPS = 1e-5
MASK_VALUE = -1e30
CORES = 2
BLOCK = 128
GELU_A = 0.7978845608028654
GELU_B = 0.044715
LOG2_E = 1.4426950408889634


def dot_nt(a, b):
    return lax.dot_general(a, b, (((1,), (1,)), ((), ())), preferred_element_type=F32)


def dot_nn(a, b):
    return lax.dot_general(a, b, (((1,), (0,)), ((), ())), preferred_element_type=F32)


def dot_tn(a, b):
    return lax.dot_general(a, b, (((0,), (0,)), ((), ())), preferred_element_type=F32)


def gelu_and_slope(x):
    sq = x * x
    t = jnp.tanh(GELU_A * (x + GELU_B * (sq * x)))
    half = 0.5 * (1.0 + t)
    slope = half + (0.5 * x) * (1.0 - t * t) * (GELU_A * (1.0 + (3.0 * GELU_B) * sq))
    return x * half, slope


def inv_rms_of(x):
    return lax.rsqrt(jnp.mean(x * x, axis=-1, keepdims=True) + EPS)


def rms_back(x, grad):
    inv = inv_rms_of(x)
    normed = x * inv
    return inv * (grad - normed * jnp.mean(grad * normed, axis=-1, keepdims=True))


def rows_at(start, size):
    return pl.ds(start if isinstance(start, int) else pl.multiple_of(start, 16), size)


def attn_projections(normed, grad, wq, wkv, wo):
    return dot_nt(normed, wq).astype(BF16), dot_nt(normed, wkv).astype(BF16), dot_nt(grad, wo).astype(BF16)


def attn_scores(span, hd, proj):
    q, kv, da = proj
    out = []
    for first in range(0, span, BLOCK):
        r = slice(first, first + BLOCK)
        q_two = jnp.concatenate([q[r, :hd], q[r, hd:]], axis=0)
        da_two = jnp.concatenate([da[r, :hd], da[r, hd:]], axis=0)
        out.append((dot_nt(q_two, kv[r, :hd]), dot_nt(da_two, kv[r, hd:])))
    return out


def attn_softmax(hd, scores, masks):
    scale = hd ** -0.5
    out = []
    for (s, dp), mask in zip(scores, masks):
        s = jnp.where(jnp.concatenate([mask, mask], axis=0), s, MASK_VALUE)
        ex = jnp.exp2((s - jnp.max(s, axis=-1, keepdims=True)) * (scale * LOG2_E))
        p = ex * (1.0 / jnp.sum(ex, axis=-1, keepdims=True))
        ds = (p * (dp - jnp.sum(dp * p, axis=-1, keepdims=True)) * scale).astype(BF16)
        out.append((p.astype(BF16), ds))
    return out


def attn_grads(span, hd, proj, probs):
    q, kv, da = proj
    a, dq, dkv = [], [], ([], [])
    for first, (p, ds) in zip(range(0, span, BLOCK), probs):
        r = slice(first, first + BLOCK)
        two = dot_nn(p, kv[r, hd:]).astype(BF16)
        a.append(jnp.concatenate([two[:BLOCK], two[BLOCK:]], axis=1))
        two = dot_nn(ds, kv[r, :hd]).astype(BF16)
        dq.append(jnp.concatenate([two[:BLOCK], two[BLOCK:]], axis=1))
        for head in range(CORES):
            own, h = slice(head * BLOCK, (head + 1) * BLOCK), slice(head * hd, (head + 1) * hd)
            dkv[head].append(jnp.concatenate([dot_tn(ds[own], q[r, h]).astype(BF16),
                                              dot_tn(p[own], da[r, h]).astype(BF16)], axis=1))
    return tuple(jnp.concatenate(parts, axis=0) for parts in (a, dq, *dkv))


def when_do(condition, step):
    @pl.when(condition)
    def _():
        step()


class Ring:
    def __init__(self, n_tp, side):
        self.chips = n_tp // CORES
        self.far = self.chips // 2
        me, group = lax.axis_index('tp'), lax.axis_index('dp')
        self.core = lax.rem(me, CORES)
        chip = lax.div(me, CORES)
        up = lax.rem(chip + 1, self.chips) * CORES + self.core
        down = lax.rem(chip + self.chips - 1, self.chips) * CORES + self.core
        self.toward = ({'tp': up}, {'tp': down})
        self.sibling = {'tp': chip * CORES + (1 - self.core)}
        self.shared = side > 0
        if self.shared:
            over, down = lax.div(group, side), lax.rem(group, side)
            self.parity = lax.rem(over + down, 2)
            self.partners = ({'dp': group + 1 - 2 * lax.rem(down, 2)}, {'dp': group + side * (1 - 2 * lax.rem(over, 2))})

    def peers(self):
        return (*self.toward, self.sibling) + (self.partners if self.shared else ())

    def slot(self, hop, way):
        return 2 * hop - 1 if hop == self.far else 2 * hop - 1 + way


def remote(src, dst, send, recv, peer):
    return pltpu.make_async_remote_copy(src_ref=src, dst_ref=dst, send_sem=send, recv_sem=recv,
                                        device_id=peer, device_id_type=pl.DeviceIdType.MESH)


class Shares:
    def __init__(self, ring, refs, rows, sems):
        self.ring, self.refs, self.rows = ring, refs, rows
        self.recv, self.pair_recv, self.d2d_recv, self.sent = sems

    def place(self, piece, slot, low=0, rows=None):
        full, part, first = self.refs[piece]
        return full.at[rows_at((slot * CORES + self.ring.core) * part + first + low, rows or self.rows)]

    def ring_place(self, piece, slot):
        if not self.ring.shared:
            return self.place(piece, slot)
        return self.place(piece, slot, self.ring.parity * (self.rows // 2), self.rows // 2)

    def bundle(self, hop, piece):
        far = self.ring.far
        return () if hop > far else (piece,) if hop == far else (0, 1)

    def hop_copy(self, piece, way, hop):
        slot = 0 if hop == 1 else self.ring.slot(hop - 1, way)
        return remote(self.ring_place(piece, slot), self.ring_place(piece, self.ring.slot(hop, way)), self.sent.at[0],
                      self.recv.at[piece, way, hop - 1], self.ring.toward[way])

    def pair_copies(self, piece, slot):
        if not self.ring.shared:
            return ()
        quarter = self.rows // 4
        refs = [self.place(piece, slot, self.ring.parity * (self.rows // 2) + i * quarter, quarter) for i in range(2)]
        return [remote(ref, ref, self.sent.at[1], self.pair_recv.at[i, piece, slot], self.ring.partners[i])
                for i, ref in enumerate(refs)]

    def sibling_copy(self, piece, slot):
        ref = self.place(piece, slot)
        return remote(ref, ref, self.sent.at[2], self.d2d_recv.at[piece, slot], self.ring.sibling)

    def start(self, piece):
        for way in self.bundle(1, piece):
            self.hop_copy(piece, way, 1).start()
        self.sibling_copy(piece, 0).start()

    def wait_own(self):
        for piece in range(2):
            self.sibling_copy(piece, 0).wait_recv()

    def take_ring(self, hop, piece):
        for way in self.bundle(hop, piece):
            self.hop_copy(piece, way, hop).wait_recv()
            if way in self.bundle(hop + 1, piece):
                self.hop_copy(piece, way, hop + 1).start()
            for copy in self.pair_copies(piece, self.ring.slot(hop, way)):
                copy.start()

    def take_pair(self, hop, piece):
        for way in self.bundle(hop, piece):
            for copy in self.pair_copies(piece, self.ring.slot(hop, way)):
                copy.wait_recv()
            self.sibling_copy(piece, self.ring.slot(hop, way)).start()

    def take_sibling(self, hop):
        for piece in range(2):
            for way in self.bundle(hop, piece):
                self.sibling_copy(piece, self.ring.slot(hop, way)).wait_recv()

    def finish(self, like):
        ring = self.ring
        hops = 2 * (ring.chips - 1)
        counts = (hops * self.rows // 2, hops * self.rows // 2) if ring.shared else (hops * self.rows, 0)
        for kind, rows in enumerate((*counts, 2 * ring.chips * self.rows)):
            if rows:
                ref = like.at[pl.ds(0, rows)]
                pltpu.make_async_copy(ref, ref, self.sent.at[kind]).wait()


def block_kernel(n_tp, side, tile, big, y1, y2, dy1, dy2, lens_in, w1_own, w2_own, wq_in, wk_in, wv_in, wo_own,
                 x1_sib, x2, dx1, dx2_sib, dw_mlp, dw_attn, acc_a, acc_b,
                 lens, w1, w2, wa, norm, grad, part, stage,
                 mlp_recv, mlp_pair_recv, mlp_d2d_recv, mlp_sent, attn_recv, attn_pair_recv, attn_d2d_recv, attn_sent,
                 norm_sem, stage_sem, out_sem, sib_send, sib_recv, dw_send, dw_recv, dw_sem, local_sem):
    ring = Ring(n_tp, side)
    far = ring.far
    size = w1_own.shape[0]
    hd = wo_own.shape[0]
    rows_own = norm.shape[0]
    base = ring.core * rows_own
    n_tiles, n_bigs = rows_own // tile, rows_own // big

    barrier = pltpu.get_barrier_semaphore()
    for peer in ring.peers():
        pl.semaphore_signal(barrier, inc=1, device_id=peer, device_id_type=pl.DeviceIdType.MESH)

    a_part = 3 * hd
    mlp = Shares(ring, ((w1, size, 0), (w2, size, 0)), size,
                 (mlp_recv, mlp_pair_recv, mlp_d2d_recv, mlp_sent))
    attn = Shares(ring, ((wa, a_part, 0), (wa, a_part, a_part // 2)), a_part // 2,
                  (attn_recv, attn_pair_recv, attn_d2d_recv, attn_sent))

    def hbm_rows(ref, first, rows):
        return ref.at[rows_at(base + first, rows)]

    depth = stage.shape[0]

    def norm_fetch(which, t):
        slot = lax.rem(t, depth)
        return pltpu.make_async_copy(hbm_rows((y1, dy2)[which], t * tile, tile), stage.at[slot, rows_at(which * tile, tile)],
                                     norm_sem.at[which, slot])

    for t in range(min(depth, n_tiles)):
        for which in range(2):
            norm_fetch(which, t).start()

    depth_w = w1.shape[1]
    flat = [(slice(wa.shape[0] - (2 - i) * depth_w, wa.shape[0] - (1 - i) * depth_w), slice(0, hd)) for i in range(2)]
    own_a = ring.core * a_part

    def local_copy(i, src=None):
        src = (w1_own, w2_own, wo_own, lens_in, wq_in, src)[i]
        dst = (mlp.place(0, 0), mlp.place(1, 0), wa.at[rows_at(own_a + 2 * hd, hd)], lens, wa.at[flat[0]], wa.at[flat[1]])[i]
        return pltpu.make_async_copy(src, dst, local_sem.at[i])

    for i in range(5):
        local_copy(i).start()
    when_do(ring.core == 0, lambda: local_copy(5, wk_in).start())
    when_do(ring.core == 1, lambda: local_copy(5, wv_in).start())
    local_copy(0).wait()
    local_copy(1).wait()
    pl.semaphore_wait(barrier, len(ring.peers()))
    mlp.start(0)

    def norm_body(t, _):
        here = rows_at(t * tile, tile)
        slot = lax.rem(t, depth)
        for which in range(2):
            norm_fetch(which, t).wait()
        y = stage[slot, 0:tile, :]
        norm[here, :] = (y * inv_rms_of(y)).astype(BF16)
        grad[here, :] = stage[slot, tile:2 * tile, :].astype(BF16)

        @pl.when(t + depth < n_tiles)
        def _():
            for which in range(2):
                norm_fetch(which, t + depth).start()

        when_do(t == n_tiles // 3, lambda: mlp.start(1))
        return 0

    lax.fori_loop(0, n_tiles, norm_body, 0)

    def mlp_hidden(here, cols):
        pre = dot_nt(norm[here, :], w1[cols, :])
        d_act = dot_nt(grad[here, :], w2[cols, :])
        act, slope = gelu_and_slope(pre)
        return act.astype(BF16), (d_act * slope).astype(BF16)

    def r(shares, hop, piece):
        with jax.named_scope('ring'):
            shares.take_ring(hop, piece)

    def y(shares, hop, piece):
        with jax.named_scope('pair'):
            shares.take_pair(hop, piece)

    def both(step, shares, hop):
        step(shares, hop, 0)
        step(shares, hop, 1)

    plan = {
        ('own', 0): lambda: r(mlp, 1, 0),
        ('own', 1): lambda: r(mlp, 1, 1),
        ('own', 2): lambda: y(mlp, 1, 0),
        ('mlp1', -1): lambda: (r(mlp, 2, 0), y(mlp, 1, 1), mlp.take_sibling(1)),
        ('mlp1', 0): lambda: (r(mlp, 2, 1), y(mlp, 2, 0)),
        ('mlp1', 1): lambda: (r(mlp, 3, 0), y(mlp, 2, 1)),
        ('mlp1', 2): lambda: r(mlp, 3, 1),
        ('mlp2', -1): lambda: mlp.take_sibling(2),
        ('mlp2', 0): lambda: (y(mlp, 3, 0), r(mlp, 4, 0)),
        ('mlp2', 1): lambda: (r(mlp, 4, 1), y(mlp, 3, 1), attn.start(0), attn.start(1)),
        ('mlp2', 2): lambda: y(mlp, 4, 0),
        ('mlp3', -1): lambda: mlp.take_sibling(3),
        ('mlp3', 0): lambda: y(mlp, 4, 1),
        ('mlp3', 1): lambda: both(r, attn, 1),
        ('last', -1): lambda: mlp.take_sibling(4),
        ('last', 0): lambda: (both(y, attn, 1), r(attn, 2, 0)),
        ('last', 1): lambda: r(attn, 2, 1),
        ('last', 2): lambda: (both(y, attn, 2), r(attn, 3, 0)),
        ('attn0', -1): lambda: (attn.wait_own(), attn.take_sibling(1)),
        ('attn0', 0): lambda: (r(attn, 3, 1), y(attn, 3, 0)),
        ('attn0', 1): lambda: (both(r, attn, 4), y(attn, 3, 1)),
        ('attn1', -1): lambda: attn.take_sibling(2),
        ('attn1', 0): lambda: both(y, attn, 4),
        ('attn2', -1): lambda: attn.take_sibling(3),
        ('attn3', -1): lambda: attn.take_sibling(4),
    }

    def serve(phase, t):
        for (name, at), step in plan.items():
            if name == phase and at >= 0:
                when_do(t == at, step)

    def serve_loop(kind, index, indices, t=None):
        for i in indices:
            if t is None and (f'{kind}{i}', -1) in plan:
                when_do(index == i, plan[f'{kind}{i}', -1])
            for at in range(n_bigs if t is not None else 0):
                if (f'{kind}{i}', at) in plan:
                    when_do((index == i) & (t == at), plan[f'{kind}{i}', at])

    width = CORES * size
    mlp.wait_own()
    part[...] = jnp.zeros_like(part)

    def mlp_own(t, _):
        here = rows_at(t * big, big)
        cols = rows_at(0, width)
        act, d_pre = mlp_hidden(here, cols)
        acc_a[here, :] = dot_nn(act, w2[cols, :])
        acc_b[here, :] = dot_nn(d_pre, w1[cols, :])
        part[0:width, :] += dot_tn(d_pre, norm[here, :])
        part[width:2 * width, :] += dot_tn(act, grad[here, :])
        serve('own', t)
        return 0

    with jax.named_scope('mlp_own'):
        lax.fori_loop(0, n_bigs, mlp_own, 0)

    eye = (lax.broadcasted_iota(jnp.int32, (hd, hd), 0) == lax.broadcasted_iota(jnp.int32, (hd, hd), 1)).astype(BF16)
    for i in range(2):
        local_copy(4 + i, wk_in).wait()
        wa[rows_at(own_a + i * hd, hd), :] = dot_nt(eye, wa[flat[i]]).astype(BF16)
    local_copy(2).wait()
    local_copy(3).wait()

    def mlp_dw(mat, which):
        core = 1 - ring.core if which else ring.core
        return rows_at(mat * width + core * size, size)

    def mlp_dw_out(mat):
        return pltpu.make_async_copy(dw_attn.at[rows_at(mat * size, size)], dw_mlp.at[mat], dw_sem.at[mat])

    def mlp_dw_copy(mat):
        return remote(part.at[mlp_dw(mat, 1)], dw_attn.at[rows_at(mat * size, size)], dw_send.at[mat], dw_recv.at[mat],
                      ring.sibling)

    def mlp_pair(hop, _):
        with jax.named_scope('mlp_wait'):
            serve_loop('mlp', hop, range(1, far))
        cols = rows_at((2 * hop - 1) * width, 2 * width)

        def body(t, _):
            here = rows_at(t * big, big)
            act, d_pre = mlp_hidden(here, cols)
            acc_a[here, :] += dot_nn(act, w2[cols, :])
            acc_b[here, :] += dot_nn(d_pre, w1[cols, :])
            serve_loop('mlp', hop, range(1, far), t)
            return 0

        with jax.named_scope('mlp_pair'):
            lax.fori_loop(0, n_bigs, body, 0)

        @pl.when(hop == 1)
        def _():
            for mat in range(2):
                mlp_dw_copy(mat).start()

        return 0

    lax.fori_loop(1, far, mlp_pair, 0)

    def out_copy(which, t):
        return pltpu.make_async_copy((acc_a, acc_b)[which].at[rows_at(t * tile, tile)],
                                     hbm_rows((x2, dx1)[which], t * tile, tile), out_sem.at[which, t])

    def sib_copy(which, t):
        span = tile if which < 2 else big
        here = rows_at(t * span, span)
        dst = (hbm_rows(x2, t * span, span), hbm_rows(dx1, t * span, span), x1_sib.at[here], dx2_sib.at[here])[which]
        return remote((acc_a, acc_b)[which % 2].at[here], dst, sib_send.at[which, t], sib_recv.at[which, t], ring.sibling)

    def stage_copy(which, src, t, span, slot=0):
        return pltpu.make_async_copy(hbm_rows(src, t * span, span), stage.at[which, rows_at(slot * span, span)],
                                     stage_sem.at[which, slot])

    with jax.named_scope('mlp_wait'):
        plan['last', -1]()
    for mat in range(2):
        mlp_dw_copy(mat).wait_send()
        mlp_dw_copy(mat).wait_recv()
        mine = rows_at(mat * size, size)
        dw_attn[mine, :] = dw_attn[mine, :] + part[mlp_dw(mat, 0), :]
        mlp_dw_out(mat).start()

    mlp_ins = (y1, y2, dy1)

    def start_mlp_ins(t):
        for which, src in enumerate(mlp_ins):
            stage_copy(which, src, t, tile, lax.rem(t, 2)).start()

    def mlp_last(t, _):
        slot = lax.rem(t, 2)
        here = rows_at(t * tile, tile)
        cols = rows_at((2 * far - 1) * width, width)
        when_do(t + 1 < n_tiles, lambda: start_mlp_ins(t + 1))
        for which, src in enumerate(mlp_ins):
            stage_copy(which, src, t, tile, slot).wait()
        now = rows_at(slot * tile, tile)
        act, d_pre = mlp_hidden(here, cols)
        x = stage[1, now, :] - (acc_a[here, :] + dot_nn(act, w2[cols, :]))
        d = stage[2, now, :] + rms_back(stage[0, now, :], acc_b[here, :] + dot_nn(d_pre, w1[cols, :]))
        acc_a[here, :] = x
        acc_b[here, :] = d
        norm[here, :] = (x * inv_rms_of(x)).astype(BF16)
        grad[here, :] = d.astype(BF16)

        @pl.when(t == n_tiles - 1)
        def _():
            for mat in range(2):
                mlp_dw_out(mat).wait()

        ratio = big // tile
        for at in range(n_bigs):
            if ('last', at) in plan:
                when_do(t == ratio * at + ratio - 1, plan['last', at])
        for which in range(2):
            out_copy(which, t).start()
            sib_copy(which, t).start()
        return 0

    with jax.named_scope('mlp_last'):
        start_mlp_ins(0)
        lax.fori_loop(0, n_tiles, mlp_last, 0)

    row_pos = lax.broadcasted_iota(jnp.int32, (BLOCK, BLOCK), 0)
    col_pos = lax.broadcasted_iota(jnp.int32, (BLOCK, BLOCK), 1)
    seq = BLOCK // 2
    causal = (col_pos <= row_pos) & ((col_pos < seq) == (row_pos < seq))
    first_seq = ring.core * (rows_own // seq)

    def masks_of(t):
        out = []
        for block in range(big // BLOCK):
            at = first_seq + t * (big // seq) + 2 * block
            end = jnp.where(col_pos < seq, lens[at], seq + lens[at + 1])
            out.append(causal & (col_pos < end))
        return out

    def attn_pair(t, j, use_f):
        here = rows_at(t * big, big)
        masks = masks_of(t)

        def weights(i):
            first = (2 * j + i) * CORES * a_part
            return [jnp.concatenate([wa[rows_at(first + core * a_part + which * hd, hd), :] for core in range(CORES)], axis=0)
                    for which in range(3)]

        def project(i):
            return attn_projections(norm[here, :], grad[here, :], *weights(i))

        def grad_sum(i, factors):
            q_w, kv_w, _ = weights(i)
            _, dq, d0, d1 = factors
            return dot_nn(dq, q_w) + dot_nn(d0, kv_w) + dot_nn(d1, kv_w)

        first = project(0)
        scores = attn_scores(big, hd, first)
        second = project(1)
        factors = attn_grads(big, hd, first, attn_softmax(hd, scores, masks))
        scores = attn_scores(big, hd, second)
        f = dot_nn(factors[0], weights(0)[2])
        g = grad_sum(0, factors)
        more = attn_grads(big, hd, second, attn_softmax(hd, scores, masks))
        f = f + dot_nn(more[0], weights(1)[2])
        use_f(f)
        return g + grad_sum(1, more), factors

    part[...] = jnp.zeros_like(part)
    own_part = 4 * hd
    mlp.finish(w1)

    def attn_dw(which):
        core = 1 - ring.core if which else ring.core
        return rows_at(core * own_part, own_part)

    def attn_dw_copy():
        return remote(part.at[attn_dw(1)], dw_attn.at[rows_at(0, own_part)], dw_send.at[2], dw_recv.at[2], ring.sibling)

    per_band = w1.shape[1] // hd

    def kept_at(k):
        return slice(k // per_band * big, (k // per_band + 1) * big), slice(k % per_band * hd, (k % per_band + 1) * hd)

    def attn_pairs(j, _):
        with jax.named_scope('attn_wait'):
            serve_loop('attn', j, range(far - 1))

        def body(t, _):
            here = rows_at(t * big, big)

            @pl.when(j == 0)
            def _():
                for which in range(2):
                    for i in range(big // tile):
                        out_copy(which, t * (big // tile) + i).wait()
                        sib_copy(which, t * (big // tile) + i).wait_send()
                acc_a[here, :] = jnp.zeros((big, acc_a.shape[1]), F32)
                acc_b[here, :] = jnp.zeros((big, acc_b.shape[1]), F32)

            def add_f(f):
                acc_a[here, :] += f

            g, own_factors = attn_pair(t, j, add_f)
            acc_b[here, :] += g
            a, dq, *dkv = own_factors
            both_heads = [slice(head * hd, (head + 1) * hd) for head in range(CORES)]
            left = [f for head, cols in enumerate(both_heads) for f in (dq[:, cols], dkv[head][:, :hd], dkv[head][:, hd:])]
            for k, factor in enumerate(left + [a[:, cols] for cols in both_heads]):
                w1[kept_at(k)] = factor

            @pl.when(j == 0)
            def _():
                where = [head * own_part + which * hd for head in range(CORES) for which in range(3)]
                where += [head * own_part + 3 * hd for head in range(CORES)]
                for k in range(0, 4 * CORES, 2):
                    right = norm if k < 3 * CORES else grad
                    two = dot_tn(jnp.concatenate([w1[kept_at(k)], w1[kept_at(k + 1)]], axis=1), right[here, :])
                    part[where[k]:where[k] + hd, :] += two[:hd]
                    part[where[k + 1]:where[k + 1] + hd, :] += two[hd:]

            serve_loop('attn', j, range(far - 1), t)
            return 0

        with jax.named_scope('attn_pair'):
            lax.fori_loop(0, n_bigs, body, 0)

        @pl.when(j == 1)
        def _():
            attn_dw_copy().start()

        return 0

    lax.fori_loop(0, far - 1, attn_pairs, 0)

    with jax.named_scope('attn_wait'):
        plan['attn3', -1]()
    attn_dw_copy().wait_send()
    attn_dw_copy().wait_recv()
    mine = rows_at(0, own_part)
    dw_attn[mine, :] = dw_attn[mine, :] + part[attn_dw(0), :]

    attn_ins = (y1, x2, dy2)

    def attn_last(t, _):
        here = rows_at(t * big, big)
        for which, src in enumerate(attn_ins):
            stage_copy(which, src, t, big).start()

        def x1_ends(f):
            stage_copy(0, y1, t, big).wait()
            acc_a[here, :] = stage[0] - (acc_a[here, :] + f)
            sib_copy(2, t).start()

        g, _ = attn_pair(t, far - 1, x1_ends)
        stage_copy(1, x2, t, big).wait()
        stage_copy(2, dy2, t, big).wait()
        acc_b[here, :] = stage[2] + rms_back(stage[1], acc_b[here, :] + g)
        sib_copy(3, t).start()
        return 0

    with jax.named_scope('attn_last'):
        lax.fori_loop(0, n_bigs, attn_last, 0)

    attn.finish(wa)

    def drain(t, _):
        for which in range(2, 4):
            sib_copy(which, t).wait_send()
            sib_copy(which, t).wait_recv()
        for which in range(2):
            for i in range(big // tile):
                sib_copy(which, t * (big // tile) + i).wait_recv()
        return 0

    with jax.named_scope('drain'):
        lax.fori_loop(0, n_bigs, drain, 0)


def block_back(n_tp, side, y1, y2, dy1, dy2, lens, w1_own, w2_own, wq_in, wk_in, wv_in, wo_own, tile=256, big=512):
    tokens, d = y1.shape
    size, hd = w1_own.shape[0], wo_own.shape[0]
    chips = n_tp // CORES
    hops = chips // 2
    half = tokens // CORES
    n_tiles = half // tile
    hidden, heads = n_tp * size, n_tp * hd
    hbm = pl.BlockSpec(memory_space=pl.ANY)
    dma = pltpu.SemaphoreType.DMA
    flops = 8 * half * d * hidden + 14 * half * d * heads
    part_rows = max(4 * size, CORES * 4 * hd)
    own_rows = max(2 * size, 4 * hd)

    ring_sems = [dma((2, 2, hops)), dma((2, 2, chips)), dma((2, chips)), dma((3,))]

    return pl.pallas_call(
        functools.partial(block_kernel, n_tp, side, tile, big),
        name='block_back',
        out_shape=[jax.ShapeDtypeStruct(shape, F32) for shape in ((half, d), (tokens, d), (tokens, d), (half, d), (2, size, d))]
        + [pltpu.VMEM((rows, d), F32) for rows in (own_rows, half, half)],
        in_specs=[hbm] * 11,
        out_specs=[hbm] * 5 + [pl.BlockSpec(memory_space=pltpu.VMEM)] * 3,
        scratch_shapes=[
            pltpu.SMEM(lens.shape, jnp.int32), pltpu.VMEM((hidden, d), BF16), pltpu.VMEM((hidden, d), BF16),
            pltpu.VMEM((3 * heads, d), BF16),
            pltpu.VMEM((half, d), BF16), pltpu.VMEM((half, d), BF16),
            pltpu.VMEM((part_rows, d), F32),
            pltpu.VMEM((3, big, d), F32),
            *ring_sems, *ring_sems,
            dma((2, 3)), dma((3, 2)), dma((2, n_tiles)), dma((4, n_tiles)), dma((4, n_tiles)), dma((3,)), dma((3,)), dma((2,)), dma((6,)),
        ],
        compiler_params=pltpu.CompilerParams(collective_id=0, has_side_effects=True, vmem_limit_bytes=67043328 - 4 * d * (2 * half + own_rows)),
        cost_estimate=pl.CostEstimate(flops=flops, bytes_accessed=10 * tokens * d * 4, transcendentals=half * hidden),
    )(y1, y2, dy1, dy2, lens, w1_own, w2_own, wq_in, wk_in, wv_in, wo_own)


def settle_kernel(chunk, depth, *refs):
    x1_sib, x2_in, dx1_in, dx2_sib, mlp_in, attn_buf, x1_own, dx2_own = refs[:8]
    x1, x2, dx1, dx2, *grads_out = refs[8:18]
    buf, mlp_buf, turned, read_sem, write_sem, small_sem, own_sem = refs[18:]
    tokens, half, hd = x2.shape[0], x1_own.shape[0], turned.shape[2]
    core = lax.rem(lax.axis_index('tp'), CORES)
    jobs = []
    for first in range(0, tokens, chunk):
        jobs += [(x2_in, first, x2, first), (dx1_in, first, dx1, first)]
    for first in range(0, half, chunk):
        jobs += [(x1_sib, first, x1, (1 - core) * half + first), (dx2_sib, first, dx2, (1 - core) * half + first)]

    def read(k):
        src, first, _, _ = jobs[k]
        return pltpu.make_async_copy(src.at[rows_at(first, chunk)], buf.at[k % depth], read_sem.at[k % depth])

    def write(k):
        _, _, dst, first = jobs[k]
        return pltpu.make_async_copy(buf.at[k % depth], dst.at[rows_at(first, chunk)], write_sem.at[k % depth])

    own = [pltpu.make_async_copy(src, dst.at[rows_at(core * half, half)], own_sem.at[i])
           for i, (src, dst) in enumerate(((x1_own, x1), (dx2_own, dx2)))]
    small_writes = [pltpu.make_async_copy(src, dst, small_sem.at[i]) for i, (src, dst) in enumerate(
        [(turned.at[i], grads_out[i]) for i in range(3)] + [(attn_buf.at[rows_at(3 * hd, hd)], grads_out[3]),
                                                            (mlp_buf.at[0], grads_out[4]), (mlp_buf.at[1], grads_out[5])])]
    mlp_read = pltpu.make_async_copy(mlp_in, mlp_buf, small_sem.at[6])
    mlp_read.start()
    for k in range(min(depth, len(jobs))):
        read(k).start()
    for copy in own:
        copy.start()
    for i in range(3):
        turned[i] = attn_buf[i * hd:(i + 1) * hd, :].T
    mlp_read.wait()
    for copy in small_writes:
        copy.start()
    lag = depth // 2
    for k in range(len(jobs)):
        read(k).wait()
        write(k).start()
        if k >= lag:
            write(k - lag).wait()
            if k - lag + depth < len(jobs):
                read(k - lag + depth).start()
    for k in range(max(len(jobs) - lag, 0), len(jobs)):
        write(k).wait()
    for copy in own + small_writes:
        copy.wait()


def settle(hd, x1_sib, x2, dx1, dx2_sib, dw_mlp, dw_attn, x1_own, dx2_own, chunk=256, depth=24):
    tokens, d = x2.shape
    size = dw_mlp.shape[1]
    hbm, vmem = pl.BlockSpec(memory_space=pl.ANY), pl.BlockSpec(memory_space=pltpu.VMEM)
    dma = pltpu.SemaphoreType.DMA
    grads = [(d, hd)] * 3 + [(hd, d), (size, d), (size, d)]
    return pl.pallas_call(
        functools.partial(settle_kernel, chunk, depth),
        name='settle',
        out_shape=[jax.ShapeDtypeStruct((tokens, d), F32)] * 4 + [jax.ShapeDtypeStruct(shape, F32) for shape in grads],
        in_specs=[hbm] * 5 + [vmem] * 3,
        out_specs=[hbm] * 10,
        scratch_shapes=[
            pltpu.VMEM((depth, chunk, d), F32), pltpu.VMEM((2, size, d), F32), pltpu.VMEM((3, d, hd), F32),
            dma((depth,)), dma((depth,)), dma((7,)), dma((2,)),
        ],
        compiler_params=pltpu.CompilerParams(vmem_limit_bytes=36 * 2 ** 20),
        cost_estimate=pl.CostEstimate(flops=0, bytes_accessed=8 * tokens * d * 4, transcendentals=0),
    )(x1_sib, x2, dx1, dx2_sib, pltpu.with_memory_space_constraint(dw_mlp, pltpu.HBM),
      *(pltpu.with_memory_space_constraint(ref, pltpu.VMEM) for ref in (dw_attn, x1_own, dx2_own)))


def layer_back(carry, lens, layer_w, n_tp, side):
    w_query, w_key, w_value, w_out, w_up, w_down = layer_w
    d, _, hd = w_query.shape
    heads = [w.reshape(d, hd) for w in (w_query, w_key, w_value)]
    *acts, dw_mlp, dw_attn, x1_own, dx2_own = block_back(n_tp, side, *carry, lens, w_up.T, w_down, *heads,
                                                         w_out.reshape(hd, d))
    *carry, dwq, dwk, dwv, dwo, dw1, dw2 = settle(hd, *acts, dw_mlp, dw_attn, x1_own, dx2_own)
    grads = (dwq.reshape(w_query.shape), dwk.reshape(w_key.shape), dwv.reshape(w_value.shape), dwo.reshape(w_out.shape),
             dw1.T, dw2)
    return tuple(carry), grads


def solution(mesh):
    act_spec = P('dp', None, None)
    w_specs = (P(None, None, 'tp', None), P(None, None, 'tp', None), P(None, None, 'tp', None),
               P(None, 'tp', None, None), P(None, None, 'tp'), P(None, 'tp', None))
    g_specs = (P('dp', None, 'tp', None), P('dp', None, 'tp', None), P('dp', None, 'tp', None),
               P('dp', 'tp', None, None), P('dp', None, 'tp'), P('dp', 'tp', None))
    n_tp = mesh.shape['tp']
    side = math.isqrt(mesh.shape['dp'])
    if side % 2 or side * side != mesh.shape['dp']:
        side = 0

    def local_fn(y_one, y_two, dy_one, dy_two, seq_lens, *weights):
        n_seqs, seq_len, d = y_one.shape
        carry = tuple(act.reshape(n_seqs * seq_len, d) for act in (y_one, y_two, dy_one, dy_two))
        n_layers = weights[0].shape[0]
        grads_by_layer = [None] * n_layers
        for layer in reversed(range(n_layers)):
            (x1, x2, dx1, dx2), grads_by_layer[layer] = layer_back(carry, seq_lens, [w[layer] for w in weights], n_tp, side)
            carry = (x1, x2, dx1, dx2)
        stacked = tuple(jnp.stack(grads) for grads in zip(*grads_by_layer))
        return tuple(act.reshape(n_seqs, seq_len, d) for act in carry) + stacked

    return jax.shard_map(local_fn, mesh=mesh,
                         in_specs=(act_spec,) * 4 + (P('dp'),) + w_specs,
                         out_specs=(act_spec,) * 4 + g_specs,
                         check_vma=False)
```

```python
import functools
import math

import jax
import jax.numpy as jnp
from jax import lax
from jax.experimental import pallas as pl
from jax.experimental.pallas import tpu as pltpu
from jax.sharding import PartitionSpec as P

F32 = jnp.float32
BF16 = jnp.bfloat16
EPS = 1e-5
MASK_VALUE = -1e30
CORES = 2
BLOCK = 128
GELU_A = 0.7978845608028654
GELU_B = 0.044715
LOG2_E = 1.4426950408889634


def dot_nt(a, b):
    return lax.dot_general(a, b, (((1,), (1,)), ((), ())), preferred_element_type=F32)


def dot_nn(a, b):
    return lax.dot_general(a, b, (((1,), (0,)), ((), ())), preferred_element_type=F32)


def dot_tn(a, b):
    return lax.dot_general(a, b, (((0,), (0,)), ((), ())), preferred_element_type=F32)


def gelu_and_slope(x):
    sq = x * x
    t = jnp.tanh(GELU_A * (x + GELU_B * (sq * x)))
    half = 0.5 * (1.0 + t)
    slope = half + (0.5 * x) * (1.0 - t * t) * (GELU_A * (1.0 + (3.0 * GELU_B) * sq))
    return x * half, slope


def inv_rms_of(x):
    return lax.rsqrt(jnp.mean(x * x, axis=-1, keepdims=True) + EPS)


def rms_back(x, grad):
    inv = inv_rms_of(x)
    normed = x * inv
    return inv * (grad - normed * jnp.mean(grad * normed, axis=-1, keepdims=True))


def rows_at(start, size):
    return pl.ds(start if isinstance(start, int) else pl.multiple_of(start, 16), size)


def attn_projections(normed, grad, wq, wkv, wo):
    return dot_nt(normed, wq).astype(BF16), dot_nt(normed, wkv).astype(BF16), dot_nt(grad, wo).astype(BF16)


def attn_scores(span, hd, proj):
    q, kv, da = proj
    out = []
    for first in range(0, span, BLOCK):
        r = slice(first, first + BLOCK)
        q_two = jnp.concatenate([q[r, :hd], q[r, hd:]], axis=0)
        da_two = jnp.concatenate([da[r, :hd], da[r, hd:]], axis=0)
        out.append((dot_nt(q_two, kv[r, :hd]), dot_nt(da_two, kv[r, hd:])))
    return out


def attn_softmax(hd, scores, masks):
    scale = hd ** -0.5
    out = []
    for (s, dp), mask in zip(scores, masks):
        s = jnp.where(jnp.concatenate([mask, mask], axis=0), s, MASK_VALUE)
        ex = jnp.exp2((s - jnp.max(s, axis=-1, keepdims=True)) * (scale * LOG2_E))
        p = ex * (1.0 / jnp.sum(ex, axis=-1, keepdims=True))
        ds = (p * (dp - jnp.sum(dp * p, axis=-1, keepdims=True)) * scale).astype(BF16)
        out.append((p.astype(BF16), ds))
    return out


def attn_grads(span, hd, proj, probs):
    q, kv, da = proj
    a, dq, dkv = [], [], ([], [])
    for first, (p, ds) in zip(range(0, span, BLOCK), probs):
        r = slice(first, first + BLOCK)
        two = dot_nn(p, kv[r, hd:]).astype(BF16)
        a.append(jnp.concatenate([two[:BLOCK], two[BLOCK:]], axis=1))
        two = dot_nn(ds, kv[r, :hd]).astype(BF16)
        dq.append(jnp.concatenate([two[:BLOCK], two[BLOCK:]], axis=1))
        for head in range(CORES):
            own, h = slice(head * BLOCK, (head + 1) * BLOCK), slice(head * hd, (head + 1) * hd)
            dkv[head].append(jnp.concatenate([dot_tn(ds[own], q[r, h]).astype(BF16),
                                              dot_tn(p[own], da[r, h]).astype(BF16)], axis=1))
    return tuple(jnp.concatenate(parts, axis=0) for parts in (a, dq, *dkv))


def when_do(condition, step):
    @pl.when(condition)
    def _():
        step()


class Ring:
    def __init__(self, n_tp, side):
        self.chips = n_tp // CORES
        self.far = self.chips // 2
        me, group = lax.axis_index('tp'), lax.axis_index('dp')
        self.core = lax.rem(me, CORES)
        chip = lax.div(me, CORES)
        up = lax.rem(chip + 1, self.chips) * CORES + self.core
        down = lax.rem(chip + self.chips - 1, self.chips) * CORES + self.core
        self.toward = ({'tp': up}, {'tp': down})
        self.sibling = {'tp': chip * CORES + (1 - self.core)}
        self.shared = side > 0
        if self.shared:
            over, down = lax.div(group, side), lax.rem(group, side)
            self.parity = lax.rem(over + down, 2)
            self.partners = ({'dp': group + 1 - 2 * lax.rem(down, 2)}, {'dp': group + side * (1 - 2 * lax.rem(over, 2))})

    def peers(self):
        return (*self.toward, self.sibling) + (self.partners if self.shared else ())

    def slot(self, hop, way):
        return 2 * hop - 1 if hop == self.far else 2 * hop - 1 + way


def remote(src, dst, send, recv, peer):
    return pltpu.make_async_remote_copy(src_ref=src, dst_ref=dst, send_sem=send, recv_sem=recv,
                                        device_id=peer, device_id_type=pl.DeviceIdType.MESH)


class Shares:
    def __init__(self, ring, refs, rows, sems):
        self.ring, self.refs, self.rows = ring, refs, rows
        self.recv, self.pair_recv, self.d2d_recv, self.sent = sems

    def place(self, piece, slot, low=0, rows=None):
        full, part, first = self.refs[piece]
        return full.at[rows_at((slot * CORES + self.ring.core) * part + first + low, rows or self.rows)]

    def ring_place(self, piece, slot):
        if not self.ring.shared:
            return self.place(piece, slot)
        return self.place(piece, slot, self.ring.parity * (self.rows // 2), self.rows // 2)

    def bundle(self, hop, piece):
        far = self.ring.far
        return () if hop > far else (piece,) if hop == far else (0, 1)

    def hop_copy(self, piece, way, hop):
        slot = 0 if hop == 1 else self.ring.slot(hop - 1, way)
        return remote(self.ring_place(piece, slot), self.ring_place(piece, self.ring.slot(hop, way)), self.sent.at[0],
                      self.recv.at[piece, way, hop - 1], self.ring.toward[way])

    def pair_copies(self, piece, slot):
        if not self.ring.shared:
            return ()
        quarter = self.rows // 4
        refs = [self.place(piece, slot, self.ring.parity * (self.rows // 2) + i * quarter, quarter) for i in range(2)]
        return [remote(ref, ref, self.sent.at[1], self.pair_recv.at[i, piece, slot], self.ring.partners[i])
                for i, ref in enumerate(refs)]

    def sibling_copy(self, piece, slot):
        ref = self.place(piece, slot)
        return remote(ref, ref, self.sent.at[2], self.d2d_recv.at[piece, slot], self.ring.sibling)

    def start(self, piece):
        for way in self.bundle(1, piece):
            self.hop_copy(piece, way, 1).start()
        self.sibling_copy(piece, 0).start()

    def wait_own(self):
        for piece in range(2):
            self.sibling_copy(piece, 0).wait_recv()

    def take_ring(self, hop, piece):
        for way in self.bundle(hop, piece):
            self.hop_copy(piece, way, hop).wait_recv()
            if way in self.bundle(hop + 1, piece):
                self.hop_copy(piece, way, hop + 1).start()
            for copy in self.pair_copies(piece, self.ring.slot(hop, way)):
                copy.start()

    def take_pair(self, hop, piece):
        for way in self.bundle(hop, piece):
            for copy in self.pair_copies(piece, self.ring.slot(hop, way)):
                copy.wait_recv()
            self.sibling_copy(piece, self.ring.slot(hop, way)).start()

    def take_sibling(self, hop):
        for piece in range(2):
            for way in self.bundle(hop, piece):
                self.sibling_copy(piece, self.ring.slot(hop, way)).wait_recv()

    def finish(self, like):
        ring = self.ring
        hops = 2 * (ring.chips - 1)
        counts = (hops * self.rows // 2, hops * self.rows // 2) if ring.shared else (hops * self.rows, 0)
        for kind, rows in enumerate((*counts, 2 * ring.chips * self.rows)):
            if rows:
                ref = like.at[pl.ds(0, rows)]
                pltpu.make_async_copy(ref, ref, self.sent.at[kind]).wait()


def block_kernel(n_tp, side, tile, big, y1, y2, dy1, dy2, lens_in, w1_own, w2_own, wq_in, wk_in, wv_in, wo_own,
                 x1_sib, x2, dx1, dx2_sib, dw_mlp, dw_attn, acc_a, acc_b,
                 lens, w1, w2, wa, norm, grad, part, stage,
                 mlp_recv, mlp_pair_recv, mlp_d2d_recv, mlp_sent, attn_recv, attn_pair_recv, attn_d2d_recv, attn_sent,
                 norm_sem, stage_sem, out_sem, sib_send, sib_recv, dw_send, dw_recv, dw_sem, local_sem):
    ring = Ring(n_tp, side)
    far = ring.far
    size = w1_own.shape[0]
    hd = wo_own.shape[0]
    rows_own = norm.shape[0]
    base = ring.core * rows_own
    n_tiles, n_bigs = rows_own // tile, rows_own // big

    barrier = pltpu.get_barrier_semaphore()
    for peer in ring.peers():
        pl.semaphore_signal(barrier, inc=1, device_id=peer, device_id_type=pl.DeviceIdType.MESH)

    a_part = 3 * hd
    mlp = Shares(ring, ((w1, size, 0), (w2, size, 0)), size,
                 (mlp_recv, mlp_pair_recv, mlp_d2d_recv, mlp_sent))
    attn = Shares(ring, ((wa, a_part, 0), (wa, a_part, a_part // 2)), a_part // 2,
                  (attn_recv, attn_pair_recv, attn_d2d_recv, attn_sent))

    def hbm_rows(ref, first, rows):
        return ref.at[rows_at(base + first, rows)]

    depth = stage.shape[0]

    def norm_fetch(which, t):
        slot = lax.rem(t, depth)
        return pltpu.make_async_copy(hbm_rows((y1, dy2)[which], t * tile, tile), stage.at[slot, rows_at(which * tile, tile)],
                                     norm_sem.at[which, slot])

    for t in range(min(depth, n_tiles)):
        for which in range(2):
            norm_fetch(which, t).start()

    depth_w = w1.shape[1]
    flat = [(slice(wa.shape[0] - (2 - i) * depth_w, wa.shape[0] - (1 - i) * depth_w), slice(0, hd)) for i in range(2)]
    own_a = ring.core * a_part

    def local_copy(i, src=None):
        src = (w1_own, w2_own, wo_own, lens_in, wq_in, src)[i]
        dst = (mlp.place(0, 0), mlp.place(1, 0), wa.at[rows_at(own_a + 2 * hd, hd)], lens, wa.at[flat[0]], wa.at[flat[1]])[i]
        return pltpu.make_async_copy(src, dst, local_sem.at[i])

    for i in range(5):
        local_copy(i).start()
    when_do(ring.core == 0, lambda: local_copy(5, wk_in).start())
    when_do(ring.core == 1, lambda: local_copy(5, wv_in).start())
    local_copy(0).wait()
    local_copy(1).wait()
    pl.semaphore_wait(barrier, len(ring.peers()))
    mlp.start(0)

    def norm_body(t, _):
        here = rows_at(t * tile, tile)
        slot = lax.rem(t, depth)
        for which in range(2):
            norm_fetch(which, t).wait()
        y = stage[slot, 0:tile, :]
        norm[here, :] = (y * inv_rms_of(y)).astype(BF16)
        grad[here, :] = stage[slot, tile:2 * tile, :].astype(BF16)

        @pl.when(t + depth < n_tiles)
        def _():
            for which in range(2):
                norm_fetch(which, t + depth).start()

        when_do(t == n_tiles // 3, lambda: mlp.start(1))
        return 0

    lax.fori_loop(0, n_tiles, norm_body, 0)

    def mlp_hidden(here, cols):
        pre = dot_nt(norm[here, :], w1[cols, :])
        d_act = dot_nt(grad[here, :], w2[cols, :])
        act, slope = gelu_and_slope(pre)
        return act.astype(BF16), (d_act * slope).astype(BF16)

    def stage_copy(which, src, t, span, slot=0):
        return pltpu.make_async_copy(hbm_rows(src, t * span, span), stage.at[which, rows_at(slot * span, span)],
                                     stage_sem.at[which, slot])

    mlp_ins = (y1, y2, dy1)

    def start_mlp_ins(t):
        for which, src in enumerate(mlp_ins):
            stage_copy(which, src, t, tile, lax.rem(t, 2)).start()

    def r(shares, hop, piece):
        with jax.named_scope('ring'):
            shares.take_ring(hop, piece)

    def y(shares, hop, piece):
        with jax.named_scope('pair'):
            shares.take_pair(hop, piece)

    def both(step, shares, hop):
        step(shares, hop, 0)
        step(shares, hop, 1)

    plan = {
        ('own', 0): lambda: r(mlp, 1, 0),
        ('own', 1): lambda: r(mlp, 1, 1),
        ('own', 2): lambda: y(mlp, 1, 0),
        ('mlp1', -1): lambda: (r(mlp, 2, 0), y(mlp, 1, 1), mlp.take_sibling(1)),
        ('mlp1', 0): lambda: (r(mlp, 2, 1), y(mlp, 2, 0)),
        ('mlp1', 1): lambda: (r(mlp, 3, 0), y(mlp, 2, 1)),
        ('mlp1', 2): lambda: r(mlp, 3, 1),
        ('mlp2', -1): lambda: mlp.take_sibling(2),
        ('mlp2', 0): lambda: (y(mlp, 3, 0), r(mlp, 4, 0)),
        ('mlp2', 1): lambda: (r(mlp, 4, 1), y(mlp, 3, 1), attn.start(0), attn.start(1)),
        ('mlp2', 2): lambda: y(mlp, 4, 0),
        ('mlp3', -1): lambda: (mlp.take_sibling(3), start_mlp_ins(0), start_mlp_ins(1)),
        ('mlp3', 0): lambda: y(mlp, 4, 1),
        ('mlp3', 1): lambda: both(r, attn, 1),
        ('last', -1): lambda: mlp.take_sibling(4),
        ('last', 0): lambda: (both(y, attn, 1), r(attn, 2, 0)),
        ('last', 1): lambda: r(attn, 2, 1),
        ('last', 2): lambda: (both(y, attn, 2), r(attn, 3, 0)),
        ('attn0', -1): lambda: (attn.wait_own(), attn.take_sibling(1)),
        ('attn0', 0): lambda: (r(attn, 3, 1), y(attn, 3, 0)),
        ('attn0', 1): lambda: (both(r, attn, 4), y(attn, 3, 1)),
        ('attn1', -1): lambda: attn.take_sibling(2),
        ('attn1', 0): lambda: both(y, attn, 4),
        ('attn2', -1): lambda: attn.take_sibling(3),
        ('attn3', -1): lambda: attn.take_sibling(4),
    }

    def serve(phase, t):
        for (name, at), step in plan.items():
            if name == phase and at >= 0:
                when_do(t == at, step)

    def serve_loop(kind, index, indices, t=None):
        for i in indices:
            if t is None and (f'{kind}{i}', -1) in plan:
                when_do(index == i, plan[f'{kind}{i}', -1])
            for at in range(n_bigs if t is not None else 0):
                if (f'{kind}{i}', at) in plan:
                    when_do((index == i) & (t == at), plan[f'{kind}{i}', at])

    width = CORES * size
    mlp.wait_own()
    part[...] = jnp.zeros_like(part)

    def mlp_own(t, _):
        here = rows_at(t * big, big)
        cols = rows_at(0, width)
        act, d_pre = mlp_hidden(here, cols)
        acc_a[here, :] = dot_nn(act, w2[cols, :])
        acc_b[here, :] = dot_nn(d_pre, w1[cols, :])
        part[0:width, :] += dot_tn(d_pre, norm[here, :])
        part[width:2 * width, :] += dot_tn(act, grad[here, :])
        serve('own', t)
        return 0

    with jax.named_scope('mlp_own'):
        lax.fori_loop(0, n_bigs, mlp_own, 0)

    eye = (lax.broadcasted_iota(jnp.int32, (hd, hd), 0) == lax.broadcasted_iota(jnp.int32, (hd, hd), 1)).astype(BF16)
    for i in range(2):
        local_copy(4 + i, wk_in).wait()
        wa[rows_at(own_a + i * hd, hd), :] = dot_nt(eye, wa[flat[i]]).astype(BF16)
    local_copy(2).wait()
    local_copy(3).wait()

    def mlp_dw(mat, which):
        core = 1 - ring.core if which else ring.core
        return rows_at(mat * width + core * size, size)

    def mlp_dw_out(mat):
        return pltpu.make_async_copy(dw_attn.at[rows_at(mat * size, size)], dw_mlp.at[mat], dw_sem.at[mat])

    def mlp_dw_copy(mat):
        return remote(part.at[mlp_dw(mat, 1)], dw_attn.at[rows_at(mat * size, size)], dw_send.at[mat], dw_recv.at[mat],
                      ring.sibling)

    def mlp_pair(hop, _):
        with jax.named_scope('mlp_wait'):
            serve_loop('mlp', hop, range(1, far))
        cols = rows_at((2 * hop - 1) * width, 2 * width)

        def body(t, _):
            here = rows_at(t * big, big)
            act, d_pre = mlp_hidden(here, cols)
            acc_a[here, :] += dot_nn(act, w2[cols, :])
            acc_b[here, :] += dot_nn(d_pre, w1[cols, :])
            serve_loop('mlp', hop, range(1, far), t)
            return 0

        with jax.named_scope('mlp_pair'):
            lax.fori_loop(0, n_bigs, body, 0)

        @pl.when(hop == 1)
        def _():
            for mat in range(2):
                mlp_dw_copy(mat).start()

        return 0

    lax.fori_loop(1, far, mlp_pair, 0)

    def out_copy(which, t):
        return pltpu.make_async_copy((acc_a, acc_b)[which].at[rows_at(t * tile, tile)],
                                     hbm_rows((x2, dx1)[which], t * tile, tile), out_sem.at[which, t])

    def sib_copy(which, t):
        span = tile if which < 2 else big
        here = rows_at(t * span, span)
        dst = (hbm_rows(x2, t * span, span), hbm_rows(dx1, t * span, span), x1_sib.at[here], dx2_sib.at[here])[which]
        return remote((acc_a, acc_b)[which % 2].at[here], dst, sib_send.at[which, t], sib_recv.at[which, t], ring.sibling)

    with jax.named_scope('mlp_wait'):
        plan['last', -1]()
    for mat in range(2):
        mlp_dw_copy(mat).wait_send()
        mlp_dw_copy(mat).wait_recv()
        mine = rows_at(mat * size, size)
        dw_attn[mine, :] = dw_attn[mine, :] + part[mlp_dw(mat, 0), :]
        mlp_dw_out(mat).start()

    def mlp_last(t, _):
        slot = lax.rem(t, 2)
        here = rows_at(t * tile, tile)
        cols = rows_at((2 * far - 1) * width, width)
        for which, src in enumerate(mlp_ins):
            stage_copy(which, src, t, tile, slot).wait()
        now = rows_at(slot * tile, tile)
        act, d_pre = mlp_hidden(here, cols)
        x = stage[1, now, :] - (acc_a[here, :] + dot_nn(act, w2[cols, :]))
        d = stage[2, now, :] + rms_back(stage[0, now, :], acc_b[here, :] + dot_nn(d_pre, w1[cols, :]))
        acc_a[here, :] = x
        acc_b[here, :] = d
        norm[here, :] = (x * inv_rms_of(x)).astype(BF16)
        grad[here, :] = d.astype(BF16)
        when_do(t + 2 < n_tiles, lambda: start_mlp_ins(t + 2))

        @pl.when(t == n_tiles - 1)
        def _():
            for mat in range(2):
                mlp_dw_out(mat).wait()

        ratio = big // tile
        for at in range(n_bigs):
            if ('last', at) in plan:
                when_do(t == ratio * at + ratio - 1, plan['last', at])
        for which in range(2):
            sib_copy(which, t).start()

        def start_out(first, end):
            for k in range(first, end):
                for which in range(2):
                    out_copy(which, k).start()

        when_do(t == n_tiles - 2, lambda: start_out(0, n_tiles - 2))
        when_do(t == n_tiles - 1, lambda: start_out(n_tiles - 2, n_tiles))
        return 0

    with jax.named_scope('mlp_last'):
        lax.fori_loop(0, n_tiles, mlp_last, 0)

    row_pos = lax.broadcasted_iota(jnp.int32, (BLOCK, BLOCK), 0)
    col_pos = lax.broadcasted_iota(jnp.int32, (BLOCK, BLOCK), 1)
    seq = BLOCK // 2
    causal = (col_pos <= row_pos) & ((col_pos < seq) == (row_pos < seq))
    first_seq = ring.core * (rows_own // seq)

    def masks_of(t):
        out = []
        for block in range(big // BLOCK):
            at = first_seq + t * (big // seq) + 2 * block
            end = jnp.where(col_pos < seq, lens[at], seq + lens[at + 1])
            out.append(causal & (col_pos < end))
        return out

    def attn_pair(t, j, use_f):
        here = rows_at(t * big, big)
        masks = masks_of(t)

        def weights(i):
            first = (2 * j + i) * CORES * a_part
            return [jnp.concatenate([wa[rows_at(first + core * a_part + which * hd, hd), :] for core in range(CORES)], axis=0)
                    for which in range(3)]

        def project(i):
            return attn_projections(norm[here, :], grad[here, :], *weights(i))

        def grad_sum(i, factors):
            q_w, kv_w, _ = weights(i)
            _, dq, d0, d1 = factors
            return dot_nn(dq, q_w) + dot_nn(d0, kv_w) + dot_nn(d1, kv_w)

        first = project(0)
        scores = attn_scores(big, hd, first)
        second = project(1)
        factors = attn_grads(big, hd, first, attn_softmax(hd, scores, masks))
        scores = attn_scores(big, hd, second)
        f = dot_nn(factors[0], weights(0)[2])
        g = grad_sum(0, factors)
        more = attn_grads(big, hd, second, attn_softmax(hd, scores, masks))
        f = f + dot_nn(more[0], weights(1)[2])
        use_f(f)
        return g + grad_sum(1, more), factors

    part[...] = jnp.zeros_like(part)
    own_part = 4 * hd
    mlp.finish(w1)

    def attn_dw(which):
        core = 1 - ring.core if which else ring.core
        return rows_at(core * own_part, own_part)

    def attn_dw_copy():
        return remote(part.at[attn_dw(1)], dw_attn.at[rows_at(0, own_part)], dw_send.at[2], dw_recv.at[2], ring.sibling)

    per_band = w1.shape[1] // hd

    def kept_at(k):
        return slice(k // per_band * big, (k // per_band + 1) * big), slice(k % per_band * hd, (k % per_band + 1) * hd)

    def attn_pairs(j, _):
        with jax.named_scope('attn_wait'):
            serve_loop('attn', j, range(far - 1))

        def body(t, _):
            here = rows_at(t * big, big)

            @pl.when(j == 0)
            def _():
                for which in range(2):
                    for i in range(big // tile):
                        out_copy(which, t * (big // tile) + i).wait()
                        sib_copy(which, t * (big // tile) + i).wait_send()
                acc_a[here, :] = jnp.zeros((big, acc_a.shape[1]), F32)
                acc_b[here, :] = jnp.zeros((big, acc_b.shape[1]), F32)

            def add_f(f):
                acc_a[here, :] += f

            g, own_factors = attn_pair(t, j, add_f)
            acc_b[here, :] += g
            a, dq, *dkv = own_factors
            both_heads = [slice(head * hd, (head + 1) * hd) for head in range(CORES)]
            left = [f for head, cols in enumerate(both_heads) for f in (dq[:, cols], dkv[head][:, :hd], dkv[head][:, hd:])]
            for k, factor in enumerate(left + [a[:, cols] for cols in both_heads]):
                w1[kept_at(k)] = factor

            @pl.when(j == 0)
            def _():
                where = [head * own_part + which * hd for head in range(CORES) for which in range(3)]
                where += [head * own_part + 3 * hd for head in range(CORES)]
                for k in range(0, 4 * CORES, 2):
                    right = norm if k < 3 * CORES else grad
                    two = dot_tn(jnp.concatenate([w1[kept_at(k)], w1[kept_at(k + 1)]], axis=1), right[here, :])
                    part[where[k]:where[k] + hd, :] += two[:hd]
                    part[where[k + 1]:where[k + 1] + hd, :] += two[hd:]

            serve_loop('attn', j, range(far - 1), t)
            return 0

        with jax.named_scope('attn_pair'):
            lax.fori_loop(0, n_bigs, body, 0)

        @pl.when(j == 1)
        def _():
            attn_dw_copy().start()

        return 0

    lax.fori_loop(0, far - 1, attn_pairs, 0)

    with jax.named_scope('attn_wait'):
        plan['attn3', -1]()
    attn_dw_copy().wait_send()
    attn_dw_copy().wait_recv()
    mine = rows_at(0, own_part)
    dw_attn[mine, :] = dw_attn[mine, :] + part[attn_dw(0), :]

    attn_ins = (y1, x2, dy2)

    def attn_last(t, _):
        here = rows_at(t * big, big)
        for which, src in enumerate(attn_ins):
            stage_copy(which, src, t, big).start()

        def x1_ends(f):
            stage_copy(0, y1, t, big).wait()
            acc_a[here, :] = stage[0] - (acc_a[here, :] + f)
            sib_copy(2, t).start()

        g, _ = attn_pair(t, far - 1, x1_ends)
        stage_copy(1, x2, t, big).wait()
        stage_copy(2, dy2, t, big).wait()
        acc_b[here, :] = stage[2] + rms_back(stage[1], acc_b[here, :] + g)
        sib_copy(3, t).start()
        return 0

    with jax.named_scope('attn_last'):
        lax.fori_loop(0, n_bigs, attn_last, 0)

    attn.finish(wa)

    def drain(t, _):
        for which in range(2, 4):
            sib_copy(which, t).wait_send()
            sib_copy(which, t).wait_recv()
        for which in range(2):
            for i in range(big // tile):
                sib_copy(which, t * (big // tile) + i).wait_recv()
        return 0

    with jax.named_scope('drain'):
        lax.fori_loop(0, n_bigs, drain, 0)


def block_back(n_tp, side, y1, y2, dy1, dy2, lens, w1_own, w2_own, wq_in, wk_in, wv_in, wo_own, tile=256, big=512):
    tokens, d = y1.shape
    size, hd = w1_own.shape[0], wo_own.shape[0]
    chips = n_tp // CORES
    hops = chips // 2
    half = tokens // CORES
    n_tiles = half // tile
    hidden, heads = n_tp * size, n_tp * hd
    hbm = pl.BlockSpec(memory_space=pl.ANY)
    dma = pltpu.SemaphoreType.DMA
    flops = 8 * half * d * hidden + 14 * half * d * heads
    part_rows = max(4 * size, CORES * 4 * hd)
    own_rows = max(2 * size, 4 * hd)

    ring_sems = [dma((2, 2, hops)), dma((2, 2, chips)), dma((2, chips)), dma((3,))]

    return pl.pallas_call(
        functools.partial(block_kernel, n_tp, side, tile, big),
        name='block_back',
        out_shape=[jax.ShapeDtypeStruct(shape, F32) for shape in ((half, d), (tokens, d), (tokens, d), (half, d), (2, size, d))]
        + [pltpu.VMEM((rows, d), F32) for rows in (own_rows, half, half)],
        in_specs=[hbm] * 11,
        out_specs=[hbm] * 5 + [pl.BlockSpec(memory_space=pltpu.VMEM)] * 3,
        scratch_shapes=[
            pltpu.SMEM(lens.shape, jnp.int32), pltpu.VMEM((hidden, d), BF16), pltpu.VMEM((hidden, d), BF16),
            pltpu.VMEM((3 * heads, d), BF16),
            pltpu.VMEM((half, d), BF16), pltpu.VMEM((half, d), BF16),
            pltpu.VMEM((part_rows, d), F32),
            pltpu.VMEM((3, big, d), F32),
            *ring_sems, *ring_sems,
            dma((2, 3)), dma((3, 2)), dma((2, n_tiles)), dma((4, n_tiles)), dma((4, n_tiles)), dma((3,)), dma((3,)), dma((2,)), dma((6,)),
        ],
        compiler_params=pltpu.CompilerParams(collective_id=0, has_side_effects=True, vmem_limit_bytes=67043328 - 4 * d * (2 * half + own_rows)),
        cost_estimate=pl.CostEstimate(flops=flops, bytes_accessed=10 * tokens * d * 4, transcendentals=half * hidden),
    )(y1, y2, dy1, dy2, lens, w1_own, w2_own, wq_in, wk_in, wv_in, wo_own)


def settle_kernel(chunk, depth, *refs):
    x1_sib, x2_in, dx1_in, dx2_sib, mlp_in, attn_buf, x1_own, dx2_own = refs[:8]
    x1, x2, dx1, dx2, *grads_out = refs[8:18]
    buf, mlp_buf, turned, read_sem, write_sem, small_sem, own_sem = refs[18:]
    tokens, half, hd = x2.shape[0], x1_own.shape[0], turned.shape[2]
    core = lax.rem(lax.axis_index('tp'), CORES)
    jobs = []
    for first in range(0, tokens, chunk):
        jobs += [(x2_in, first, x2, first), (dx1_in, first, dx1, first)]
    for first in range(0, half, chunk):
        jobs += [(x1_sib, first, x1, (1 - core) * half + first), (dx2_sib, first, dx2, (1 - core) * half + first)]

    def read(k):
        src, first, _, _ = jobs[k]
        return pltpu.make_async_copy(src.at[rows_at(first, chunk)], buf.at[k % depth], read_sem.at[k % depth])

    def write(k):
        _, _, dst, first = jobs[k]
        return pltpu.make_async_copy(buf.at[k % depth], dst.at[rows_at(first, chunk)], write_sem.at[k % depth])

    own = [pltpu.make_async_copy(src, dst.at[rows_at(core * half, half)], own_sem.at[i])
           for i, (src, dst) in enumerate(((x1_own, x1), (dx2_own, dx2)))]
    small_writes = [pltpu.make_async_copy(src, dst, small_sem.at[i]) for i, (src, dst) in enumerate(
        [(turned.at[i], grads_out[i]) for i in range(3)] + [(attn_buf.at[rows_at(3 * hd, hd)], grads_out[3]),
                                                            (mlp_buf.at[0], grads_out[4]), (mlp_buf.at[1], grads_out[5])])]
    mlp_read = pltpu.make_async_copy(mlp_in, mlp_buf, small_sem.at[6])
    mlp_read.start()
    for k in range(min(depth, len(jobs))):
        read(k).start()
    for copy in own:
        copy.start()
    for i in range(3):
        turned[i] = attn_buf[i * hd:(i + 1) * hd, :].T
    mlp_read.wait()
    for copy in small_writes:
        copy.start()
    lag = depth // 2
    for k in range(len(jobs)):
        read(k).wait()
        write(k).start()
        if k >= lag:
            write(k - lag).wait()
            if k - lag + depth < len(jobs):
                read(k - lag + depth).start()
    for k in range(max(len(jobs) - lag, 0), len(jobs)):
        write(k).wait()
    for copy in own + small_writes:
        copy.wait()


def settle(hd, x1_sib, x2, dx1, dx2_sib, dw_mlp, dw_attn, x1_own, dx2_own, chunk=256, depth=24):
    tokens, d = x2.shape
    size = dw_mlp.shape[1]
    hbm, vmem = pl.BlockSpec(memory_space=pl.ANY), pl.BlockSpec(memory_space=pltpu.VMEM)
    dma = pltpu.SemaphoreType.DMA
    grads = [(d, hd)] * 3 + [(hd, d), (size, d), (size, d)]
    return pl.pallas_call(
        functools.partial(settle_kernel, chunk, depth),
        name='settle',
        out_shape=[jax.ShapeDtypeStruct((tokens, d), F32)] * 4 + [jax.ShapeDtypeStruct(shape, F32) for shape in grads],
        in_specs=[hbm] * 5 + [vmem] * 3,
        out_specs=[hbm] * 10,
        scratch_shapes=[
            pltpu.VMEM((depth, chunk, d), F32), pltpu.VMEM((2, size, d), F32), pltpu.VMEM((3, d, hd), F32),
            dma((depth,)), dma((depth,)), dma((7,)), dma((2,)),
        ],
        compiler_params=pltpu.CompilerParams(vmem_limit_bytes=36 * 2 ** 20),
        cost_estimate=pl.CostEstimate(flops=0, bytes_accessed=8 * tokens * d * 4, transcendentals=0),
    )(x1_sib, x2, dx1, dx2_sib, pltpu.with_memory_space_constraint(dw_mlp, pltpu.HBM),
      *(pltpu.with_memory_space_constraint(ref, pltpu.VMEM) for ref in (dw_attn, x1_own, dx2_own)))


def layer_back(carry, lens, layer_w, n_tp, side):
    w_query, w_key, w_value, w_out, w_up, w_down = layer_w
    d, _, hd = w_query.shape
    heads = [w.reshape(d, hd) for w in (w_query, w_key, w_value)]
    *acts, dw_mlp, dw_attn, x1_own, dx2_own = block_back(n_tp, side, *carry, lens, w_up.T, w_down, *heads,
                                                         w_out.reshape(hd, d))
    *carry, dwq, dwk, dwv, dwo, dw1, dw2 = settle(hd, *acts, dw_mlp, dw_attn, x1_own, dx2_own)
    grads = (dwq.reshape(w_query.shape), dwk.reshape(w_key.shape), dwv.reshape(w_value.shape), dwo.reshape(w_out.shape),
             dw1.T, dw2)
    return tuple(carry), grads


def solution(mesh):
    act_spec = P('dp', None, None)
    w_specs = (P(None, None, 'tp', None), P(None, None, 'tp', None), P(None, None, 'tp', None),
               P(None, 'tp', None, None), P(None, None, 'tp'), P(None, 'tp', None))
    g_specs = (P('dp', None, 'tp', None), P('dp', None, 'tp', None), P('dp', None, 'tp', None),
               P('dp', 'tp', None, None), P('dp', None, 'tp'), P('dp', 'tp', None))
    n_tp = mesh.shape['tp']
    side = math.isqrt(mesh.shape['dp'])
    if side % 2 or side * side != mesh.shape['dp']:
        side = 0

    def local_fn(y_one, y_two, dy_one, dy_two, seq_lens, *weights):
        n_seqs, seq_len, d = y_one.shape
        carry = tuple(act.reshape(n_seqs * seq_len, d) for act in (y_one, y_two, dy_one, dy_two))
        n_layers = weights[0].shape[0]
        grads_by_layer = [None] * n_layers
        for layer in reversed(range(n_layers)):
            (x1, x2, dx1, dx2), grads_by_layer[layer] = layer_back(carry, seq_lens, [w[layer] for w in weights], n_tp, side)
            carry = (x1, x2, dx1, dx2)
        stacked = tuple(jnp.stack(grads) for grads in zip(*grads_by_layer))
        return tuple(act.reshape(n_seqs, seq_len, d) for act in carry) + stacked

    return jax.shard_map(local_fn, mesh=mesh,
                         in_specs=(act_spec,) * 4 + (P('dp'),) + w_specs,
                         out_specs=(act_spec,) * 4 + g_specs,
                         check_vma=False)
```

```python
import functools
import math

import jax
import jax.numpy as jnp
from jax import lax
from jax.experimental import pallas as pl
from jax.experimental.pallas import tpu as pltpu
from jax.sharding import PartitionSpec as P

F32 = jnp.float32
BF16 = jnp.bfloat16
EPS = 1e-5
MASK_VALUE = -1e30
CORES = 2
BLOCK = 128
GELU_A = 0.7978845608028654
GELU_B = 0.044715
LOG2_E = 1.4426950408889634


def dot_nt(a, b):
    return lax.dot_general(a, b, (((1,), (1,)), ((), ())), preferred_element_type=F32)


def dot_nn(a, b):
    return lax.dot_general(a, b, (((1,), (0,)), ((), ())), preferred_element_type=F32)


def dot_tn(a, b):
    return lax.dot_general(a, b, (((0,), (0,)), ((), ())), preferred_element_type=F32)


def gelu_and_slope(x):
    sq = x * x
    t = jnp.tanh(GELU_A * (x + GELU_B * (sq * x)))
    half = 0.5 * (1.0 + t)
    slope = half + (0.5 * x) * (1.0 - t * t) * (GELU_A * (1.0 + (3.0 * GELU_B) * sq))
    return x * half, slope


def inv_rms_of(x):
    return lax.rsqrt(jnp.mean(x * x, axis=-1, keepdims=True) + EPS)


def rms_back(x, grad):
    inv = inv_rms_of(x)
    normed = x * inv
    return inv * (grad - normed * jnp.mean(grad * normed, axis=-1, keepdims=True))


def rows_at(start, size):
    return pl.ds(start if isinstance(start, int) else pl.multiple_of(start, 16), size)


def attn_projections(normed, grad, wq, wkv, wo):
    return dot_nt(normed, wq).astype(BF16), dot_nt(normed, wkv).astype(BF16), dot_nt(grad, wo).astype(BF16)


def attn_scores(span, hd, proj):
    q, kv, da = proj
    out = []
    for first in range(0, span, BLOCK):
        r = slice(first, first + BLOCK)
        q_two = jnp.concatenate([q[r, :hd], q[r, hd:]], axis=0)
        da_two = jnp.concatenate([da[r, :hd], da[r, hd:]], axis=0)
        out.append((dot_nt(q_two, kv[r, :hd]), dot_nt(da_two, kv[r, hd:])))
    return out


def attn_softmax(hd, scores, masks):
    scale = hd ** -0.5
    out = []
    for (s, dp), mask in zip(scores, masks):
        s = jnp.where(jnp.concatenate([mask, mask], axis=0), s, MASK_VALUE)
        ex = jnp.exp2((s - jnp.max(s, axis=-1, keepdims=True)) * (scale * LOG2_E))
        p = ex * (1.0 / jnp.sum(ex, axis=-1, keepdims=True))
        ds = (p * (dp - jnp.sum(dp * p, axis=-1, keepdims=True)) * scale).astype(BF16)
        out.append((p.astype(BF16), ds))
    return out


def attn_grads(span, hd, proj, probs):
    q, kv, da = proj
    a, dq, dkv = [], [], ([], [])
    for first, (p, ds) in zip(range(0, span, BLOCK), probs):
        r = slice(first, first + BLOCK)
        two = dot_nn(p, kv[r, hd:]).astype(BF16)
        a.append(jnp.concatenate([two[:BLOCK], two[BLOCK:]], axis=1))
        two = dot_nn(ds, kv[r, :hd]).astype(BF16)
        dq.append(jnp.concatenate([two[:BLOCK], two[BLOCK:]], axis=1))
        for head in range(CORES):
            own, h = slice(head * BLOCK, (head + 1) * BLOCK), slice(head * hd, (head + 1) * hd)
            dkv[head].append(jnp.concatenate([dot_tn(ds[own], q[r, h]).astype(BF16),
                                              dot_tn(p[own], da[r, h]).astype(BF16)], axis=1))
    return tuple(jnp.concatenate(parts, axis=0) for parts in (a, dq, *dkv))


def when_do(condition, step):
    @pl.when(condition)
    def _():
        step()


class Ring:
    def __init__(self, n_tp, side):
        self.chips = n_tp // CORES
        self.far = self.chips // 2
        me, group = lax.axis_index('tp'), lax.axis_index('dp')
        self.core = lax.rem(me, CORES)
        chip = lax.div(me, CORES)
        up = lax.rem(chip + 1, self.chips) * CORES + self.core
        down = lax.rem(chip + self.chips - 1, self.chips) * CORES + self.core
        self.toward = ({'tp': up}, {'tp': down})
        self.sibling = {'tp': chip * CORES + (1 - self.core)}
        self.shared = side > 0
        if self.shared:
            over, down = lax.div(group, side), lax.rem(group, side)
            self.parity = lax.rem(over + down, 2)
            self.partners = ({'dp': group + 1 - 2 * lax.rem(down, 2)}, {'dp': group + side * (1 - 2 * lax.rem(over, 2))})

    def peers(self):
        return (*self.toward, self.sibling) + (self.partners if self.shared else ())

    def slot(self, hop, way):
        return 2 * hop - 1 if hop == self.far else 2 * hop - 1 + way


def remote(src, dst, send, recv, peer):
    return pltpu.make_async_remote_copy(src_ref=src, dst_ref=dst, send_sem=send, recv_sem=recv,
                                        device_id=peer, device_id_type=pl.DeviceIdType.MESH)


class Shares:
    def __init__(self, ring, refs, rows, sems):
        self.ring, self.refs, self.rows = ring, refs, rows
        self.recv, self.pair_recv, self.d2d_recv, self.sent = sems

    def place(self, piece, slot, low=0, rows=None):
        full, part, first = self.refs[piece]
        return full.at[rows_at((slot * CORES + self.ring.core) * part + first + low, rows or self.rows)]

    def ring_place(self, piece, slot):
        if not self.ring.shared:
            return self.place(piece, slot)
        return self.place(piece, slot, self.ring.parity * (self.rows // 2), self.rows // 2)

    def bundle(self, hop, piece):
        far = self.ring.far
        return () if hop > far else (piece,) if hop == far else (0, 1)

    def hop_copy(self, piece, way, hop):
        slot = 0 if hop == 1 else self.ring.slot(hop - 1, way)
        return remote(self.ring_place(piece, slot), self.ring_place(piece, self.ring.slot(hop, way)), self.sent.at[0],
                      self.recv.at[piece, way, hop - 1], self.ring.toward[way])

    def pair_copies(self, piece, slot):
        if not self.ring.shared:
            return ()
        quarter = self.rows // 4
        refs = [self.place(piece, slot, self.ring.parity * (self.rows // 2) + i * quarter, quarter) for i in range(2)]
        return [remote(ref, ref, self.sent.at[1], self.pair_recv.at[i, piece, slot], self.ring.partners[i])
                for i, ref in enumerate(refs)]

    def sibling_copy(self, piece, slot):
        ref = self.place(piece, slot)
        return remote(ref, ref, self.sent.at[2], self.d2d_recv.at[piece, slot], self.ring.sibling)

    def start(self, piece):
        for way in self.bundle(1, piece):
            self.hop_copy(piece, way, 1).start()
        self.sibling_copy(piece, 0).start()

    def wait_own(self):
        for piece in range(2):
            self.sibling_copy(piece, 0).wait_recv()

    def take_ring(self, hop, piece):
        for way in self.bundle(hop, piece):
            self.hop_copy(piece, way, hop).wait_recv()
            if way in self.bundle(hop + 1, piece):
                self.hop_copy(piece, way, hop + 1).start()
            for copy in self.pair_copies(piece, self.ring.slot(hop, way)):
                copy.start()

    def take_pair(self, hop, piece):
        for way in self.bundle(hop, piece):
            for copy in self.pair_copies(piece, self.ring.slot(hop, way)):
                copy.wait_recv()
            self.sibling_copy(piece, self.ring.slot(hop, way)).start()

    def take_sibling(self, hop):
        for piece in range(2):
            for way in self.bundle(hop, piece):
                self.sibling_copy(piece, self.ring.slot(hop, way)).wait_recv()

    def finish(self, like):
        ring = self.ring
        hops = 2 * (ring.chips - 1)
        counts = (hops * self.rows // 2, hops * self.rows // 2) if ring.shared else (hops * self.rows, 0)
        for kind, rows in enumerate((*counts, 2 * ring.chips * self.rows)):
            if rows:
                ref = like.at[pl.ds(0, rows)]
                pltpu.make_async_copy(ref, ref, self.sent.at[kind]).wait()


def block_kernel(n_tp, side, tile, big, y1, y2, dy1, dy2, lens_in, w1_own, w2_own, wq_in, wk_in, wv_in, wo_own,
                 x1_sib, x2, dx1, dx2_sib, dw_mlp, dw_attn, acc_a, acc_b,
                 lens, w1, w2, wa, norm, grad, part, stage,
                 mlp_recv, mlp_pair_recv, mlp_d2d_recv, mlp_sent, attn_recv, attn_pair_recv, attn_d2d_recv, attn_sent,
                 norm_sem, stage_sem, out_sem, sib_send, sib_recv, dw_send, dw_recv, dw_sem, local_sem):
    ring = Ring(n_tp, side)
    far = ring.far
    size = w1_own.shape[0]
    hd = wo_own.shape[0]
    rows_own = norm.shape[0]
    base = ring.core * rows_own
    n_tiles, n_bigs = rows_own // tile, rows_own // big

    barrier = pltpu.get_barrier_semaphore()
    for peer in ring.peers():
        pl.semaphore_signal(barrier, inc=1, device_id=peer, device_id_type=pl.DeviceIdType.MESH)

    a_part = 3 * hd
    mlp = Shares(ring, ((w1, size, 0), (w2, size, 0)), size,
                 (mlp_recv, mlp_pair_recv, mlp_d2d_recv, mlp_sent))
    attn = Shares(ring, ((wa, a_part, 0), (wa, a_part, a_part // 2)), a_part // 2,
                  (attn_recv, attn_pair_recv, attn_d2d_recv, attn_sent))

    def hbm_rows(ref, first, rows):
        return ref.at[rows_at(base + first, rows)]

    depth = stage.shape[0]

    def norm_fetch(which, t):
        slot = lax.rem(t, depth)
        return pltpu.make_async_copy(hbm_rows((y1, dy2)[which], t * tile, tile), stage.at[slot, rows_at(which * tile, tile)],
                                     norm_sem.at[which, slot])

    for t in range(min(depth, n_tiles)):
        for which in range(2):
            norm_fetch(which, t).start()

    depth_w = w1.shape[1]
    flat = [(slice(wa.shape[0] - (2 - i) * depth_w, wa.shape[0] - (1 - i) * depth_w), slice(0, hd)) for i in range(2)]
    own_a = ring.core * a_part

    def local_copy(i, src=None):
        src = (w1_own, w2_own, wo_own, lens_in, wq_in, src)[i]
        dst = (mlp.place(0, 0), mlp.place(1, 0), wa.at[rows_at(own_a + 2 * hd, hd)], lens, wa.at[flat[0]], wa.at[flat[1]])[i]
        return pltpu.make_async_copy(src, dst, local_sem.at[i])

    for i in range(5):
        local_copy(i).start()
    when_do(ring.core == 0, lambda: local_copy(5, wk_in).start())
    when_do(ring.core == 1, lambda: local_copy(5, wv_in).start())
    local_copy(0).wait()
    local_copy(1).wait()
    pl.semaphore_wait(barrier, len(ring.peers()))
    mlp.start(0)

    def norm_body(t, _):
        here = rows_at(t * tile, tile)
        slot = lax.rem(t, depth)
        for which in range(2):
            norm_fetch(which, t).wait()
        y = stage[slot, 0:tile, :]
        norm[here, :] = (y * inv_rms_of(y)).astype(BF16)
        grad[here, :] = stage[slot, tile:2 * tile, :].astype(BF16)

        @pl.when(t + depth < n_tiles)
        def _():
            for which in range(2):
                norm_fetch(which, t + depth).start()

        when_do(t == n_tiles // 3, lambda: mlp.start(1))
        return 0

    lax.fori_loop(0, n_tiles, norm_body, 0)

    def mlp_hidden(here, cols):
        pre = dot_nt(norm[here, :], w1[cols, :])
        d_act = dot_nt(grad[here, :], w2[cols, :])
        act, slope = gelu_and_slope(pre)
        return act.astype(BF16), (d_act * slope).astype(BF16)

    def stage_copy(which, src, t, span, slot=0):
        return pltpu.make_async_copy(hbm_rows(src, t * span, span), stage.at[which, rows_at(slot * span, span)],
                                     stage_sem.at[which, slot])

    mlp_ins = (y1, y2, dy1)

    def start_mlp_ins(t):
        for which, src in enumerate(mlp_ins):
            stage_copy(which, src, t, tile, lax.rem(t, 2)).start()

    def r(shares, hop, piece):
        with jax.named_scope('ring'):
            shares.take_ring(hop, piece)

    def y(shares, hop, piece):
        with jax.named_scope('pair'):
            shares.take_pair(hop, piece)

    def both(step, shares, hop):
        step(shares, hop, 0)
        step(shares, hop, 1)

    plan = {
        ('own', 0): lambda: r(mlp, 1, 0),
        ('own', 1): lambda: r(mlp, 1, 1),
        ('own', 2): lambda: y(mlp, 1, 0),
        ('mlp1', -1): lambda: (r(mlp, 2, 0), y(mlp, 1, 1), mlp.take_sibling(1)),
        ('mlp1', 0): lambda: (r(mlp, 2, 1), y(mlp, 2, 0)),
        ('mlp1', 1): lambda: (r(mlp, 3, 0), y(mlp, 2, 1)),
        ('mlp1', 2): lambda: r(mlp, 3, 1),
        ('mlp2', -1): lambda: mlp.take_sibling(2),
        ('mlp2', 0): lambda: (y(mlp, 3, 0), r(mlp, 4, 0)),
        ('mlp2', 1): lambda: (r(mlp, 4, 1), y(mlp, 3, 1), attn.start(0), attn.start(1)),
        ('mlp2', 2): lambda: y(mlp, 4, 0),
        ('mlp3', -1): lambda: (mlp.take_sibling(3), start_mlp_ins(0), start_mlp_ins(1)),
        ('mlp3', 0): lambda: y(mlp, 4, 1),
        ('mlp3', 1): lambda: both(r, attn, 1),
        ('last', -1): lambda: mlp.take_sibling(4),
        ('last', 0): lambda: (y(attn, 1, 0), r(attn, 2, 0)),
        ('last', 1): lambda: (y(attn, 1, 1), r(attn, 2, 1)),
        ('last', 2): lambda: r(attn, 3, 0),
        ('attn0', -1): lambda: (attn.wait_own(), attn.take_sibling(1)),
        ('attn0', 0): lambda: (both(y, attn, 2), r(attn, 3, 1)),
        ('attn0', 1): lambda: y(attn, 3, 0),
        ('attn0', 2): lambda: (both(r, attn, 4), y(attn, 3, 1)),
        ('attn1', -1): lambda: attn.take_sibling(2),
        ('attn1', 1): lambda: both(y, attn, 4),
        ('attn2', -1): lambda: attn.take_sibling(3),
        ('attn3', -1): lambda: attn.take_sibling(4),
    }

    def serve(phase, t):
        for (name, at), step in plan.items():
            if name == phase and at >= 0:
                when_do(t == at, step)

    def serve_loop(kind, index, indices, t=None):
        for i in indices:
            if t is None and (f'{kind}{i}', -1) in plan:
                when_do(index == i, plan[f'{kind}{i}', -1])
            for at in range(n_bigs if t is not None else 0):
                if (f'{kind}{i}', at) in plan:
                    when_do((index == i) & (t == at), plan[f'{kind}{i}', at])

    width = CORES * size
    mlp.wait_own()
    part[...] = jnp.zeros_like(part)

    def mlp_own(t, _):
        here = rows_at(t * big, big)
        cols = rows_at(0, width)
        act, d_pre = mlp_hidden(here, cols)
        acc_a[here, :] = dot_nn(act, w2[cols, :])
        acc_b[here, :] = dot_nn(d_pre, w1[cols, :])
        part[0:width, :] += dot_tn(d_pre, norm[here, :])
        part[width:2 * width, :] += dot_tn(act, grad[here, :])
        serve('own', t)
        return 0

    with jax.named_scope('mlp_own'):
        lax.fori_loop(0, n_bigs, mlp_own, 0)

    eye = (lax.broadcasted_iota(jnp.int32, (hd, hd), 0) == lax.broadcasted_iota(jnp.int32, (hd, hd), 1)).astype(BF16)
    for i in range(2):
        local_copy(4 + i, wk_in).wait()
        wa[rows_at(own_a + i * hd, hd), :] = dot_nt(eye, wa[flat[i]]).astype(BF16)
    local_copy(2).wait()
    local_copy(3).wait()

    def mlp_dw(mat, which):
        core = 1 - ring.core if which else ring.core
        return rows_at(mat * width + core * size, size)

    def mlp_dw_out(mat):
        return pltpu.make_async_copy(dw_attn.at[rows_at(mat * size, size)], dw_mlp.at[mat], dw_sem.at[mat])

    def mlp_dw_copy(mat):
        return remote(part.at[mlp_dw(mat, 1)], dw_attn.at[rows_at(mat * size, size)], dw_send.at[mat], dw_recv.at[mat],
                      ring.sibling)

    def mlp_pair(hop, _):
        with jax.named_scope('mlp_wait'):
            serve_loop('mlp', hop, range(1, far))
        cols = rows_at((2 * hop - 1) * width, 2 * width)

        def body(t, _):
            here = rows_at(t * big, big)
            act, d_pre = mlp_hidden(here, cols)
            acc_a[here, :] += dot_nn(act, w2[cols, :])
            acc_b[here, :] += dot_nn(d_pre, w1[cols, :])
            serve_loop('mlp', hop, range(1, far), t)
            return 0

        with jax.named_scope('mlp_pair'):
            lax.fori_loop(0, n_bigs, body, 0)

        @pl.when(hop == 1)
        def _():
            for mat in range(2):
                mlp_dw_copy(mat).start()

        return 0

    lax.fori_loop(1, far, mlp_pair, 0)

    def out_copy(which, t):
        return pltpu.make_async_copy((acc_a, acc_b)[which].at[rows_at(t * tile, tile)],
                                     hbm_rows((x2, dx1)[which], t * tile, tile), out_sem.at[which, t])

    def sib_copy(which, t):
        span = tile if which < 2 else big
        here = rows_at(t * span, span)
        dst = (hbm_rows(x2, t * span, span), hbm_rows(dx1, t * span, span), x1_sib.at[here], dx2_sib.at[here])[which]
        return remote((acc_a, acc_b)[which % 2].at[here], dst, sib_send.at[which, t], sib_recv.at[which, t], ring.sibling)

    with jax.named_scope('mlp_wait'):
        plan['last', -1]()
    for mat in range(2):
        mlp_dw_copy(mat).wait_send()
        mlp_dw_copy(mat).wait_recv()
        mine = rows_at(mat * size, size)
        dw_attn[mine, :] = dw_attn[mine, :] + part[mlp_dw(mat, 0), :]
        mlp_dw_out(mat).start()

    def mlp_last(t, _):
        slot = lax.rem(t, 2)
        here = rows_at(t * tile, tile)
        cols = rows_at((2 * far - 1) * width, width)
        for which, src in enumerate(mlp_ins):
            stage_copy(which, src, t, tile, slot).wait()
        now = rows_at(slot * tile, tile)
        act, d_pre = mlp_hidden(here, cols)
        x = stage[1, now, :] - (acc_a[here, :] + dot_nn(act, w2[cols, :]))
        d = stage[2, now, :] + rms_back(stage[0, now, :], acc_b[here, :] + dot_nn(d_pre, w1[cols, :]))
        acc_a[here, :] = x
        acc_b[here, :] = d
        norm[here, :] = (x * inv_rms_of(x)).astype(BF16)
        grad[here, :] = d.astype(BF16)
        when_do(t + 2 < n_tiles, lambda: start_mlp_ins(t + 2))

        @pl.when(t == n_tiles - 1)
        def _():
            for mat in range(2):
                mlp_dw_out(mat).wait()

        ratio = big // tile
        for at in range(n_bigs):
            if ('last', at) in plan:
                when_do(t == ratio * at + ratio - 1, plan['last', at])
        for which in range(2):
            sib_copy(which, t).start()

        def start_out(first, end):
            for k in range(first, end):
                for which in range(2):
                    out_copy(which, k).start()

        when_do(t == n_tiles - 2, lambda: start_out(0, n_tiles - 2))
        when_do(t == n_tiles - 1, lambda: start_out(n_tiles - 2, n_tiles))
        return 0

    with jax.named_scope('mlp_last'):
        lax.fori_loop(0, n_tiles, mlp_last, 0)

    row_pos = lax.broadcasted_iota(jnp.int32, (BLOCK, BLOCK), 0)
    col_pos = lax.broadcasted_iota(jnp.int32, (BLOCK, BLOCK), 1)
    seq = BLOCK // 2
    causal = (col_pos <= row_pos) & ((col_pos < seq) == (row_pos < seq))
    first_seq = ring.core * (rows_own // seq)

    def masks_of(t):
        out = []
        for block in range(big // BLOCK):
            at = first_seq + t * (big // seq) + 2 * block
            end = jnp.where(col_pos < seq, lens[at], seq + lens[at + 1])
            out.append(causal & (col_pos < end))
        return out

    def attn_pair(t, j, use_f):
        here = rows_at(t * big, big)
        masks = masks_of(t)

        def weights(i):
            first = (2 * j + i) * CORES * a_part
            return [jnp.concatenate([wa[rows_at(first + core * a_part + which * hd, hd), :] for core in range(CORES)], axis=0)
                    for which in range(3)]

        def project(i):
            return attn_projections(norm[here, :], grad[here, :], *weights(i))

        def grad_sum(i, factors):
            q_w, kv_w, _ = weights(i)
            _, dq, d0, d1 = factors
            return dot_nn(dq, q_w) + dot_nn(d0, kv_w) + dot_nn(d1, kv_w)

        first = project(0)
        scores = attn_scores(big, hd, first)
        second = project(1)
        factors = attn_grads(big, hd, first, attn_softmax(hd, scores, masks))
        scores = attn_scores(big, hd, second)
        f = dot_nn(factors[0], weights(0)[2])
        g = grad_sum(0, factors)
        more = attn_grads(big, hd, second, attn_softmax(hd, scores, masks))
        f = f + dot_nn(more[0], weights(1)[2])
        use_f(f)
        return g + grad_sum(1, more), factors

    part[...] = jnp.zeros_like(part)
    own_part = 4 * hd
    mlp.finish(w1)

    def attn_dw(which):
        core = 1 - ring.core if which else ring.core
        return rows_at(core * own_part, own_part)

    def attn_dw_copy():
        return remote(part.at[attn_dw(1)], dw_attn.at[rows_at(0, own_part)], dw_send.at[2], dw_recv.at[2], ring.sibling)

    per_band = w1.shape[1] // hd

    def kept_at(k):
        return slice(k // per_band * big, (k // per_band + 1) * big), slice(k % per_band * hd, (k % per_band + 1) * hd)

    def attn_pairs(j, _):
        with jax.named_scope('attn_wait'):
            serve_loop('attn', j, range(far - 1))

        def body(t, _):
            here = rows_at(t * big, big)

            @pl.when(j == 0)
            def _():
                for which in range(2):
                    for i in range(big // tile):
                        out_copy(which, t * (big // tile) + i).wait()
                        sib_copy(which, t * (big // tile) + i).wait_send()
                acc_a[here, :] = jnp.zeros((big, acc_a.shape[1]), F32)
                acc_b[here, :] = jnp.zeros((big, acc_b.shape[1]), F32)

            def add_f(f):
                acc_a[here, :] += f

            g, own_factors = attn_pair(t, j, add_f)
            acc_b[here, :] += g
            a, dq, *dkv = own_factors
            both_heads = [slice(head * hd, (head + 1) * hd) for head in range(CORES)]
            left = [f for head, cols in enumerate(both_heads) for f in (dq[:, cols], dkv[head][:, :hd], dkv[head][:, hd:])]
            for k, factor in enumerate(left + [a[:, cols] for cols in both_heads]):
                w1[kept_at(k)] = factor

            @pl.when(j == 0)
            def _():
                where = [head * own_part + which * hd for head in range(CORES) for which in range(3)]
                where += [head * own_part + 3 * hd for head in range(CORES)]
                for k in range(0, 4 * CORES, 2):
                    right = norm if k < 3 * CORES else grad
                    two = dot_tn(jnp.concatenate([w1[kept_at(k)], w1[kept_at(k + 1)]], axis=1), right[here, :])
                    part[where[k]:where[k] + hd, :] += two[:hd]
                    part[where[k + 1]:where[k + 1] + hd, :] += two[hd:]

            serve_loop('attn', j, range(far - 1), t)
            return 0

        with jax.named_scope('attn_pair'):
            lax.fori_loop(0, n_bigs, body, 0)

        @pl.when(j == 1)
        def _():
            attn_dw_copy().start()

        return 0

    lax.fori_loop(0, far - 1, attn_pairs, 0)

    with jax.named_scope('attn_wait'):
        plan['attn3', -1]()
    attn_dw_copy().wait_send()
    attn_dw_copy().wait_recv()
    mine = rows_at(0, own_part)
    dw_attn[mine, :] = dw_attn[mine, :] + part[attn_dw(0), :]

    attn_ins = (y1, x2, dy2)

    def attn_last(t, _):
        here = rows_at(t * big, big)
        for which, src in enumerate(attn_ins):
            stage_copy(which, src, t, big).start()

        def x1_ends(f):
            stage_copy(0, y1, t, big).wait()
            acc_a[here, :] = stage[0] - (acc_a[here, :] + f)
            sib_copy(2, t).start()

        g, _ = attn_pair(t, far - 1, x1_ends)
        stage_copy(1, x2, t, big).wait()
        stage_copy(2, dy2, t, big).wait()
        acc_b[here, :] = stage[2] + rms_back(stage[1], acc_b[here, :] + g)
        sib_copy(3, t).start()
        return 0

    with jax.named_scope('attn_last'):
        lax.fori_loop(0, n_bigs, attn_last, 0)

    attn.finish(wa)

    def drain(t, _):
        for which in range(2, 4):
            sib_copy(which, t).wait_send()
            sib_copy(which, t).wait_recv()
        for which in range(2):
            for i in range(big // tile):
                sib_copy(which, t * (big // tile) + i).wait_recv()
        return 0

    with jax.named_scope('drain'):
        lax.fori_loop(0, n_bigs, drain, 0)


def block_back(n_tp, side, y1, y2, dy1, dy2, lens, w1_own, w2_own, wq_in, wk_in, wv_in, wo_own, tile=256, big=512):
    tokens, d = y1.shape
    size, hd = w1_own.shape[0], wo_own.shape[0]
    chips = n_tp // CORES
    hops = chips // 2
    half = tokens // CORES
    n_tiles = half // tile
    hidden, heads = n_tp * size, n_tp * hd
    hbm = pl.BlockSpec(memory_space=pl.ANY)
    dma = pltpu.SemaphoreType.DMA
    flops = 8 * half * d * hidden + 14 * half * d * heads
    part_rows = max(4 * size, CORES * 4 * hd)
    own_rows = max(2 * size, 4 * hd)

    ring_sems = [dma((2, 2, hops)), dma((2, 2, chips)), dma((2, chips)), dma((3,))]

    return pl.pallas_call(
        functools.partial(block_kernel, n_tp, side, tile, big),
        name='block_back',
        out_shape=[jax.ShapeDtypeStruct(shape, F32) for shape in ((half, d), (tokens, d), (tokens, d), (half, d), (2, size, d))]
        + [pltpu.VMEM((rows, d), F32) for rows in (own_rows, half, half)],
        in_specs=[hbm] * 11,
        out_specs=[hbm] * 5 + [pl.BlockSpec(memory_space=pltpu.VMEM)] * 3,
        scratch_shapes=[
            pltpu.SMEM(lens.shape, jnp.int32), pltpu.VMEM((hidden, d), BF16), pltpu.VMEM((hidden, d), BF16),
            pltpu.VMEM((3 * heads, d), BF16),
            pltpu.VMEM((half, d), BF16), pltpu.VMEM((half, d), BF16),
            pltpu.VMEM((part_rows, d), F32),
            pltpu.VMEM((3, big, d), F32),
            *ring_sems, *ring_sems,
            dma((2, 3)), dma((3, 2)), dma((2, n_tiles)), dma((4, n_tiles)), dma((4, n_tiles)), dma((3,)), dma((3,)), dma((2,)), dma((6,)),
        ],
        compiler_params=pltpu.CompilerParams(collective_id=0, has_side_effects=True, vmem_limit_bytes=67043328 - 4 * d * (2 * half + own_rows)),
        cost_estimate=pl.CostEstimate(flops=flops, bytes_accessed=10 * tokens * d * 4, transcendentals=half * hidden),
    )(y1, y2, dy1, dy2, lens, w1_own, w2_own, wq_in, wk_in, wv_in, wo_own)


def settle_kernel(chunk, depth, *refs):
    x1_sib, x2_in, dx1_in, dx2_sib, mlp_in, attn_buf, x1_own, dx2_own = refs[:8]
    x1, x2, dx1, dx2, *grads_out = refs[8:18]
    buf, mlp_buf, turned, read_sem, write_sem, small_sem, own_sem = refs[18:]
    tokens, half, hd = x2.shape[0], x1_own.shape[0], turned.shape[2]
    core = lax.rem(lax.axis_index('tp'), CORES)
    jobs = []
    for first in range(0, tokens, chunk):
        jobs += [(x2_in, first, x2, first), (dx1_in, first, dx1, first)]
    for first in range(0, half, chunk):
        jobs += [(x1_sib, first, x1, (1 - core) * half + first), (dx2_sib, first, dx2, (1 - core) * half + first)]

    def read(k):
        src, first, _, _ = jobs[k]
        return pltpu.make_async_copy(src.at[rows_at(first, chunk)], buf.at[k % depth], read_sem.at[k % depth])

    def write(k):
        _, _, dst, first = jobs[k]
        return pltpu.make_async_copy(buf.at[k % depth], dst.at[rows_at(first, chunk)], write_sem.at[k % depth])

    own = [pltpu.make_async_copy(src, dst.at[rows_at(core * half, half)], own_sem.at[i])
           for i, (src, dst) in enumerate(((x1_own, x1), (dx2_own, dx2)))]
    small_writes = [pltpu.make_async_copy(src, dst, small_sem.at[i]) for i, (src, dst) in enumerate(
        [(turned.at[i], grads_out[i]) for i in range(3)] + [(attn_buf.at[rows_at(3 * hd, hd)], grads_out[3]),
                                                            (mlp_buf.at[0], grads_out[4]), (mlp_buf.at[1], grads_out[5])])]
    mlp_read = pltpu.make_async_copy(mlp_in, mlp_buf, small_sem.at[6])
    mlp_read.start()
    for k in range(min(depth, len(jobs))):
        read(k).start()
    for copy in own:
        copy.start()
    for i in range(3):
        turned[i] = attn_buf[i * hd:(i + 1) * hd, :].T
    mlp_read.wait()
    for copy in small_writes:
        copy.start()
    lag = depth // 2
    for k in range(len(jobs)):
        read(k).wait()
        write(k).start()
        if k >= lag:
            write(k - lag).wait()
            if k - lag + depth < len(jobs):
                read(k - lag + depth).start()
    for k in range(max(len(jobs) - lag, 0), len(jobs)):
        write(k).wait()
    for copy in own + small_writes:
        copy.wait()


def settle(hd, x1_sib, x2, dx1, dx2_sib, dw_mlp, dw_attn, x1_own, dx2_own, chunk=256, depth=24):
    tokens, d = x2.shape
    size = dw_mlp.shape[1]
    hbm, vmem = pl.BlockSpec(memory_space=pl.ANY), pl.BlockSpec(memory_space=pltpu.VMEM)
    dma = pltpu.SemaphoreType.DMA
    grads = [(d, hd)] * 3 + [(hd, d), (size, d), (size, d)]
    return pl.pallas_call(
        functools.partial(settle_kernel, chunk, depth),
        name='settle',
        out_shape=[jax.ShapeDtypeStruct((tokens, d), F32)] * 4 + [jax.ShapeDtypeStruct(shape, F32) for shape in grads],
        in_specs=[hbm] * 5 + [vmem] * 3,
        out_specs=[hbm] * 10,
        scratch_shapes=[
            pltpu.VMEM((depth, chunk, d), F32), pltpu.VMEM((2, size, d), F32), pltpu.VMEM((3, d, hd), F32),
            dma((depth,)), dma((depth,)), dma((7,)), dma((2,)),
        ],
        compiler_params=pltpu.CompilerParams(vmem_limit_bytes=36 * 2 ** 20),
        cost_estimate=pl.CostEstimate(flops=0, bytes_accessed=8 * tokens * d * 4, transcendentals=0),
    )(x1_sib, x2, dx1, dx2_sib, pltpu.with_memory_space_constraint(dw_mlp, pltpu.HBM),
      *(pltpu.with_memory_space_constraint(ref, pltpu.VMEM) for ref in (dw_attn, x1_own, dx2_own)))


def layer_back(carry, lens, layer_w, n_tp, side):
    w_query, w_key, w_value, w_out, w_up, w_down = layer_w
    d, _, hd = w_query.shape
    heads = [w.reshape(d, hd) for w in (w_query, w_key, w_value)]
    *acts, dw_mlp, dw_attn, x1_own, dx2_own = block_back(n_tp, side, *carry, lens, w_up.T, w_down, *heads,
                                                         w_out.reshape(hd, d))
    *carry, dwq, dwk, dwv, dwo, dw1, dw2 = settle(hd, *acts, dw_mlp, dw_attn, x1_own, dx2_own)
    grads = (dwq.reshape(w_query.shape), dwk.reshape(w_key.shape), dwv.reshape(w_value.shape), dwo.reshape(w_out.shape),
             dw1.T, dw2)
    return tuple(carry), grads


def solution(mesh):
    act_spec = P('dp', None, None)
    w_specs = (P(None, None, 'tp', None), P(None, None, 'tp', None), P(None, None, 'tp', None),
               P(None, 'tp', None, None), P(None, None, 'tp'), P(None, 'tp', None))
    g_specs = (P('dp', None, 'tp', None), P('dp', None, 'tp', None), P('dp', None, 'tp', None),
               P('dp', 'tp', None, None), P('dp', None, 'tp'), P('dp', 'tp', None))
    n_tp = mesh.shape['tp']
    side = math.isqrt(mesh.shape['dp'])
    if side % 2 or side * side != mesh.shape['dp']:
        side = 0

    def local_fn(y_one, y_two, dy_one, dy_two, seq_lens, *weights):
        n_seqs, seq_len, d = y_one.shape
        carry = tuple(act.reshape(n_seqs * seq_len, d) for act in (y_one, y_two, dy_one, dy_two))
        n_layers = weights[0].shape[0]
        grads_by_layer = [None] * n_layers
        for layer in reversed(range(n_layers)):
            (x1, x2, dx1, dx2), grads_by_layer[layer] = layer_back(carry, seq_lens, [w[layer] for w in weights], n_tp, side)
            carry = (x1, x2, dx1, dx2)
        stacked = tuple(jnp.stack(grads) for grads in zip(*grads_by_layer))
        return tuple(act.reshape(n_seqs, seq_len, d) for act in carry) + stacked

    return jax.shard_map(local_fn, mesh=mesh,
                         in_specs=(act_spec,) * 4 + (P('dp'),) + w_specs,
                         out_specs=(act_spec,) * 4 + g_specs,
                         check_vma=False)
```
